768 devices in a mesh: gx: 48 (over z_hi, y, core), gy: 4 (over x), gz: 4 (over z_lo).
Axes of the slice: x: 4, y: 8, z: 12 (z_hi: 3, z_lo: 4; z = z_hi * 4 + z_lo), core: 2. Of those that a mesh axis runs over, the one named last changes fastest.
Arguments:
- thermal_state: float32 [384, 32, 512], P('gx', 'gy', 'gz'), may hold values from 0.5 to 1.5
- diffusivity: float32 [384, 32, 512], P('gx', 'gy', 'gz'), may hold values from 1.1 to 13.2
- staggered_flux_density: float32 [3, 384, 32, 512], P(None, 'gx', 'gy', 'gz'), may hold values from -6 to 6
- bulk_motion: float32 [3, 384, 32, 512], P(None, 'gx', 'gy', 'gz'), may hold values from -3 to 3
- mass_per_volume: float32 [384, 32, 512], P('gx', 'gy', 'gz'), may hold values from 0.5 to 2
Outputs:
- temperature_out: float32 [384, 32, 512], P('gx', 'gy', 'gz')
- face_field_out: float32 [3, 384, 32, 512], P(None, 'gx', 'gy', 'gz')
The draws below stay inside these ranges and needn't reach their ends.
All inputs are finite; a program needn't handle non-finite values.
Results may differ from the reference program's by a relative error of at most 0.00002.
Values sent between devices are 32-bit elements; how exact they have to be, the bound alone decides.
No kernel may reach another device: no remote copies, remote signals or barrier semaphores. Data moves between devices by JAX's collectives and lax.ppermute only.
A program may use at most 128 MiB of HBM per device.

```python
import math
import jax
import jax.numpy as jnp
from jax import lax

SECTIONS = 8
EXTENT_LEADING = 384
EXTENT_MIDDLE = 32
EXTENT_TRAILING = 512


def draw_diffusivity(key, part):
    jitter_key = jax.random.fold_in(key, 11)
    jitter = jnp.exp(jax.random.uniform(jitter_key, (EXTENT_LEADING, EXTENT_MIDDLE, EXTENT_TRAILING), jnp.float32, math.log(0.5), math.log(2.0)))
    position = jnp.arange(EXTENT_LEADING, dtype=jnp.float32) / max(EXTENT_LEADING - 1, 1)
    growth = jnp.exp(math.log(3.0) * position)[:, None, None]
    return (2.2 * growth * jitter).astype(jnp.float32)


def block_levels(rng, extent, split, least, top_value):
    gain, own = 1.0, jax.random.fold_in(rng, 6)
    for axis_at, parts in split:
        draws = jnp.exp(jax.random.uniform(jax.random.fold_in(own, axis_at), (parts,), jnp.float32, least / len(split), top_value / len(split)))
        gain = gain * jnp.repeat(draws, extent[axis_at] // parts).reshape([-1 if axis == axis_at else 1 for axis in range(len(extent))])
    return gain


def bell_draw(rng, shape, scale, most, pieces=(), held_as=jnp.bfloat16):
    drawn = jax.random.normal(rng, shape, jnp.float32) * scale
    if len(pieces) > 0:
        drawn = block_levels(rng, shape, pieces, -0.22, 0.18) * drawn
    return jnp.clip(drawn, min=-most, max=most).astype(held_as)


def setup_inputs(seed: int = 0) -> dict:
    seeds = jax.random.split(jax.random.key(seed), 6)
    thermal_state = jnp.clip(0.5 + 1.0 * jax.random.uniform(seeds[0], (EXTENT_LEADING, EXTENT_MIDDLE, EXTENT_TRAILING), jnp.float32) ** block_levels(seeds[0], (EXTENT_LEADING, EXTENT_MIDDLE, EXTENT_TRAILING), ((0, 48), (1, 4), (2, 4)), -0.2, 0.2), 0.5, 1.5)
    diffusivity = draw_diffusivity(jax.random.fold_in(seeds[5], 71), 0)
    staggered_flux_density = bell_draw(seeds[2], (3, EXTENT_LEADING, EXTENT_MIDDLE, EXTENT_TRAILING), 1.0, 6.0, ((1, 48), (2, 4), (3, 4)), jnp.float32)
    bulk_motion = bell_draw(seeds[3], (3, EXTENT_LEADING, EXTENT_MIDDLE, EXTENT_TRAILING), 0.5, 3.0, ((1, 48), (2, 4), (3, 4)), jnp.float32)
    mass_per_volume = jnp.clip(jnp.exp(math.log(2.0) - 1.3862944 * jax.random.uniform(seeds[4], (EXTENT_LEADING, EXTENT_MIDDLE, EXTENT_TRAILING), jnp.float32) ** block_levels(seeds[4], (EXTENT_LEADING, EXTENT_MIDDLE, EXTENT_TRAILING), ((0, 48), (1, 4), (2, 4)), -0.2, 0.2)), 0.5, 2.0)
    return dict(thermal_state=thermal_state, diffusivity=diffusivity, staggered_flux_density=staggered_flux_density, bulk_motion=bulk_motion, mass_per_volume=mass_per_volume)


GAMMA = 5.0 / 3.0
FACE_FLOOR = 0.25
REFERENCE_SPOT = (0, 0, 0)

def unit_step(direction, amount):
    return tuple((amount if candidate == direction else 0 for candidate in range(3)))

def combine_steps(left_step, right_step):
    return tuple(map(lambda first_part, second_part: first_part + second_part, left_step, right_step))

def even_reach(amount):
    return (amount, amount, amount)

def sites_placed(source, ghost_layer_sites, offset, low_side, high_side):
    extents = source.shape[-3:]
    selector = [slice(None)] * (source.ndim - 3)
    for direction in range(3):
        interior = extents[direction] - 2 * ghost_layer_sites
        begin_at = ghost_layer_sites - low_side[direction] + offset[direction]
        selector.append(slice(begin_at, begin_at + interior + low_side[direction] + high_side[direction]))
    return source[tuple(selector)]

def trim_extent(source, ghost_layer_sites, amount):
    return sites_placed(source, ghost_layer_sites, REFERENCE_SPOT, even_reach(amount), even_reach(amount))

def face_coefficients(diffusion_coefficient, interface_quantities, ghost_layer_sites, reach):
    interior_block = even_reach(reach)
    lookup_arrays = []
    for normal in range(3):
        backward = unit_step(normal, -1)
        kappa_face = 0.5 * (sites_placed(diffusion_coefficient, ghost_layer_sites, REFERENCE_SPOT, interior_block, interior_block) + sites_placed(diffusion_coefficient, ghost_layer_sites, backward, interior_block, interior_block))
        normal_part = sites_placed(interface_quantities[normal], ghost_layer_sites, REFERENCE_SPOT, interior_block, interior_block)
        across = []
        for rotation in (1, 2):
            other_axis = (normal + rotation) % 3
            forward = unit_step(other_axis, 1)
            across.append(0.25 * (sites_placed(interface_quantities[other_axis], ghost_layer_sites, REFERENCE_SPOT, interior_block, interior_block) + sites_placed(interface_quantities[other_axis], ghost_layer_sites, forward, interior_block, interior_block) + sites_placed(interface_quantities[other_axis], ghost_layer_sites, backward, interior_block, interior_block) + sites_placed(interface_quantities[other_axis], ghost_layer_sites, combine_steps(backward, forward), interior_block, interior_block)))
        squared = normal_part * normal_part + across[0] * across[0] + across[1] * across[1]
        scaling = kappa_face / jnp.maximum(squared, FACE_FLOOR)
        lookup_arrays.append((scaling * normal_part * normal_part, scaling * normal_part * across[0], scaling * normal_part * across[1]))
    return lookup_arrays

def diffuse_thermal(profile, ghost_layer_sites, lookup_arrays, reach, target):
    interior_block = even_reach(target)
    balance = None
    for normal in range(3):
        upper_side = tuple((target + (1 if candidate == normal else 0) for candidate in range(3)))
        backward = unit_step(normal, -1)

        def shifted(offset):
            return sites_placed(profile, ghost_layer_sites, offset, interior_block, upper_side)
        slopes = []
        for rotation in (1, 2):
            other_axis = (normal + rotation) % 3
            forward = unit_step(other_axis, 1)
            rearward = unit_step(other_axis, -1)
            slopes.append(0.25 * (shifted(forward) - shifted(rearward) + shifted(combine_steps(backward, forward)) - shifted(combine_steps(backward, rearward))))
        along_normal, along_first, along_second = [sites_placed(coefficient, reach, REFERENCE_SPOT, interior_block, upper_side) for coefficient in lookup_arrays[normal]]
        face_flux = -(along_normal * (shifted(REFERENCE_SPOT) - shifted(backward)) + along_first * slopes[0] + along_second * slopes[1])
        length = face_flux.shape[normal]
        change = lax.slice_in_dim(face_flux, 1, length, axis=normal) - lax.slice_in_dim(face_flux, 0, length - 1, axis=normal)
        balance = -change if balance is None else balance - change
    return balance

def section_weights(total):
    first_rate = 4.0 / (total * total + total - 2)
    factors = [1.0 / 3.0, 1.0 / 3.0, 1.0 / 3.0]
    for ordinal in range(3, total + 1):
        factors.append((ordinal * ordinal + ordinal - 2) / (2.0 * ordinal * (ordinal + 1)))
    layout_recipe = [None, factors[1] * first_rate]
    for ordinal in range(2, total + 1):
        weight_prev = (2.0 * ordinal - 1.0) / ordinal * factors[ordinal] / factors[ordinal - 1]
        weight_older = -(ordinal - 1.0) / ordinal * factors[ordinal] / factors[ordinal - 2]
        rate_prev = weight_prev * first_rate
        rate_zero = -(1.0 - factors[ordinal - 1]) * rate_prev
        layout_recipe.append((weight_prev, weight_older, 1.0 - weight_prev - weight_older, rate_prev, rate_zero))
    return layout_recipe

def subdivision_advance(weights, interval_increment, newest_iterate, newest_extended, previous_iterate, previous_extended, initial, initial_margin, initial_derivative, zero_margin, lookup_arrays, reach):
    target = newest_extended - 1
    weight_prev, weight_older, weight_zero, rate_prev, rate_zero = weights
    prev_rate = diffuse_thermal(newest_iterate, newest_extended, lookup_arrays, reach, target)
    return weight_prev * trim_extent(newest_iterate, newest_extended, target) + weight_older * trim_extent(previous_iterate, previous_extended, target) + weight_zero * trim_extent(initial, initial_margin, target) + rate_prev * interval_increment * prev_rate + rate_zero * interval_increment * trim_extent(initial_derivative, zero_margin, target)

def fastest_characteristic(thermal_state, mass_per_volume, interface_quantities, bulk_motion, ghost_layer_sites):
    interior_block = even_reach(1)
    centred = []
    for direction in range(3):
        centred.append(0.5 * (sites_placed(interface_quantities[direction], ghost_layer_sites, REFERENCE_SPOT, interior_block, interior_block) + sites_placed(interface_quantities[direction], ghost_layer_sites, unit_step(direction, 1), interior_block, interior_block)))
    moving = [sites_placed(bulk_motion[direction], ghost_layer_sites, REFERENCE_SPOT, interior_block, interior_block) for direction in range(3)]
    field_square = centred[0] * centred[0] + centred[1] * centred[1] + centred[2] * centred[2]
    flow_speed = jnp.sqrt(moving[0] * moving[0] + moving[1] * moving[1] + moving[2] * moving[2])
    thermal_energy = sites_placed(thermal_state, ghost_layer_sites, REFERENCE_SPOT, interior_block, interior_block)
    inertia = sites_placed(mass_per_volume, ghost_layer_sites, REFERENCE_SPOT, interior_block, interior_block)
    return flow_speed + jnp.sqrt(GAMMA * thermal_energy + field_square / inertia)

def edge_fields(interface_quantities, face_margin, bulk_motion, ghost_layer_sites, propagation_rate):
    low_side = REFERENCE_SPOT
    high_side = (1, 1, 1)
    fields_out = []
    for edge_axis in range(3):
        first_axis = (edge_axis + 1) % 3
        second_axis = (edge_axis + 2) % 3
        back_first = unit_step(first_axis, -1)
        back_second = unit_step(second_axis, -1)
        back_both = combine_steps(back_first, back_second)

        def corner_mean(source, source_margin):
            return 0.25 * (sites_placed(source, source_margin, REFERENCE_SPOT, low_side, high_side) + sites_placed(source, source_margin, back_first, low_side, high_side) + sites_placed(source, source_margin, back_second, low_side, high_side) + sites_placed(source, source_margin, back_both, low_side, high_side))
        mean_first = corner_mean(bulk_motion[first_axis], ghost_layer_sites)
        mean_second = corner_mean(bulk_motion[second_axis], ghost_layer_sites)
        mean_speed = corner_mean(propagation_rate, 1)
        first_here = sites_placed(interface_quantities[first_axis], face_margin, REFERENCE_SPOT, low_side, high_side)
        first_below = sites_placed(interface_quantities[first_axis], face_margin, back_second, low_side, high_side)
        second_here = sites_placed(interface_quantities[second_axis], face_margin, REFERENCE_SPOT, low_side, high_side)
        second_below = sites_placed(interface_quantities[second_axis], face_margin, back_first, low_side, high_side)
        fields_out.append(mean_second * (0.5 * (first_here + first_below)) - mean_first * (0.5 * (second_here + second_below)) + 0.5 * mean_speed * (second_here - second_below) - 0.5 * mean_speed * (first_here - first_below))
    return fields_out

def edge_cells(source, offset):
    return source[tuple((slice(offset[candidate], offset[candidate] + source.shape[candidate] - 1) for candidate in range(3)))]

def faraday(interface_quantities, face_margin, edges, interval_increment):
    renewed_result = []
    for normal in range(3):
        next_axis = (normal + 1) % 3
        last_axis = (normal + 2) % 3
        curl_part = edge_cells(edges[last_axis], unit_step(next_axis, 1)) - edge_cells(edges[last_axis], REFERENCE_SPOT) - (edge_cells(edges[next_axis], unit_step(last_axis, 1)) - edge_cells(edges[next_axis], REFERENCE_SPOT))
        renewed_result.append(trim_extent(interface_quantities[normal], face_margin, 0) - interval_increment * curl_part)
    return jnp.stack(renewed_result)

def cyclic_wraparound(values, ghost_layer_sites):
    widths = [(0, 0)] * (values.ndim - 3) + [(ghost_layer_sites, ghost_layer_sites)] * 3
    return jnp.pad(values, widths, mode='wrap')

def reference(thermal_state, diffusivity, staggered_flux_density, bulk_motion, mass_per_volume):
    ghost_width = 2
    subdivision_width = 1
    thermal_state_extended = cyclic_wraparound(thermal_state, ghost_width)
    diffusivity_extended = cyclic_wraparound(diffusivity, ghost_width)
    staggered_extended = cyclic_wraparound(staggered_flux_density, ghost_width)
    velocity_extended = cyclic_wraparound(bulk_motion, ghost_width)
    mass_per_volume_extended = cyclic_wraparound(mass_per_volume, ghost_width)
    diffusion_coefficient = diffusivity_extended * jnp.power(thermal_state_extended, 2.5)
    limit_scale = (SECTIONS * SECTIONS + SECTIONS - 2) / 16.0
    interval_increment = jnp.min(limit_scale / trim_extent(diffusion_coefficient, ghost_width, 0))
    propagation_rate = fastest_characteristic(thermal_state_extended, mass_per_volume_extended, staggered_extended, velocity_extended, ghost_width)
    edges_now = edge_fields(staggered_extended, ghost_width, velocity_extended, ghost_width, propagation_rate)
    faces_mid = faraday(staggered_extended, ghost_width, edges_now, interval_increment)
    faces_mid_pad = cyclic_wraparound(faces_mid, 1)
    lookup_arrays = face_coefficients(diffusion_coefficient, staggered_extended, ghost_width, subdivision_width)
    initial_derivative = diffuse_thermal(thermal_state_extended, ghost_width, lookup_arrays, subdivision_width, subdivision_width - 1)
    layout_recipe = section_weights(SECTIONS)
    previous_iterate, previous_extended = (thermal_state_extended, ghost_width)
    newest_iterate = trim_extent(thermal_state_extended, ghost_width, subdivision_width - 1) + layout_recipe[1] * interval_increment * initial_derivative
    newest_extended = subdivision_width - 1
    for subdivision_number in range(2, SECTIONS + 1):
        if newest_extended == 0:
            newest_iterate = cyclic_wraparound(newest_iterate, subdivision_width)
            newest_extended = subdivision_width
        renewed_result = subdivision_advance(layout_recipe[subdivision_number], interval_increment, newest_iterate, newest_extended, previous_iterate, previous_extended, thermal_state_extended, ghost_width, initial_derivative, subdivision_width - 1, lookup_arrays, subdivision_width)
        previous_iterate, previous_extended = (newest_iterate, newest_extended)
        newest_iterate, newest_extended = (renewed_result, newest_extended - 1)
    edges_mid = edge_fields(faces_mid_pad, 1, velocity_extended, ghost_width, propagation_rate)
    faces_end = faraday(faces_mid_pad, 1, edges_mid, interval_increment)
    face_out = 0.5 * (trim_extent(staggered_extended, ghost_width, 0) + faces_end)
    return (newest_iterate, face_out)
```

```python
import functools

import jax
import jax.numpy as jnp
from jax import lax
from jax.experimental import pallas as pl
from jax.experimental.pallas import tpu as pltpu
from jax.sharding import PartitionSpec as P

SECTIONS = 8
GAMMA = 5.0 / 3.0
FACE_FLOOR = 0.25

W = 8
LANES = 128
XE = 3 * W
ROWS = 6 * W
FULL = 5
AUX = 4
AX = 2
XA = W + 2 * AX
SIDE = FULL * W + AUX * AX
TILES = FULL * XE + AUX * XA
PIECES = 16
ZT = -(-TILES // PIECES)
YT = FULL * XE + AUX * XA // 4 + 2 * ZT
FIRST_RATE = 4.0 / (SECTIONS * SECTIONS + SECTIONS - 2)
LIMIT = (SECTIONS * SECTIONS + SECTIONS - 2) / 16.0


def lane_ids(rows):
    return lax.broadcasted_iota(jnp.int32, (rows, LANES), 1)


def lroll(u, amount):
    return pltpu.roll(u, amount % LANES, 1)


def rroll(u, amount):
    return pltpu.roll(u, amount % u.shape[0], 0)


def pack_x(slots, t_ref, d_ref, b_ref, v_ref, r_ref, fwd_ref, bwd_ref, kap_ref, low_ref):
    t = t_ref[...]
    kappa = d_ref[...] * (t * t * jnp.sqrt(t))
    kap_ref[...] = kappa
    low = jnp.min(LIMIT / kappa, axis=0)
    low = jnp.min(jnp.min(low, axis=0, keepdims=True), axis=1, keepdims=True)
    low_ref[...] = jnp.broadcast_to(low.reshape(1, 1, 1), (slots, 1, LANES))
    for ref in (fwd_ref, bwd_ref):
        ref[0:W] = t
        ref[W : 2 * W] = kappa
        for k in range(3):
            ref[(2 + k) * W : (3 + k) * W] = b_ref[k]
    for k in range(AUX):
        at = FULL * W + k * AX
        source = v_ref.at[k] if k < 3 else r_ref
        fwd_ref[at : at + AX] = source[W - AX : W]
        bwd_ref[at : at + AX] = source[0:AX]


def extended_tile(i, lo_ref, hi_ref, own):
    if i < FULL * XE:
        field, plane = divmod(i, XE)
        part, at = divmod(plane, W)
        return (lo_ref, None, hi_ref)[part][field * W + at] if part != 1 else own(field, at)
    field, plane = divmod(i - FULL * XE, XA)
    at = FULL * W + field * AX
    if plane < AX:
        return lo_ref[at + plane]
    if plane < AX + W:
        return own(FULL + field, plane - AX)
    return hi_ref[at + plane - AX - W]


def owner(t_ref, k_ref, b_ref, v_ref, r_ref):
    def own(field, at):
        if field == 0:
            return t_ref[at]
        if field == 1:
            return k_ref[at]
        if field < FULL:
            return b_ref[field - 2, at]
        return v_ref[field - FULL, at] if field < FULL + 3 else r_ref[at]

    return own


def pack_z(lo_ref, hi_ref, t_ref, k_ref, b_ref, v_ref, r_ref, left_ref, right_ref):
    own = owner(t_ref, k_ref, b_ref, v_ref, r_ref)
    lane = lane_ids(W)
    for tile in range(ZT):
        left = jnp.zeros((W, LANES), jnp.float32)
        right = left
        for k in range(PIECES):
            i = tile * PIECES + k
            if i >= TILES:
                break
            u = extended_tile(i, lo_ref, hi_ref, own)
            here = (lane >= 8 * k) & (lane < 8 * k + 8)
            left = jnp.where(here, lroll(u, 8 * k), left)
            right = jnp.where(here, lroll(u, 8 * k - (LANES - 8)), right)
        left_ref[tile] = left
        right_ref[tile] = right


def pack_y(lo_ref, hi_ref, t_ref, k_ref, b_ref, v_ref, r_ref, gl_ref, gr_ref, fwd_ref, bwd_ref):
    own = owner(t_ref, k_ref, b_ref, v_ref, r_ref)
    for i in range(FULL * XE):
        u = extended_tile(i, lo_ref, hi_ref, own)
        fwd_ref[i] = u
        bwd_ref[i] = u
    for i in range(AUX * XA):
        u = extended_tile(FULL * XE + i, lo_ref, hi_ref, own)
        tile, k = FULL * XE + i // 4, i % 4
        fwd_ref[tile, AX * k : AX * k + AX] = u[W - AX : W]
        bwd_ref[tile, AX * k : AX * k + AX] = u[0:AX]
    at = YT - 2 * ZT
    for ref in (fwd_ref, bwd_ref):
        ref[at : at + ZT] = gl_ref[...]
        ref[at + ZT : at + 2 * ZT] = gr_ref[...]


def strips(u, left, right, k, lane):
    inner = jnp.where(lane < 32, lroll(u, 8), lroll(u, 32 - (LANES - 16)))
    edge = jnp.where(lane < 8, lroll(left, -8 * k), lroll(right, 48 - 8 * k))
    return jnp.where((lane < 8) | (lane >= 48), edge, inner)


def advance(
    lo_ref,
    hi_ref,
    t_ref,
    k_ref,
    b_ref,
    v_ref,
    r_ref,
    gl_ref,
    gr_ref,
    ly_ref,
    hy_ref,
    low_ref,
    tout_ref,
    bout_ref,
    full,
    aux,
    coef,
    qa,
    qb,
    ecoef,
    edge,
    mid,
):
    own = owner(t_ref, k_ref, b_ref, v_ref, r_ref)
    lane = lane_ids(W)
    dt = jnp.min(jnp.min(low_ref[...], axis=0), axis=1, keepdims=True)

    at = YT - 2 * ZT
    for i in range(TILES):
        tile, k = divmod(i, PIECES)
        u = extended_tile(i, lo_ref, hi_ref, own)
        mine = (u, gl_ref[tile], gr_ref[tile])
        sides = []
        for ref, row in ((ly_ref, W - AX), (hy_ref, 0)):
            if i < FULL * XE:
                side = ref[i]
            else:
                j = i - FULL * XE
                rows = ref[FULL * XE + j // 4, AX * (j % 4) : AX * (j % 4) + AX]
                side = jnp.concatenate([rows] * 4, axis=0)
            sides.append((side, ref[at + tile], ref[at + ZT + tile]))
        for part, (u, left, right) in enumerate((sides[0], mine, sides[1])):
            s = strips(u, left, right, k, lane)
            if i < FULL * XE:
                field, plane = divmod(i, XE)
                full[field, plane, part * W : part * W + W] = u
                full[field, plane, 3 * W + part * W : 3 * W + part * W + W] = s
            else:
                field, plane = divmod(i - FULL * XE, XA)
                aux[field, plane, part * W : part * W + W] = u
                aux[field, plane, 3 * W + part * W : 3 * W + part * W + W] = s

    def sums(x):
        bx, by, bz = full[2, x], full[3, x], full[4, x]
        sx = bx + full[2, jnp.minimum(x + 1, XE - 1)]
        sy = by + rroll(by, -1)
        sz = bz + lroll(bz, -1)
        return bx, by, bz, sx, sy, sz

    def face(n, x, kk, bn, b1, b2):
        b1, b2 = 0.25 * b1, 0.25 * b2
        q = bn * bn + b1 * b1 + b2 * b2
        s = (0.5 * FIRST_RATE * dt) * kk / jnp.maximum(q, FACE_FLOOR) * bn
        coef[3 * n, x] = s * bn
        coef[3 * n + 1, x] = 0.25 * (s * b1)
        coef[3 * n + 2, x] = 0.25 * (s * b2)

    def faces(x, carry):
        k_m, sy_m, sz_m = carry
        kap = full[1, x]
        bx, by, bz, sx, sy, sz = sums(x)
        face(0, x, kap + k_m, bx, sy + sy_m, sz + sz_m)
        face(1, x, kap + rroll(kap, 1), by, sz + rroll(sz, 1), sx + rroll(sx, 1))
        face(2, x, kap + lroll(kap, 1), bz, sx + lroll(sx, 1), sy + lroll(sy, 1))
        return kap, sy, sz

    _, _, _, _, sy, sz = sums(0)
    lax.fori_loop(1, XE, faces, (full[1, 0], sy, sz))

    source, older = full.at[0], None
    for j in range(1, SECTIONS + 1):
        target = qa if j % 2 else qb
        grow = (2.0 * j - 1.0) / j
        back = (j - 1.0) / j

        def slopes(u):
            return rroll(u, -1) - rroll(u, 1), lroll(u, -1) - lroll(u, 1)

        def flux_x(x, u, u_m, dy, dy_m, dz, dz_m):
            return coef[0, x] * (u - u_m) + coef[1, x] * (dy + dy_m) + coef[2, x] * (dz + dz_m)

        def plane(x, carry, source=source, older=older, target=target, grow=grow, back=back, j=j):
            u_m, u, dy, dz, fx = carry
            u_p = source[x + 1]
            dy_p, dz_p = slopes(u_p)
            fx_p = flux_x(x + 1, u_p, u, dy_p, dy, dz_p, dz)
            dx = u_p - u_m
            fy = (
                coef[3, x] * (u - rroll(u, 1))
                + coef[4, x] * (dz + rroll(dz, 1))
                + coef[5, x] * (dx + rroll(dx, 1))
            )
            fz = (
                coef[6, x] * (u - lroll(u, 1))
                + coef[7, x] * (dx + lroll(dx, 1))
                + coef[8, x] * (dy + lroll(dy, 1))
            )
            rate = (fx_p - fx) + (rroll(fy, -1) - fy) + (lroll(fz, -1) - fz)
            new = u + rate
            if j > 1:
                new = grow * new - back * older[x]
            if j == SECTIONS:
                b = (SECTIONS * SECTIONS + SECTIONS - 2) / (2.0 * SECTIONS * (SECTIONS + 1))
                new = (1.0 - b) * full[0, x] + b * new
            target[x] = new
            return u, u_p, dy_p, dz_p, fx_p

        u_m, u = source[j - 1], source[j]
        dy_m, dz_m = slopes(u_m)
        dy, dz = slopes(u)
        fx = flux_x(j, u, u_m, dy, dy_m, dz, dz_m)
        lax.fori_loop(j, XE - j, plane, (u_m, u, dy, dz, fx))
        source, older = target, source

    def seam(main, strip):
        high = lroll(strip, LANES - 8 - 40)
        return jnp.where(lane < 8, lroll(strip, -8), jnp.where(lane >= LANES - 8, high, main))

    for x in range(W):
        tout_ref[x] = seam(source[W + x, W : 2 * W], source[W + x, 4 * W : 5 * W])

    off = W - AX
    SPEED = 3

    def speed(i, carry):
        x = i + off
        bx, by, bz, sx, sy, sz = sums(x)
        field = 0.25 * (sx * sx + sy * sy + sz * sz)
        vx, vy, vz = aux[0, i], aux[1, i], aux[2, i]
        flow = jnp.sqrt(vx * vx + vy * vy + vz * vz)
        aux[SPEED, i] = flow + jnp.sqrt(GAMMA * full[0, x] + field / aux[SPEED, i])
        return carry

    lax.fori_loop(0, XA, speed, 0)

    def by_axis(u, u_m, axis):
        if axis == 0:
            return u_m
        return rroll(u, 1) if axis == 1 else lroll(u, 1)

    def edges(i, carry):
        for c in range(3):
            a, b = (c + 1) % 3, (c + 2) % 3

            def mean(f):
                if 0 in (a, b):
                    other = a + b
                    u = aux[f, i] + aux[f, i - 1]
                else:
                    other = 2
                    u = aux[f, i]
                    u = u + by_axis(u, None, 1)
                return 0.125 * (u + by_axis(u, None, other))

            va, vb, s = mean(a), mean(b), mean(SPEED)
            ecoef[4 * c, i] = vb - s
            ecoef[4 * c + 1, i] = vb + s
            ecoef[4 * c + 2, i] = s - va
            ecoef[4 * c + 3, i] = -s - va
        return carry

    lax.fori_loop(1, XA, edges, 0)

    def fields(get, first, last):
        def body(i, carry):
            for c in range(3):
                a, b = (c + 1) % 3, (c + 2) % 3
                ua, ub = get(a, i), get(b, i)
                ua_b = by_axis(ua, get(a, i - 1) if b == 0 else None, b)
                ub_a = by_axis(ub, get(b, i - 1) if a == 0 else None, a)
                edge[c, i] = (ecoef[4 * c, i] * ua + ecoef[4 * c + 1, i] * ua_b) + (
                    ecoef[4 * c + 2, i] * ub + ecoef[4 * c + 3, i] * ub_a
                )
            return carry

        lax.fori_loop(first, last, body, 0)

    def ahead(f, i, axis):
        if axis == 0:
            return edge[f, i + 1]
        u = edge[f, i]
        return rroll(u, -1) if axis == 1 else lroll(u, -1)

    def curl(d, i):
        e, f = (d + 1) % 3, (d + 2) % 3
        return (ahead(f, i, e) - edge[f, i]) - (ahead(e, i, f) - edge[e, i])

    fields(lambda d, i: full[2 + d, i + off], 1, XA)

    def middle(i, carry):
        for d in range(3):
            mid[d, i] = full[2 + d, i + off] - dt * curl(d, i)
        return carry

    lax.fori_loop(1, XA - 1, middle, 0)
    fields(lambda d, i: mid[d, i], 2, XA - 1)

    def last(i, carry):
        for d in range(3):
            u = 0.5 * (full[2 + d, i + off] + (mid[d, i] - dt * curl(d, i)))
            bout_ref[d, i - AX] = seam(u[W : 2 * W], u[4 * W : 5 * W])
        return carry

    lax.fori_loop(AX, AX + W, last, 0)


def exchange(low_going, high_going, axis):
    count = lax.axis_size(axis)
    forward = [(i, (i + 1) % count) for i in range(count)]
    backward = [(target, source) for source, target in forward]
    from_low = lax.ppermute(high_going, axis, forward)
    from_high = lax.ppermute(low_going, axis, backward)
    return from_low, from_high


def f32(*shape):
    return jax.ShapeDtypeStruct(shape, jnp.float32)


def on_device(t, diffusivity, b, v, rho):
    yz = lax.axis_size("gy") * lax.axis_size("gz")
    xs = lax.axis_size("gx")
    fwd, bwd, kappa, low = pl.pallas_call(
        functools.partial(pack_x, yz),
        out_shape=(f32(SIDE, W, LANES), f32(SIDE, W, LANES), f32(W, W, LANES), f32(yz, 1, LANES)),
        name="pack_x",
    )(t, diffusivity, b, v, rho)
    from_lo, from_hi = exchange(bwd, fwd, "gx")
    low = lax.all_to_all(low, ("gy", "gz"), 0, 0, tiled=True)
    low = jnp.broadcast_to(jnp.min(low, axis=0, keepdims=True), (xs, 1, LANES))
    own = (t, kappa, b, v, rho)
    left, right = pl.pallas_call(
        pack_z,
        out_shape=(f32(ZT, W, LANES), f32(ZT, W, LANES)),
        name="pack_z",
    )(from_lo, from_hi, *own)
    g_left, g_right = exchange(left, right, "gz")
    fwd, bwd = pl.pallas_call(
        pack_y,
        out_shape=(f32(YT, W, LANES), f32(YT, W, LANES)),
        name="pack_y",
    )(from_lo, from_hi, *own, g_left, g_right)
    y_lo, y_hi = exchange(bwd, fwd, "gy")
    low = lax.all_to_all(low, "gx", 0, 0, tiled=True)
    scratch = [
        pltpu.VMEM((FULL, XE, ROWS, LANES), jnp.float32),
        pltpu.VMEM((AUX, XA, ROWS, LANES), jnp.float32),
        pltpu.VMEM((9, XE, ROWS, LANES), jnp.float32),
        pltpu.VMEM((XE, ROWS, LANES), jnp.float32),
        pltpu.VMEM((XE, ROWS, LANES), jnp.float32),
        pltpu.VMEM((12, XA, ROWS, LANES), jnp.float32),
        pltpu.VMEM((3, XA, ROWS, LANES), jnp.float32),
        pltpu.VMEM((3, XA, ROWS, LANES), jnp.float32),
    ]
    return pl.pallas_call(
        advance,
        out_shape=(f32(W, W, LANES), f32(3, W, W, LANES)),
        scratch_shapes=scratch,
        name="advance",
    )(from_lo, from_hi, *own, g_left, g_right, y_lo, y_hi, low)


def solution(mesh):
    cell = P("gx", "gy", "gz")
    face = P(None, "gx", "gy", "gz")
    return jax.shard_map(
        on_device,
        mesh=mesh,
        in_specs=(cell, cell, face, face, cell),
        out_specs=(cell, face),
        check_vma=False,
    )
```

```python
import jax
import jax.numpy as jnp
from jax import lax
from jax.experimental import pallas as pl
from jax.experimental.pallas import tpu as pltpu
from jax.sharding import PartitionSpec as P

SECTIONS = 8
GAMMA = 5.0 / 3.0
FACE_FLOOR = 0.25

W = 8
LANES = 128
XE = 3 * W
ROWS = 6 * W
FULL = 5
AUX = 4
AX = 2
XA = W + 2 * AX
PIECES = 16
ZT = (FULL + AUX) * W // PIECES + 1
SPARE = LANES // 2
SIDE = FULL * W + AUX * AX + 2 * ZT
YT = FULL * XE + AUX * XA // 4 + 6 * ZT
FIRST_RATE = 4.0 / (SECTIONS * SECTIONS + SECTIONS - 2)
LIMIT = (SECTIONS * SECTIONS + SECTIONS - 2) / 16.0


def lane_ids(rows):
    return lax.broadcasted_iota(jnp.int32, (rows, LANES), 1)


def lroll(u, amount):
    return pltpu.roll(u, amount % LANES, 1)


def rroll(u, amount):
    return pltpu.roll(u, amount % u.shape[0], 0)


def lowest(u):
    return jnp.min(jnp.min(u, axis=0, keepdims=True), axis=1, keepdims=True)


def neighbours(axis):
    count = lax.axis_size(axis)
    at = lax.axis_index(axis)
    return lax.rem(at + count - 1, count), lax.rem(at + 1, count)


def is_odd(axis):
    return lax.rem(lax.axis_index(axis), 2) == 1


def piece(field, plane):
    return divmod(field * W + plane, PIECES)


def pack_z(t_ref, d_ref, b_ref, v_ref, r_ref, kap_ref, out_ref):
    t = t_ref[...]
    kappa = d_ref[...] * (t * t * jnp.sqrt(t))
    kap_ref[...] = kappa
    low = lowest(jnp.min(LIMIT / kappa, axis=0))
    lane = lane_ids(W)
    left, right = [], []
    for tile in range(ZT):
        below = above = jnp.broadcast_to(low, (W, LANES))
        for k in range(PIECES):
            field, plane = divmod(tile * PIECES + k, W)
            if field >= FULL + AUX:
                break
            if field == 0:
                u = t[plane]
            elif field == 1:
                u = kappa[plane]
            elif field < FULL:
                u = b_ref[field - 2, plane]
            else:
                u = v_ref[field - FULL, plane] if field < FULL + 3 else r_ref[plane]
            here = (lane >= 8 * k) & (lane < 8 * k + 8)
            below = jnp.where(here, lroll(u, 8 * k), below)
            above = jnp.where(here, lroll(u, 8 * k - (LANES - 8)), above)
        left.append(below)
        right.append(above)
    lo, _ = neighbours("gz")
    for slot in range(out_ref.shape[0]):
        for tile in range(ZT):
            out_ref[slot, tile] = jnp.where(lo == slot, left[tile], right[tile])


def pack_x(t_ref, k_ref, b_ref, v_ref, r_ref, z_ref, a_ref, o_ref, low_ref):
    odd = is_odd("gx")
    for ref in (a_ref, o_ref):
        ref[0:W] = t_ref[...]
        ref[W : 2 * W] = k_ref[...]
        for k in range(3):
            ref[(2 + k) * W : (3 + k) * W] = b_ref[k]
    for k in range(AUX):
        at = FULL * W + k * AX
        source = v_ref.at[k] if k < 3 else r_ref
        up, down = source[W - AX : W], source[0:AX]
        a_ref[at : at + AX] = jnp.where(odd, down, up)
        o_ref[at : at + AX] = jnp.where(odd, up, down)
    lo, hi = neighbours("gz")
    at = SIDE - 2 * ZT
    for tile in range(ZT):
        left, right = z_ref[lo, tile], z_ref[hi, tile]
        for ref in (a_ref, o_ref):
            ref[at + tile] = left
            ref[at + ZT + tile] = right
    low = z_ref[0, ZT - 1]
    for slot in range(1, z_ref.shape[0]):
        low = jnp.minimum(low, z_ref[slot, ZT - 1])
    low = lowest(jnp.where(lane_ids(W) >= SPARE, low, jnp.max(low)))
    low_ref[...] = jnp.broadcast_to(low.reshape(1, 1, 1), low_ref.shape)


def pack_y(own_ref, v_ref, r_ref, xa_ref, xo_ref, gy_ref, a_ref, o_ref, aux_ref, low_ref):
    odd_x, odd_y = is_odd("gx"), is_odd("gy")

    def below(i):
        return jnp.where(odd_x, xa_ref[i], xo_ref[i])

    def above(i):
        return jnp.where(odd_x, xo_ref[i], xa_ref[i])

    for field in range(FULL):
        for plane in range(W):
            i = field * W + plane
            for part, u in enumerate((below(i), own_ref[i], above(i))):
                a_ref[field * XE + part * W + plane] = u
                o_ref[field * XE + part * W + plane] = u
    for field in range(AUX):
        for plane in range(XA):
            at = FULL * W + field * AX + plane
            if plane < AX:
                u = below(at)
            elif plane < AX + W:
                u = v_ref[field, plane - AX] if field < 3 else r_ref[plane - AX]
            else:
                u = above(at - AX - W)
            i = field * XA + plane
            aux_ref[i] = u
            tile, k = FULL * XE + i // 4, i % 4
            up, down = u[W - AX : W], u[0:AX]
            a_ref[tile, AX * k : AX * k + AX] = jnp.where(odd_y, down, up)
            o_ref[tile, AX * k : AX * k + AX] = jnp.where(odd_y, up, down)
    at = SIDE - 2 * ZT
    for i in range(2 * ZT):
        for part, u in enumerate((below(at + i), own_ref[at + i], above(at + i))):
            a_ref[YT - (6 - 2 * part) * ZT + i] = u
            o_ref[YT - (6 - 2 * part) * ZT + i] = u
    low = lowest(jnp.min(gy_ref[...], axis=0))
    low_ref[...] = jnp.broadcast_to(low.reshape(1, 1, 1), low_ref.shape)


def strips(u, left, right, k, lane):
    inner = jnp.where(lane < 32, lroll(u, 8), lroll(u, 32 - (LANES - 16)))
    edge = jnp.where(lane < 8, lroll(left, -8 * k), lroll(right, 48 - 8 * k))
    return jnp.where((lane < 8) | (lane >= 48), edge, inner)


def sweep(first, last, body, carry, by):
    trips = (last - first) // by

    def several(i, carry):
        for k in range(by):
            carry = body(first + i * by + k, carry)
        return carry

    if trips:
        carry = lax.fori_loop(0, trips, several, carry)
    for x in range(first + trips * by, last):
        carry = body(x, carry)
    return carry


def advance(
    own_ref, aux_ref, ya_ref, yo_ref, low_ref, tout_ref, bout_ref,
    us, full, aux, coef, ecoef, edge, mid,
):
    lane = lane_ids(W)
    dt = lowest(jnp.min(low_ref[...], axis=0))
    odd = is_odd("gy")

    def below(i):
        return jnp.where(odd, ya_ref[i], yo_ref[i])

    def above(i):
        return jnp.where(odd, yo_ref[i], ya_ref[i])

    def lay(put, field, plane, x, parts):
        part_x, at = divmod(x, W)
        tile, k = piece(field, at)
        z = YT - (6 - 2 * part_x) * ZT + tile
        for part, (u, get) in enumerate(zip(parts, (below, own_ref.__getitem__, above))):
            put(plane, part * W, u)
            put(plane, 3 * W + part * W, strips(u, get(z), get(z + ZT), k, lane))

    def put_field(field):
        def put(x, row, u):
            if field == 0:
                us[0, 0, x, row : row + W] = u
            else:
                full[field - 1, x, row : row + W] = u

        return put

    def put_aux(field):
        def put(i, row, u):
            aux[field, i, row : row + W] = u

        return put

    off = W - AX
    for field in range(FULL):
        for x in range(XE):
            i = field * XE + x
            lay(put_field(field), field, x, x, (below(i), own_ref[i], above(i)))
    for field in range(AUX):
        for plane in range(XA):
            i = field * XA + plane
            tile, k = FULL * XE + i // 4, i % 4

            def spread(get, k=k, tile=tile):
                return get(tile)[AX * k : AX * k + AX]

            lo = jnp.concatenate([spread(below)] * 4, axis=0)
            hi = jnp.concatenate([spread(above)] * 4, axis=0)
            lay(put_aux(field), FULL + field, plane, plane + off, (lo, aux_ref[i], hi))

    def sums(x, x_p):
        bx, by, bz = full[1, x], full[2, x], full[3, x]
        sx = bx + full[1, x_p]
        sy = by + rroll(by, -1)
        sz = bz + lroll(bz, -1)
        return bx, by, bz, sx, sy, sz

    def face(n, x, kk, bn, b1, b2):
        b1, b2 = 0.25 * b1, 0.25 * b2
        q = bn * bn + b1 * b1 + b2 * b2
        s = (0.5 * FIRST_RATE * dt) * kk / jnp.maximum(q, FACE_FLOOR) * bn
        coef[3 * n, x] = s * bn
        coef[3 * n + 1, x] = 0.25 * (s * b1)
        coef[3 * n + 2, x] = 0.25 * (s * b2)

    def faces(x, carry):
        k_m, sy_m, sz_m = carry
        kap = full[0, x]
        u = us[0, 0, x]
        us[0, 1, x] = lroll(u, -1)
        us[0, 2, x] = lroll(u, 1)
        x_p = jnp.minimum(x + 1, XE - 1)
        bx, by, bz, sx, sy, sz = sums(x, x_p)
        face(0, x, kap + k_m, bx, sy + sy_m, sz + sz_m)
        face(1, x, kap + rroll(kap, 1), by, sz + rroll(sz, 1), sx + rroll(sx, 1))
        face(2, x, kap + lroll(kap, 1), bz, sx + lroll(sx, 1), sy + lroll(sy, 1))
        return kap, sy, sz

    _, _, _, _, sy, sz = sums(0, 1)
    sweep(0, XE, faces, (full[0, 0], sy, sz), 2)

    def upper(x, carry):
        for k in range(3):
            coef[9 + k, x] = lroll(coef[6 + k, x], -1)
        return carry

    sweep(1, XE - 1, upper, 0, 4)

    source, older = us.at[0], None
    for j in range(1, SECTIONS + 1):
        target = us.at[2 - j % 2]
        grow = (2.0 * j - 1.0) / j
        back = (j - 1.0) / j

        def rolled(u, u_p, u_m):
            down = rroll(u, 1)
            return down, rroll(u, -1) - down, u_p - u_m

        def flux_x(x, du, sum_y, sum_z):
            return coef[0, x] * du + coef[1, x] * sum_y + coef[2, x] * sum_z

        def plane(x, carry, source=source, older=older, target=target, grow=grow, back=back, j=j):
            dy, dz, fx, down, new = carry
            if j < SECTIONS:
                target[1, x - 1] = lroll(new, -1)
                target[2, x - 1] = lroll(new, 1)
            u, p, m = source[0, x], source[1, x], source[2, x]
            u_p, p_p, m_p = source[0, x + 1], source[1, x + 1], source[2, x + 1]
            down_p, dy_p, dz_p = rolled(u_p, p_p, m_p)
            fx_p = flux_x(x + 1, u_p - u, dy_p + dy, dz_p + dz)
            dx = u_p - source[0, x - 1]
            dx_zp = p_p - source[1, x - 1]
            dx_zm = m_p - source[2, x - 1]
            p_down, m_down = rroll(p, 1), rroll(m, 1)
            dy_zp = rroll(p, -1) - p_down
            dy_zm = rroll(m, -1) - m_down
            fy = (
                coef[3, x] * (u - down)
                + coef[4, x] * (dz + (p_down - m_down))
                + coef[5, x] * (dx + rroll(dx, 1))
            )
            fz = coef[6, x] * (u - m) + coef[7, x] * (dx + dx_zm) + coef[8, x] * (dy + dy_zm)
            fz_p = coef[9, x] * (p - u) + coef[10, x] * (dx_zp + dx) + coef[11, x] * (dy_zp + dy)
            rate = (fx_p - fx) + (rroll(fy, -1) - fy) + (fz_p - fz)
            new = u + rate
            if j > 1:
                new = grow * new - back * older[0, x]
            if j == SECTIONS:
                b = (SECTIONS * SECTIONS + SECTIONS - 2) / (2.0 * SECTIONS * (SECTIONS + 1))
                new = (1.0 - b) * us[0, 0, x] + b * new
            target[0, x] = new
            return dy_p, dz_p, fx_p, down_p, new

        u_m, u = source[0, j - 1], source[0, j]
        _, dy_m, dz_m = rolled(u_m, source[1, j - 1], source[2, j - 1])
        down, dy, dz = rolled(u, source[1, j], source[2, j])
        fx = flux_x(j, u - u_m, dy + dy_m, dz + dz_m)
        *_, new = sweep(j, XE - j, plane, (dy, dz, fx, down, u), 2)
        if j < SECTIONS:
            target[1, XE - j - 1] = lroll(new, -1)
            target[2, XE - j - 1] = lroll(new, 1)
        source, older = target, source

    def seam(main, strip):
        high = lroll(strip, LANES - 8 - 40)
        return jnp.where(lane < 8, lroll(strip, -8), jnp.where(lane >= LANES - 8, high, main))

    for x in range(W):
        tout_ref[x] = seam(source[0, W + x, W : 2 * W], source[0, W + x, 4 * W : 5 * W])

    SPEED = 3
    for i in range(XA):
        x = i + off
        _, _, _, sx, sy, sz = sums(x, x + 1)
        field = 0.25 * (sx * sx + sy * sy + sz * sz)
        vx, vy, vz = aux[0, i], aux[1, i], aux[2, i]
        flow = jnp.sqrt(vx * vx + vy * vy + vz * vz)
        aux[SPEED, i] = flow + jnp.sqrt(GAMMA * us[0, 0, x] + field / aux[SPEED, i])

    def by_axis(u, u_m, axis):
        if axis == 0:
            return u_m
        return rroll(u, 1) if axis == 1 else lroll(u, 1)

    for i in range(1, XA):
        for c in range(3):
            a, b = (c + 1) % 3, (c + 2) % 3

            def mean(f, i=i, a=a, b=b):
                if 0 in (a, b):
                    other = a + b
                    u = aux[f, i] + aux[f, i - 1]
                else:
                    other = 2
                    u = aux[f, i]
                    u = u + by_axis(u, None, 1)
                return 0.125 * (u + by_axis(u, None, other))

            va, vb, s = mean(a), mean(b), mean(SPEED)
            ecoef[4 * c, i] = vb - s
            ecoef[4 * c + 1, i] = vb + s
            ecoef[4 * c + 2, i] = s - va
            ecoef[4 * c + 3, i] = -s - va

    def fields(get, first, last):
        for i in range(first, last):
            for c in range(3):
                a, b = (c + 1) % 3, (c + 2) % 3
                ua, ub = get(a, i), get(b, i)
                ua_b = by_axis(ua, get(a, i - 1) if b == 0 else None, b)
                ub_a = by_axis(ub, get(b, i - 1) if a == 0 else None, a)
                edge[c, i] = (ecoef[4 * c, i] * ua + ecoef[4 * c + 1, i] * ua_b) + (
                    ecoef[4 * c + 2, i] * ub + ecoef[4 * c + 3, i] * ub_a
                )

    def ahead(f, i, axis):
        if axis == 0:
            return edge[f, i + 1]
        u = edge[f, i]
        return rroll(u, -1) if axis == 1 else lroll(u, -1)

    def curl(d, i):
        e, f = (d + 1) % 3, (d + 2) % 3
        return (ahead(f, i, e) - edge[f, i]) - (ahead(e, i, f) - edge[e, i])

    fields(lambda d, i: full[1 + d, i + off], 1, XA)
    for i in range(1, XA - 1):
        for d in range(3):
            mid[d, i] = full[1 + d, i + off] - dt * curl(d, i)
    fields(lambda d, i: mid[d, i], 2, XA - 1)
    for i in range(AX, AX + W):
        for d in range(3):
            u = 0.5 * (full[1 + d, i + off] + (mid[d, i] - dt * curl(d, i)))
            bout_ref[d, i - AX] = seam(u[W : 2 * W], u[4 * W : 5 * W])


def exchange(first, second, axis):
    count = lax.axis_size(axis)
    swaps = [(i, i + 1) for i in range(0, count, 2)] + [(i + 1, i) for i in range(0, count, 2)]
    others = [((a + 1) % count, (b + 1) % count) for a, b in swaps]
    return lax.ppermute(first, axis, swaps), lax.ppermute(second, axis, others)


def f32(*shape):
    return jax.ShapeDtypeStruct(shape, jnp.float32)


def on_core(kernel, out, *args, scratch=()):
    space = pl.BlockSpec(memory_space=pltpu.VMEM)
    return pl.pallas_call(
        kernel,
        out_shape=out,
        in_specs=[space] * len(args),
        out_specs=(space,) * len(out),
        scratch_shapes=[pltpu.VMEM(shape, jnp.float32) for shape in scratch],
        name=kernel.__name__,
    )(*args)


def on_device(t, diffusivity, b, v, rho):
    xs, ys, zs = (lax.axis_size(axis) for axis in ("gx", "gy", "gz"))
    out = (f32(W, W, LANES), f32(zs, ZT, W, LANES))
    kappa, edges = on_core(pack_z, out, t, diffusivity, b, v, rho)
    edges = lax.all_to_all(edges, "gz", 0, 0, tiled=True)
    out = (f32(SIDE, W, LANES), f32(SIDE, W, LANES), f32(ys, 1, LANES))
    first, second, low = on_core(pack_x, out, t, kappa, b, v, rho, edges)
    x_first, x_second = exchange(first, second, "gx")
    low = lax.all_to_all(low, "gy", 0, 0, tiled=True)
    out = (f32(YT, W, LANES), f32(YT, W, LANES), f32(AUX * XA, W, LANES), f32(xs, 1, LANES))
    first, second, aux, low = on_core(pack_y, out, first, v, rho, x_first, x_second, low)
    y_first, y_second = exchange(first, second, "gy")
    low = lax.all_to_all(low, "gx", 0, 0, tiled=True)
    scratch = [
        (3, 3, XE, ROWS, LANES),
        (FULL - 1, XE, ROWS, LANES),
        (AUX, XA, ROWS, LANES),
        (12, XE, ROWS, LANES),
        (12, XA, ROWS, LANES),
        (3, XA, ROWS, LANES),
        (3, XA, ROWS, LANES),
    ]
    out = (f32(W, W, LANES), f32(3, W, W, LANES))
    return on_core(advance, out, first, aux, y_first, y_second, low, scratch=scratch)


def solution(mesh):
    cell = P("gx", "gy", "gz")
    face = P(None, "gx", "gy", "gz")
    return jax.shard_map(
        on_device,
        mesh=mesh,
        in_specs=(cell, cell, face, face, cell),
        out_specs=(cell, face),
        check_vma=False,
    )
```

```python
import jax
import jax.numpy as jnp
from jax import lax
from jax.experimental import pallas as pl
from jax.experimental.pallas import tpu as pltpu
from jax.sharding import Mesh
from jax.sharding import PartitionSpec as P

SECTIONS = 8
GAMMA = 5.0 / 3.0
FACE_FLOOR = 0.25

GX = ("gx_0", "gx_1", "gx_2")
W = 8
LANES = 128
XE = 3 * W
ROWS = 6 * W
FULL = 5
AUX = 4
AX = 2
XA = W + 2 * AX
PIECES = 16
ZT = (FULL + AUX) * W // PIECES + 1
SPARE = LANES // 2
SIDE = FULL * W + AUX * AX + 2 * ZT
YT = FULL * XE + AUX * XA // 4 + 6 * ZT
FIRST_RATE = 4.0 / (SECTIONS * SECTIONS + SECTIONS - 2)
LIMIT = (SECTIONS * SECTIONS + SECTIONS - 2) / 16.0


def lane_ids(rows):
    return lax.broadcasted_iota(jnp.int32, (rows, LANES), 1)


def lroll(u, amount):
    return pltpu.roll(u, amount % LANES, 1)


def rroll(u, amount):
    return pltpu.roll(u, amount % u.shape[0], 0)


def lowest(u):
    return jnp.min(jnp.min(u, axis=0, keepdims=True), axis=1, keepdims=True)


def neighbours(axis):
    count = lax.axis_size(axis)
    at = lax.axis_index(axis)
    return lax.rem(at + count - 1, count), lax.rem(at + 1, count)


def is_odd(axis):
    return lax.rem(lax.axis_index(axis), 2) == 1


def piece(field, plane):
    return divmod(field * W + plane, PIECES)


def pack_z(t_ref, d_ref, b_ref, v_ref, r_ref, kap_ref, out_ref):
    t = t_ref[...]
    kappa = d_ref[...] * (t * t * jnp.sqrt(t))
    kap_ref[...] = kappa
    low = lowest(jnp.min(LIMIT / kappa, axis=0))
    lane = lane_ids(W)
    left, right = [], []
    for tile in range(ZT):
        below = above = jnp.broadcast_to(low, (W, LANES))
        for k in range(PIECES):
            field, plane = divmod(tile * PIECES + k, W)
            if field >= FULL + AUX:
                break
            if field == 0:
                u = t[plane]
            elif field == 1:
                u = kappa[plane]
            elif field < FULL:
                u = b_ref[field - 2, plane]
            else:
                u = v_ref[field - FULL, plane] if field < FULL + 3 else r_ref[plane]
            here = (lane >= 8 * k) & (lane < 8 * k + 8)
            below = jnp.where(here, lroll(u, 8 * k), below)
            above = jnp.where(here, lroll(u, 8 * k - (LANES - 8)), above)
        left.append(below)
        right.append(above)
    lo, _ = neighbours("gz")
    for slot in range(out_ref.shape[0]):
        for tile in range(ZT):
            out_ref[slot, tile] = jnp.where(lo == slot, left[tile], right[tile])


def pack_x(t_ref, k_ref, b_ref, v_ref, r_ref, z_ref, a_ref, o_ref, low_ref):
    odd = is_odd(GX)
    for ref in (a_ref, o_ref):
        ref[0:W] = t_ref[...]
        ref[W : 2 * W] = k_ref[...]
        for k in range(3):
            ref[(2 + k) * W : (3 + k) * W] = b_ref[k]
    for k in range(AUX):
        at = FULL * W + k * AX
        source = v_ref.at[k] if k < 3 else r_ref
        up, down = source[W - AX : W], source[0:AX]
        a_ref[at : at + AX] = jnp.where(odd, down, up)
        o_ref[at : at + AX] = jnp.where(odd, up, down)
    lo, hi = neighbours("gz")
    at = SIDE - 2 * ZT
    for tile in range(ZT):
        left, right = z_ref[lo, tile], z_ref[hi, tile]
        for ref in (a_ref, o_ref):
            ref[at + tile] = left
            ref[at + ZT + tile] = right
    low = z_ref[0, ZT - 1]
    for slot in range(1, z_ref.shape[0]):
        low = jnp.minimum(low, z_ref[slot, ZT - 1])
    low = lowest(jnp.where(lane_ids(W) >= SPARE, low, jnp.max(low)))
    low_ref[...] = jnp.broadcast_to(low.reshape(1, 1, 1), low_ref.shape)


def pack_y(own_ref, v_ref, r_ref, xa_ref, xo_ref, gy_ref, a_ref, o_ref, aux_ref, low_ref):
    odd_x, odd_y = is_odd(GX), is_odd("gy")

    def below(i):
        return jnp.where(odd_x, xa_ref[i], xo_ref[i])

    def above(i):
        return jnp.where(odd_x, xo_ref[i], xa_ref[i])

    for field in range(FULL):
        for plane in range(W):
            i = field * W + plane
            for part, u in enumerate((below(i), own_ref[i], above(i))):
                a_ref[field * XE + part * W + plane] = u
                o_ref[field * XE + part * W + plane] = u
    for field in range(AUX):
        for plane in range(XA):
            at = FULL * W + field * AX + plane
            if plane < AX:
                u = below(at)
            elif plane < AX + W:
                u = v_ref[field, plane - AX] if field < 3 else r_ref[plane - AX]
            else:
                u = above(at - AX - W)
            i = field * XA + plane
            aux_ref[i] = u
            tile, k = FULL * XE + i // 4, i % 4
            up, down = u[W - AX : W], u[0:AX]
            a_ref[tile, AX * k : AX * k + AX] = jnp.where(odd_y, down, up)
            o_ref[tile, AX * k : AX * k + AX] = jnp.where(odd_y, up, down)
    at = SIDE - 2 * ZT
    for i in range(2 * ZT):
        for part, u in enumerate((below(at + i), own_ref[at + i], above(at + i))):
            a_ref[YT - (6 - 2 * part) * ZT + i] = u
            o_ref[YT - (6 - 2 * part) * ZT + i] = u
    low = lowest(jnp.min(gy_ref[...], axis=0))
    low_ref[...] = jnp.broadcast_to(low.reshape(1, 1, 1), low_ref.shape)


def strips(u, left, right, k, lane):
    inner = jnp.where(lane < 32, lroll(u, 8), lroll(u, 32 - (LANES - 16)))
    edge = jnp.where(lane < 8, lroll(left, -8 * k), lroll(right, 48 - 8 * k))
    return jnp.where((lane < 8) | (lane >= 48), edge, inner)


def sweep(first, last, body, carry, by):
    trips = (last - first) // by

    def several(i, carry):
        for k in range(by):
            carry = body(first + i * by + k, carry)
        return carry

    if trips:
        carry = lax.fori_loop(0, trips, several, carry)
    for x in range(first + trips * by, last):
        carry = body(x, carry)
    return carry


def advance(
    own_ref, aux_ref, ya_ref, yo_ref, low_ref, tout_ref, bout_ref,
    us, full, aux, coef, ecoef, edge, mid,
):
    lane = lane_ids(W)
    dt = lowest(jnp.min(low_ref[...], axis=0))
    odd = is_odd("gy")

    def below(i):
        return jnp.where(odd, ya_ref[i], yo_ref[i])

    def above(i):
        return jnp.where(odd, yo_ref[i], ya_ref[i])

    def lay(put, field, plane, x, parts):
        part_x, at = divmod(x, W)
        tile, k = piece(field, at)
        z = YT - (6 - 2 * part_x) * ZT + tile
        for part, (u, get) in enumerate(zip(parts, (below, own_ref.__getitem__, above))):
            put(plane, part * W, u)
            put(plane, 3 * W + part * W, strips(u, get(z), get(z + ZT), k, lane))

    def put_field(field):
        def put(x, row, u):
            if field == 0:
                us[0, 0, x, row : row + W] = u
            else:
                full[field - 1, x, row : row + W] = u

        return put

    def put_aux(field):
        def put(i, row, u):
            aux[field, i, row : row + W] = u

        return put

    off = W - AX
    for field in range(FULL):
        for x in range(XE):
            i = field * XE + x
            lay(put_field(field), field, x, x, (below(i), own_ref[i], above(i)))
    for field in range(AUX):
        for plane in range(XA):
            i = field * XA + plane
            tile, k = FULL * XE + i // 4, i % 4

            def spread(get, k=k, tile=tile):
                return get(tile)[AX * k : AX * k + AX]

            lo = jnp.concatenate([spread(below)] * 4, axis=0)
            hi = jnp.concatenate([spread(above)] * 4, axis=0)
            lay(put_aux(field), FULL + field, plane, plane + off, (lo, aux_ref[i], hi))

    def sums(x, x_p):
        bx, by, bz = full[1, x], full[2, x], full[3, x]
        sx = bx + full[1, x_p]
        sy = by + rroll(by, -1)
        sz = bz + lroll(bz, -1)
        return bx, by, bz, sx, sy, sz

    def face(n, x, kk, bn, b1, b2):
        b1, b2 = 0.25 * b1, 0.25 * b2
        q = bn * bn + b1 * b1 + b2 * b2
        s = (0.5 * FIRST_RATE * dt) * kk / jnp.maximum(q, FACE_FLOOR) * bn
        coef[3 * n, x] = s * bn
        coef[3 * n + 1, x] = 0.25 * (s * b1)
        coef[3 * n + 2, x] = 0.25 * (s * b2)

    def faces(x, carry):
        k_m, sy_m, sz_m = carry
        kap = full[0, x]
        u = us[0, 0, x]
        us[0, 1, x] = lroll(u, -1)
        us[0, 2, x] = lroll(u, 1)
        x_p = jnp.minimum(x + 1, XE - 1)
        bx, by, bz, sx, sy, sz = sums(x, x_p)
        face(0, x, kap + k_m, bx, sy + sy_m, sz + sz_m)
        face(1, x, kap + rroll(kap, 1), by, sz + rroll(sz, 1), sx + rroll(sx, 1))
        face(2, x, kap + lroll(kap, 1), bz, sx + lroll(sx, 1), sy + lroll(sy, 1))
        return kap, sy, sz

    _, _, _, _, sy, sz = sums(0, 1)
    sweep(0, XE, faces, (full[0, 0], sy, sz), 2)

    def upper(x, carry):
        for k in range(3):
            coef[9 + k, x] = lroll(coef[6 + k, x], -1)
        return carry

    sweep(1, XE - 1, upper, 0, 4)

    source, older = us.at[0], None
    for j in range(1, SECTIONS + 1):
        target = us.at[2 - j % 2]
        grow = (2.0 * j - 1.0) / j
        back = (j - 1.0) / j

        def rolled(u, u_p, u_m):
            down = rroll(u, 1)
            return down, rroll(u, -1) - down, u_p - u_m

        def flux_x(x, du, sum_y, sum_z):
            return coef[0, x] * du + coef[1, x] * sum_y + coef[2, x] * sum_z

        def plane(x, carry, source=source, older=older, target=target, grow=grow, back=back, j=j):
            dy, dz, fx, down, new = carry
            if j < SECTIONS:
                target[1, x - 1] = lroll(new, -1)
                target[2, x - 1] = lroll(new, 1)
            u, p, m = source[0, x], source[1, x], source[2, x]
            u_p, p_p, m_p = source[0, x + 1], source[1, x + 1], source[2, x + 1]
            down_p, dy_p, dz_p = rolled(u_p, p_p, m_p)
            fx_p = flux_x(x + 1, u_p - u, dy_p + dy, dz_p + dz)
            dx = u_p - source[0, x - 1]
            dx_zp = p_p - source[1, x - 1]
            dx_zm = m_p - source[2, x - 1]
            p_down, m_down = rroll(p, 1), rroll(m, 1)
            dy_zp = rroll(p, -1) - p_down
            dy_zm = rroll(m, -1) - m_down
            fy = (
                coef[3, x] * (u - down)
                + coef[4, x] * (dz + (p_down - m_down))
                + coef[5, x] * (dx + rroll(dx, 1))
            )
            fz = coef[6, x] * (u - m) + coef[7, x] * (dx + dx_zm) + coef[8, x] * (dy + dy_zm)
            fz_p = coef[9, x] * (p - u) + coef[10, x] * (dx_zp + dx) + coef[11, x] * (dy_zp + dy)
            rate = (fx_p - fx) + (rroll(fy, -1) - fy) + (fz_p - fz)
            new = u + rate
            if j > 1:
                new = grow * new - back * older[0, x]
            if j == SECTIONS:
                b = (SECTIONS * SECTIONS + SECTIONS - 2) / (2.0 * SECTIONS * (SECTIONS + 1))
                new = (1.0 - b) * us[0, 0, x] + b * new
            target[0, x] = new
            return dy_p, dz_p, fx_p, down_p, new

        u_m, u = source[0, j - 1], source[0, j]
        _, dy_m, dz_m = rolled(u_m, source[1, j - 1], source[2, j - 1])
        down, dy, dz = rolled(u, source[1, j], source[2, j])
        fx = flux_x(j, u - u_m, dy + dy_m, dz + dz_m)
        *_, new = sweep(j, XE - j, plane, (dy, dz, fx, down, u), 2)
        if j < SECTIONS:
            target[1, XE - j - 1] = lroll(new, -1)
            target[2, XE - j - 1] = lroll(new, 1)
        source, older = target, source

    def seam(main, strip):
        high = lroll(strip, LANES - 8 - 40)
        return jnp.where(lane < 8, lroll(strip, -8), jnp.where(lane >= LANES - 8, high, main))

    for x in range(W):
        tout_ref[x] = seam(source[0, W + x, W : 2 * W], source[0, W + x, 4 * W : 5 * W])

    SPEED = 3
    for i in range(XA):
        x = i + off
        _, _, _, sx, sy, sz = sums(x, x + 1)
        field = 0.25 * (sx * sx + sy * sy + sz * sz)
        vx, vy, vz = aux[0, i], aux[1, i], aux[2, i]
        flow = jnp.sqrt(vx * vx + vy * vy + vz * vz)
        aux[SPEED, i] = flow + jnp.sqrt(GAMMA * us[0, 0, x] + field / aux[SPEED, i])

    def by_axis(u, u_m, axis):
        if axis == 0:
            return u_m
        return rroll(u, 1) if axis == 1 else lroll(u, 1)

    for i in range(1, XA):
        for c in range(3):
            a, b = (c + 1) % 3, (c + 2) % 3

            def mean(f, i=i, a=a, b=b):
                if 0 in (a, b):
                    other = a + b
                    u = aux[f, i] + aux[f, i - 1]
                else:
                    other = 2
                    u = aux[f, i]
                    u = u + by_axis(u, None, 1)
                return 0.125 * (u + by_axis(u, None, other))

            va, vb, s = mean(a), mean(b), mean(SPEED)
            ecoef[4 * c, i] = vb - s
            ecoef[4 * c + 1, i] = vb + s
            ecoef[4 * c + 2, i] = s - va
            ecoef[4 * c + 3, i] = -s - va

    def fields(get, first, last):
        for i in range(first, last):
            for c in range(3):
                a, b = (c + 1) % 3, (c + 2) % 3
                ua, ub = get(a, i), get(b, i)
                ua_b = by_axis(ua, get(a, i - 1) if b == 0 else None, b)
                ub_a = by_axis(ub, get(b, i - 1) if a == 0 else None, a)
                edge[c, i] = (ecoef[4 * c, i] * ua + ecoef[4 * c + 1, i] * ua_b) + (
                    ecoef[4 * c + 2, i] * ub + ecoef[4 * c + 3, i] * ub_a
                )

    def ahead(f, i, axis):
        if axis == 0:
            return edge[f, i + 1]
        u = edge[f, i]
        return rroll(u, -1) if axis == 1 else lroll(u, -1)

    def curl(d, i):
        e, f = (d + 1) % 3, (d + 2) % 3
        return (ahead(f, i, e) - edge[f, i]) - (ahead(e, i, f) - edge[e, i])

    fields(lambda d, i: full[1 + d, i + off], 1, XA)
    for i in range(1, XA - 1):
        for d in range(3):
            mid[d, i] = full[1 + d, i + off] - dt * curl(d, i)
    fields(lambda d, i: mid[d, i], 2, XA - 1)
    for i in range(AX, AX + W):
        for d in range(3):
            u = 0.5 * (full[1 + d, i + off] + (mid[d, i] - dt * curl(d, i)))
            bout_ref[d, i - AX] = seam(u[W : 2 * W], u[4 * W : 5 * W])


def exchange(first, second, axis):
    count = lax.axis_size(axis)
    swaps = [(i, i + 1) for i in range(0, count, 2)] + [(i + 1, i) for i in range(0, count, 2)]
    others = [((a + 1) % count, (b + 1) % count) for a, b in swaps]
    return lax.ppermute(first, axis, swaps), lax.ppermute(second, axis, others)


def on_core(kernel, out, *args, scratch=(), last=False):
    space = pl.BlockSpec(memory_space=pltpu.VMEM)
    shape = [
        jax.ShapeDtypeStruct(o, jnp.float32) if last else pltpu.VMEM(o, jnp.float32) for o in out
    ]
    return pl.pallas_call(
        kernel,
        out_shape=shape,
        in_specs=[space] * len(args),
        out_specs=[space] * len(out),
        scratch_shapes=[pltpu.VMEM(shape, jnp.float32) for shape in scratch],
        name=kernel.__name__,
    )(*args)


def held(*arrays):
    return [pltpu.with_memory_space_constraint(a, pltpu.VMEM) for a in arrays]


def on_device(t, diffusivity, b, v, rho):
    zs = lax.axis_size("gz")
    outer = lax.axis_size("gx_0") * lax.axis_size("gy")
    inner = lax.axis_size("gx_1") * lax.axis_size("gx_2")
    out = [(W, W, LANES), (zs, ZT, W, LANES)]
    kappa, edges = on_core(pack_z, out, t, diffusivity, b, v, rho)
    edges = lax.all_to_all(edges, "gz", 0, 0, tiled=True)
    kappa, edges = held(kappa, edges)
    out = [(SIDE, W, LANES), (SIDE, W, LANES), (outer, 1, LANES)]
    first, second, low = on_core(pack_x, out, t, kappa, b, v, rho, edges)
    x_first, x_second = exchange(first, second, GX)
    low = lax.all_to_all(low, ("gx_0", "gy"), 0, 0, tiled=True)
    first, x_first, x_second, low = held(first, x_first, x_second, low)
    out = [(YT, W, LANES), (YT, W, LANES), (AUX * XA, W, LANES), (inner, 1, LANES)]
    first, second, aux, low = on_core(pack_y, out, first, v, rho, x_first, x_second, low)
    y_first, y_second = exchange(first, second, "gy")
    low = lax.all_to_all(low, ("gx_1", "gx_2"), 0, 0, tiled=True)
    scratch = [
        (3, 3, XE, ROWS, LANES),
        (FULL - 1, XE, ROWS, LANES),
        (AUX, XA, ROWS, LANES),
        (12, XE, ROWS, LANES),
        (12, XA, ROWS, LANES),
        (3, XA, ROWS, LANES),
        (3, XA, ROWS, LANES),
    ]
    out = [(W, W, LANES), (3, W, W, LANES)]
    args = held(first, aux, y_first, y_second, low)
    return tuple(on_core(advance, out, *args, scratch=scratch, last=True))


def solution(mesh):
    gx, gy, gz = (mesh.shape[axis] for axis in ("gx", "gy", "gz"))
    outer = 3 if gx % 6 == 0 else 1
    finer = Mesh(mesh.devices.reshape(outer, gx // outer // 2, 2, gy, gz), (*GX, "gy", "gz"))
    cell = P(GX, "gy", "gz")
    face = P(None, GX, "gy", "gz")
    return jax.shard_map(
        on_device,
        mesh=finer,
        in_specs=(cell, cell, face, face, cell),
        out_specs=(cell, face),
        check_vma=False,
    )
```

```python
import jax
import jax.numpy as jnp
from jax import lax
from jax.experimental import pallas as pl
from jax.experimental.pallas import tpu as pltpu
from jax.sharding import Mesh
from jax.sharding import PartitionSpec as P

SECTIONS = 8
GAMMA = 5.0 / 3.0
FACE_FLOOR = 0.25

GX = ("gx_0", "gx_1", "gx_2")
W = 8
LANES = 128
XE = 3 * W
WIDE = 4 * W
GROUPS = LANES // WIDE
XG = XE // GROUPS
LOW, HIGH = XE, XE + XG + 1
PLANES = HIGH + 1
ROWS = 3 * W
FULL = 5
AUX = 4
AX = 2
XA = W + 2 * AX
OFF = W - AX
A_LOW, A_HIGH = XA, XA + XG + 1
A_PLANES = A_HIGH + 1
ZT = (FULL + AUX) * W // 16 + 1
SPARE = LANES // 2
SIDE = FULL * W + AUX * AX + FULL + 1
A_TILES = AUX * (XA + XG)
Y_FULL = FULL * (XE + XG)
YT = Y_FULL + A_TILES // 4
FIRST_RATE = 4.0 / (SECTIONS * SECTIONS + SECTIONS - 2)
LIMIT = (SECTIONS * SECTIONS + SECTIONS - 2) / 16.0


def lane_ids(rows):
    return lax.broadcasted_iota(jnp.int32, (rows, LANES), 1)


def lroll(u, amount):
    return pltpu.roll(u, amount % LANES, 1)


def rroll(u, amount):
    return pltpu.roll(u, amount % u.shape[0], 0)


def lowest(u):
    return jnp.min(jnp.min(u, axis=0, keepdims=True), axis=1, keepdims=True)


def neighbours(axis):
    count = lax.axis_size(axis)
    at = lax.axis_index(axis)
    return lax.rem(at + count - 1, count), lax.rem(at + 1, count)


def is_odd(axis):
    return lax.rem(lax.axis_index(axis), 2) == 1


def piece(field, plane):
    return divmod(field * W + plane, 16)


def pack_z(t_ref, d_ref, b_ref, v_ref, r_ref, kap_ref, out_ref):
    t = t_ref[...]
    kappa = d_ref[...] * (t * t * jnp.sqrt(t))
    kap_ref[...] = kappa
    low = lowest(jnp.min(LIMIT / kappa, axis=0))
    lane = lane_ids(W)
    left, right = [], []
    for tile in range(ZT):
        below = above = jnp.broadcast_to(low, (W, LANES))
        for k in range(16):
            field, plane = divmod(tile * 16 + k, W)
            if field >= FULL + AUX:
                break
            if field == 0:
                u = t[plane]
            elif field == 1:
                u = kappa[plane]
            elif field < FULL:
                u = b_ref[field - 2, plane]
            else:
                u = v_ref[field - FULL, plane] if field < FULL + 3 else r_ref[plane]
            here = (lane >= 8 * k) & (lane < 8 * k + 8)
            below = jnp.where(here, lroll(u, 8 * k), below)
            above = jnp.where(here, lroll(u, 8 * k - (LANES - 8)), above)
        left.append(below)
        right.append(above)
    lo, _ = neighbours("gz")
    for slot in range(out_ref.shape[0]):
        for tile in range(ZT):
            out_ref[slot, tile] = jnp.where(lo == slot, left[tile], right[tile])


def pack_x(t_ref, k_ref, b_ref, v_ref, r_ref, z_ref, a_ref, o_ref, aux_ref, low_ref):
    odd = is_odd(GX)
    lo, hi = neighbours("gz")
    lane = lane_ids(W)
    left = [z_ref[lo, tile] for tile in range(ZT)]
    right = [z_ref[hi, tile] for tile in range(ZT)]
    up_ends = down_ends = jnp.zeros((W, LANES), jnp.float32)
    for field in range(FULL + AUX):
        ends = jnp.zeros((W, LANES), jnp.float32)
        for plane in range(W):
            if field < FULL:
                u = (t_ref, k_ref, b_ref.at[0], b_ref.at[1], b_ref.at[2])[field][plane]
            else:
                u = v_ref[field - FULL, plane] if field < FULL + 3 else r_ref[plane]
            tile, k = piece(field, plane)
            main = jnp.where(lane < 8, lroll(left[tile], -8 * k), lroll(u, 8))
            to = 16 * plane
            end = jnp.where(
                lane < to + 8, lroll(u, to + 8 - LANES), lroll(right[tile], to + 8 - 8 * k)
            )
            ends = jnp.where(lane < to, ends, end)
            if field < FULL:
                a_ref[field * W + plane] = main
                o_ref[field * W + plane] = main
                continue
            aux_ref[(field - FULL) * W + plane] = main
            at = FULL * W + (field - FULL) * AX
            if plane < AX:
                a_ref[at + plane] = main
                o_ref[at + plane] = main
            elif plane >= W - AX:
                i = at + plane - (W - AX)
                down = a_ref[i]
                a_ref[i] = jnp.where(odd, down, main)
                o_ref[i] = jnp.where(odd, main, down)
        if field < FULL:
            a_ref[FULL * W + AUX * AX + field] = ends
            o_ref[FULL * W + AUX * AX + field] = ends
        else:
            f = field - FULL
            aux_ref[AUX * W + f] = ends
            here = lane >= 32 * f
            down_ends = jnp.where(here, lroll(ends, 32 * f), down_ends)
            up_ends = jnp.where(here, lroll(ends, 32 * f - (LANES - 32)), up_ends)
    a_ref[SIDE - 1] = jnp.where(odd, down_ends, up_ends)
    o_ref[SIDE - 1] = jnp.where(odd, up_ends, down_ends)
    low = z_ref[0, ZT - 1]
    for slot in range(1, z_ref.shape[0]):
        low = jnp.minimum(low, z_ref[slot, ZT - 1])
    low = lowest(jnp.where(lane >= SPARE, low, jnp.max(low)))
    low_ref[...] = jnp.broadcast_to(low.reshape(1, 1, 1), low_ref.shape)


def pack_y(own_ref, ownaux_ref, xa_ref, xo_ref, min_ref, a_ref, o_ref, aux_ref, low_ref):
    odd_x, odd_y = is_odd(GX), is_odd("gy")
    lane = lane_ids(W)

    def below(i):
        return jnp.where(odd_x, xa_ref[i], xo_ref[i])

    def above(i):
        return jnp.where(odd_x, xo_ref[i], xa_ref[i])

    sides = (below, own_ref.__getitem__, above)

    def send(i, u):
        a_ref[i] = u
        o_ref[i] = u

    ends_at = FULL * W + AUX * AX
    for field in range(FULL):
        ends = [get(ends_at + field) for get in sides]
        mains = []
        for x in range(XE):
            part, at = divmod(x, W)
            mains.append(sides[part](field * W + at))
            send(field * XE + x, mains[x])
        for k in range(XG):
            strip = None
            for g in range(GROUPS):
                part, at = divmod(g * XG + k, W)
                to = g * WIDE
                new = jnp.where(
                    lane < to + 16,
                    lroll(mains[g * XG + k], to + 16 - LANES),
                    lroll(ends[part], to + 16 - 16 * at),
                )
                strip = jnp.where(lane < to, strip, new) if g else new
            send(FULL * XE + field * XG + k, strip)

    def put(i, u):
        aux_ref[i] = u
        tile, k = Y_FULL + i // 4, AX * (i % 4)
        up, down = u[W - AX : W], u[0:AX]
        a_ref[tile, k : k + AX] = jnp.where(odd_y, down, up)
        o_ref[tile, k : k + AX] = jnp.where(odd_y, up, down)

    outer = below(SIDE - 1), above(SIDE - 1)
    for field in range(AUX):
        mains, ends = [], []
        at = FULL * W + field * AX
        for i in range(XA):
            if i < AX:
                mains.append(below(at + i))
                ends.append((outer[0], field * AX + i))
            elif i < AX + W:
                mains.append(ownaux_ref[field * W + i - AX])
                ends.append((ownaux_ref[AUX * W + field], i - AX))
            else:
                mains.append(above(at + i - AX - W))
                ends.append((outer[1], field * AX + i - AX - W))
            put(field * XA + i, mains[i])
        for k in range(XG):
            strip = None
            for g in range(XA // XG):
                u, (end, at_end) = mains[g * XG + k], ends[g * XG + k]
                to = (g + OFF // XG) * WIDE
                new = lroll(u, to + 16 - LANES)
                strip = jnp.where(lane < to, strip, new) if g else new
                new = lroll(end, to + 16 - 16 * at_end)
                strip = jnp.where((lane >= to + 16) & (lane < to + 32), new, strip)
            put(AUX * XA + field * XG + k, strip)
    low = lowest(jnp.min(min_ref[...], axis=0))
    low_ref[...] = jnp.broadcast_to(low.reshape(1, 1, 1), low_ref.shape)


def sweep(first, last, body, carry, by):
    trips = (last - first) // by

    def several(i, carry):
        for k in range(by):
            carry = body(first + i * by + k, carry)
        return carry

    if trips:
        carry = lax.fori_loop(0, trips, several, carry)
    for x in range(first + trips * by, last):
        carry = body(x, carry)
    return carry


def advance(
    own_ref, aux_ref, ya_ref, yo_ref, low_ref, tout_ref, bout_ref,
    us, full, aux, coef, ecoef, edge, mid,
):
    lane = lane_ids(W)
    dt = lowest(jnp.min(low_ref[...], axis=0))
    odd = is_odd("gy")

    sides = (
        lambda i: jnp.where(odd, ya_ref[i], yo_ref[i]),
        own_ref.__getitem__,
        lambda i: jnp.where(odd, yo_ref[i], ya_ref[i]),
    )
    for field in range(FULL):
        to = us.at[0, 0] if field == 0 else full.at[field - 1]
        for x in range(XE + XG):
            i, plane = field * XE + x, x
            if x >= XE:
                i, plane = FULL * XE + field * XG + x - XE, x + 1
            for part in range(3):
                to[plane, part * W : part * W + W] = sides[part](i)
    for field in range(AUX):
        for x in range(XA + XG):
            i, plane = field * XA + x, x
            if x >= XA:
                i, plane = AUX * XA + field * XG + x - XA, x + 1
            tile, k = Y_FULL + i // 4, AX * (i % 4)
            for part in range(3):
                u = aux_ref[i] if part == 1 else jnp.tile(sides[part](tile)[k : k + AX], (4, 1))
                aux[field, plane, part * W : part * W + W] = u

    def beside(ref, low, high):
        ref[low] = lroll(ref[high - 1], WIDE)
        ref[high] = lroll(ref[low + 1], -WIDE)

    beside(us.at[0, 0], LOW, HIGH)
    for k in range(FULL - 1):
        beside(full.at[k], LOW, HIGH)

    def sums(x, x_p):
        bx, by, bz = full[1, x], full[2, x], full[3, x]
        sx = bx + full[1, x_p]
        sy = by + rroll(by, -1)
        sz = bz + lroll(bz, -1)
        return bx, by, bz, sx, sy, sz

    def face(n, x, kk, bn, b1, b2):
        b1, b2 = 0.25 * b1, 0.25 * b2
        q = bn * bn + b1 * b1 + b2 * b2
        s = (0.5 * FIRST_RATE * dt) * kk / jnp.maximum(q, FACE_FLOOR) * bn
        coef[3 * n, x] = s * bn
        coef[3 * n + 1, x] = 0.25 * (s * b1)
        coef[3 * n + 2, x] = 0.25 * (s * b2)

    def faces(x, carry):
        k_m, sy_m, sz_m = carry
        kap = full[0, x]
        u = us[0, 0, x]
        us[0, 1, x] = lroll(u, -1)
        us[0, 2, x] = lroll(u, 1)
        x_p = jnp.minimum(x + 1, PLANES - 1)
        bx, by, bz, sx, sy, sz = sums(x, x_p)
        face(0, x, kap + k_m, bx, sy + sy_m, sz + sz_m)
        face(1, x, kap + rroll(kap, 1), by, sz + rroll(sz, 1), sx + rroll(sx, 1))
        face(2, x, kap + lroll(kap, 1), bz, sx + lroll(sx, 1), sy + lroll(sy, 1))
        return kap, sy, sz

    for first, last in ((0, XE), (LOW, PLANES)):
        _, _, _, _, sy, sz = sums(first, first + 1)
        sweep(first, last, faces, (full[0, first], sy, sz), 4)

    def upper(x, carry):
        for k in range(3):
            coef[9 + k, x] = lroll(coef[6 + k, x], -1)
        return carry

    sweep(0, PLANES, upper, 0, 8)

    source, older = us.at[0], None
    for j in range(1, SECTIONS + 1):
        target = us.at[2 - j % 2]
        grow = (2.0 * j - 1.0) / j
        back = (j - 1.0) / j

        def rolled(u, u_p, u_m):
            down = rroll(u, 1)
            return down, rroll(u, -1) - down, u_p - u_m

        def flux_x(x, du, sum_y, sum_z):
            return coef[0, x] * du + coef[1, x] * sum_y + coef[2, x] * sum_z

        def plane(x, carry, source=source, older=older, target=target, grow=grow, back=back, j=j):
            dy, dz, fx, down = carry
            u, p, m = source[0, x], source[1, x], source[2, x]
            u_p, p_p, m_p = source[0, x + 1], source[1, x + 1], source[2, x + 1]
            down_p, dy_p, dz_p = rolled(u_p, p_p, m_p)
            fx_p = flux_x(x + 1, u_p - u, dy_p + dy, dz_p + dz)
            dx = u_p - source[0, x - 1]
            dx_zp = p_p - source[1, x - 1]
            dx_zm = m_p - source[2, x - 1]
            p_down, m_down = rroll(p, 1), rroll(m, 1)
            dy_zp = rroll(p, -1) - p_down
            dy_zm = rroll(m, -1) - m_down
            fy = (
                coef[3, x] * (u - down)
                + coef[4, x] * (dz + (p_down - m_down))
                + coef[5, x] * (dx + rroll(dx, 1))
            )
            fz = coef[6, x] * (u - m) + coef[7, x] * (dx + dx_zm) + coef[8, x] * (dy + dy_zm)
            fz_p = coef[9, x] * (p - u) + coef[10, x] * (dx_zp + dx) + coef[11, x] * (dy_zp + dy)
            rate = (fx_p - fx) + (rroll(fy, -1) - fy) + (fz_p - fz)
            new = u + rate
            if j > 1:
                new = grow * new - back * older[0, x]
            if j == SECTIONS:
                b = (SECTIONS * SECTIONS + SECTIONS - 2) / (2.0 * SECTIONS * (SECTIONS + 1))
                new = (1.0 - b) * us[0, 0, x] + b * new
            target[0, x] = new
            return dy_p, dz_p, fx_p, down_p

        def start(x, source=source):
            u_m, u = source[0, x - 1], source[0, x]
            _, dy_m, dz_m = rolled(u_m, source[1, x - 1], source[2, x - 1])
            down, dy, dz = rolled(u, source[1, x], source[2, x])
            return dy, dz, flux_x(x, u - u_m, dy + dy_m, dz + dz_m), down

        def turn(x, target=target):
            u = target[0, x]
            target[1, x] = lroll(u, -1)
            target[2, x] = lroll(u, 1)

        carry = start(LOW + 1)
        for x in range(LOW + 1, HIGH):
            carry = plane(x, carry)
        if j < SECTIONS:
            for x in range(LOW + 1, HIGH):
                turn(x)
            beside(target.at[0], LOW, HIGH)
            turn(LOW)
            turn(HIGH)

        def two(i, carry, target=target, plane=plane, turn=turn, j=j):
            x = j + 2 * i
            if j < SECTIONS:
                turn(jnp.maximum(x - 2, 0))
                turn(jnp.maximum(x - 1, 0))
            return plane(x + 1, plane(x, carry))

        lax.fori_loop(0, (XE - 2 * j) // 2, two, start(j))
        if j < SECTIONS:
            turn(XE - j - 2)
            turn(XE - j - 1)
        source, older = target, source

    def seam(main, strip, g):
        return jnp.where(
            lane < LANES - 16, lroll(main, -8), lroll(strip, LANES - 16 - 8 - WIDE * g)
        )

    for x in range(W):
        g, k = divmod(W + x, XG)
        tout_ref[x] = seam(source[0, W + x, W : 2 * W], source[0, LOW + 1 + k, W : 2 * W], g)

    SPEED = 3
    strip = range(A_LOW + 1, A_HIGH)

    def within(i):
        return i + OFF if i < XA else i - A_LOW + LOW

    for i in (*range(XA), *strip):
        x = within(i)
        _, _, _, sx, sy, sz = sums(x, x + 1)
        field = 0.25 * (sx * sx + sy * sy + sz * sz)
        vx, vy, vz = aux[0, i], aux[1, i], aux[2, i]
        flow = jnp.sqrt(vx * vx + vy * vy + vz * vz)
        aux[SPEED, i] = flow + jnp.sqrt(GAMMA * us[0, 0, x] + field / aux[SPEED, i])
    for k in range(AUX):
        aux[k, A_LOW] = lroll(aux[k, A_HIGH - 1], WIDE)

    def by_axis(u, u_m, axis):
        if axis == 0:
            return u_m
        return rroll(u, 1) if axis == 1 else lroll(u, 1)

    for i in (*range(1, XA), *strip):
        for c in range(3):
            a, b = (c + 1) % 3, (c + 2) % 3

            def mean(f, i=i, a=a, b=b):
                if 0 in (a, b):
                    other = a + b
                    u = aux[f, i] + aux[f, i - 1]
                else:
                    other = 2
                    u = aux[f, i]
                    u = u + by_axis(u, None, 1)
                return 0.125 * (u + by_axis(u, None, other))

            va, vb, s = mean(a), mean(b), mean(SPEED)
            ecoef[4 * c, i] = vb - s
            ecoef[4 * c + 1, i] = vb + s
            ecoef[4 * c + 2, i] = s - va
            ecoef[4 * c + 3, i] = -s - va

    def fields(get, first, last):
        for i in (*range(first, last), *strip):
            for c in range(3):
                a, b = (c + 1) % 3, (c + 2) % 3
                ua, ub = get(a, i), get(b, i)
                ua_b = by_axis(ua, get(a, i - 1) if b == 0 else None, b)
                ub_a = by_axis(ub, get(b, i - 1) if a == 0 else None, a)
                edge[c, i] = (ecoef[4 * c, i] * ua + ecoef[4 * c + 1, i] * ua_b) + (
                    ecoef[4 * c + 2, i] * ub + ecoef[4 * c + 3, i] * ub_a
                )
        for c in range(1, 3):
            edge[c, A_HIGH] = lroll(edge[c, A_LOW + 1], -WIDE)

    def ahead(f, i, axis):
        if axis == 0:
            return edge[f, i + 1]
        u = edge[f, i]
        return rroll(u, -1) if axis == 1 else lroll(u, -1)

    def curl(d, i):
        e, f = (d + 1) % 3, (d + 2) % 3
        return (ahead(f, i, e) - edge[f, i]) - (ahead(e, i, f) - edge[e, i])

    fields(lambda d, i: full[1 + d, within(i)], 1, XA)
    for i in (*range(1, XA - 1), *strip):
        for d in range(3):
            mid[d, i] = full[1 + d, within(i)] - dt * curl(d, i)
    for d in range(1, 3):
        mid[d, A_LOW] = lroll(mid[d, A_HIGH - 1], WIDE)
    fields(lambda d, i: mid[d, i], 2, XA - 1)

    def final(d, i):
        u = 0.5 * (full[1 + d, within(i)] + (mid[d, i] - dt * curl(d, i)))
        return u[W : 2 * W]

    for d in range(3):
        ends = [final(d, i) for i in strip]
        for x in range(W):
            g, k = divmod(W + x, XG)
            bout_ref[d, x] = seam(final(d, x + AX), ends[k], g)


def exchange(first, second, axis):
    count = lax.axis_size(axis)
    swaps = [(i, i + 1) for i in range(0, count, 2)] + [(i + 1, i) for i in range(0, count, 2)]
    others = [((a + 1) % count, (b + 1) % count) for a, b in swaps]
    return lax.ppermute(first, axis, swaps), lax.ppermute(second, axis, others)


def on_core(kernel, out, *args, scratch=(), last=False):
    space = pl.BlockSpec(memory_space=pltpu.VMEM)
    shape = [
        jax.ShapeDtypeStruct(o, jnp.float32) if last else pltpu.VMEM(o, jnp.float32) for o in out
    ]
    return pl.pallas_call(
        kernel,
        out_shape=shape,
        in_specs=[space] * len(args),
        out_specs=[space] * len(out),
        scratch_shapes=[pltpu.VMEM(shape, jnp.float32) for shape in scratch],
        name=kernel.__name__,
    )(*args)


def held(*arrays):
    return [pltpu.with_memory_space_constraint(a, pltpu.VMEM) for a in arrays]


def on_device(t, diffusivity, b, v, rho):
    zs = lax.axis_size("gz")
    outer = lax.axis_size("gx_0") * lax.axis_size("gy")
    inner = lax.axis_size("gx_1") * lax.axis_size("gx_2")
    out = [(W, W, LANES), (zs, ZT, W, LANES)]
    kappa, edges = on_core(pack_z, out, t, diffusivity, b, v, rho)
    edges = lax.all_to_all(edges, "gz", 0, 0, tiled=True)
    kappa, edges = held(kappa, edges)
    out = [(SIDE, W, LANES)] * 2 + [((W + 1) * AUX, W, LANES), (outer, 1, LANES)]
    first, second, aux, low = on_core(pack_x, out, t, kappa, b, v, rho, edges)
    x_first, x_second = exchange(first, second, GX)
    low = lax.all_to_all(low, ("gx_0", "gy"), 0, 0, tiled=True)
    args = held(first, aux, x_first, x_second, low)
    out = [(YT, W, LANES)] * 2 + [(A_TILES, W, LANES), (inner, 1, LANES)]
    first, second, aux, low = on_core(pack_y, out, *args)
    y_first, y_second = exchange(first, second, "gy")
    low = lax.all_to_all(low, ("gx_1", "gx_2"), 0, 0, tiled=True)
    scratch = [
        (3, 3, PLANES, ROWS, LANES),
        (FULL - 1, PLANES, ROWS, LANES),
        (AUX, A_PLANES, ROWS, LANES),
        (12, PLANES, ROWS, LANES),
        (12, A_PLANES, ROWS, LANES),
        (3, A_PLANES, ROWS, LANES),
        (3, A_PLANES, ROWS, LANES),
    ]
    out = [(W, W, LANES), (3, W, W, LANES)]
    args = held(first, aux, y_first, y_second, low)
    return tuple(on_core(advance, out, *args, scratch=scratch, last=True))


def solution(mesh):
    gx, gy, gz = (mesh.shape[axis] for axis in ("gx", "gy", "gz"))
    outer = 3 if gx % 6 == 0 else 1
    finer = Mesh(mesh.devices.reshape(outer, gx // outer // 2, 2, gy, gz), (*GX, "gy", "gz"))
    cell = P(GX, "gy", "gz")
    face = P(None, GX, "gy", "gz")
    return jax.shard_map(
        on_device,
        mesh=finer,
        in_specs=(cell, cell, face, face, cell),
        out_specs=(cell, face),
        check_vma=False,
    )
```

```python
import jax
import jax.numpy as jnp
from jax import lax
from jax.experimental import pallas as pl
from jax.experimental.pallas import tpu as pltpu
from jax.sharding import Mesh
from jax.sharding import PartitionSpec as P

SECTIONS = 8
GAMMA = 5.0 / 3.0
FACE_FLOOR = 0.25

GX = ("gx_0", "gx_1", "gx_2")
W = 8
LANES = 128
XE = 3 * W
WIDE = 4 * W
GROUPS = LANES // WIDE
XG = XE // GROUPS
LOW, HIGH = XE, XE + XG + 1
PLANES = HIGH + 1
ROWS = 3 * W
FULL = 5
AUX = 4
AX = 2
XA = W + 2 * AX
OFF = W - AX
A_LOW, A_HIGH = XA, XA + XG + 1
A_PLANES = A_HIGH + 1
ZT = (FULL + AUX) * W // 16 + 1
SPARE = LANES // 2
SIDE = FULL * W + AUX * AX + FULL + 1
A_TILES = AUX * (XA + XG)
Y_FULL = FULL * (XE + XG)
YT = Y_FULL + A_TILES // 4
SCRATCH = [(PLANES, ROWS, LANES)] * 9 + [
    (FULL - 1, PLANES, ROWS, LANES),
    (AUX, A_PLANES, ROWS, LANES),
    (9, PLANES, ROWS, LANES),
    (3, PLANES, ROWS, LANES),
    (12, A_PLANES, ROWS, LANES),
    (3, A_PLANES, ROWS, LANES),
    (3, A_PLANES, ROWS, LANES),
]
FIRST_RATE = 4.0 / (SECTIONS * SECTIONS + SECTIONS - 2)
LIMIT = (SECTIONS * SECTIONS + SECTIONS - 2) / 16.0


def lane_ids(rows):
    return lax.broadcasted_iota(jnp.int32, (rows, LANES), 1)


def lroll(u, amount):
    return pltpu.roll(u, amount % LANES, 1)


def rroll(u, amount):
    return pltpu.roll(u, amount % u.shape[0], 0)


def lowest(u):
    return jnp.min(jnp.min(u, axis=0, keepdims=True), axis=1, keepdims=True)


def neighbours(axis):
    count = lax.axis_size(axis)
    at = lax.axis_index(axis)
    return lax.rem(at + count - 1, count), lax.rem(at + 1, count)


def is_odd(axis):
    return lax.rem(lax.axis_index(axis), 2) == 1


def piece(field, plane):
    return divmod(field * W + plane, 16)


def pack_z(t_ref, d_ref, b_ref, v_ref, r_ref, kap_ref, out_ref):
    t = t_ref[...]
    kappa = d_ref[...] * (t * t * jnp.sqrt(t))
    kap_ref[...] = kappa
    low = lowest(jnp.min(LIMIT / kappa, axis=0))
    lane = lane_ids(W)
    left, right = [], []
    for tile in range(ZT):
        below = above = jnp.broadcast_to(low, (W, LANES))
        for k in range(16):
            field, plane = divmod(tile * 16 + k, W)
            if field >= FULL + AUX:
                break
            if field == 0:
                u = t[plane]
            elif field == 1:
                u = kappa[plane]
            elif field < FULL:
                u = b_ref[field - 2, plane]
            else:
                u = v_ref[field - FULL, plane] if field < FULL + 3 else r_ref[plane]
            here = (lane >= 8 * k) & (lane < 8 * k + 8)
            below = jnp.where(here, lroll(u, 8 * k), below)
            above = jnp.where(here, lroll(u, 8 * k - (LANES - 8)), above)
        left.append(below)
        right.append(above)
    lo, _ = neighbours("gz")
    for slot in range(out_ref.shape[0]):
        for tile in range(ZT):
            out_ref[slot, tile] = jnp.where(lo == slot, left[tile], right[tile])


def pack_x(t_ref, k_ref, b_ref, v_ref, r_ref, z_ref, a_ref, o_ref, aux_ref, low_ref):
    odd = is_odd(GX)
    lo, hi = neighbours("gz")
    lane = lane_ids(W)
    left = [z_ref[lo, tile] for tile in range(ZT)]
    right = [z_ref[hi, tile] for tile in range(ZT)]
    up_ends = down_ends = jnp.zeros((W, LANES), jnp.float32)
    for field in range(FULL + AUX):
        ends = jnp.zeros((W, LANES), jnp.float32)
        for plane in range(W):
            if field < FULL:
                u = (t_ref, k_ref, b_ref.at[0], b_ref.at[1], b_ref.at[2])[field][plane]
            else:
                u = v_ref[field - FULL, plane] if field < FULL + 3 else r_ref[plane]
            tile, k = piece(field, plane)
            main = jnp.where(lane < 8, lroll(left[tile], -8 * k), lroll(u, 8))
            to = 16 * plane
            end = jnp.where(
                lane < to + 8, lroll(u, to + 8 - LANES), lroll(right[tile], to + 8 - 8 * k)
            )
            ends = jnp.where(lane < to, ends, end)
            if field < FULL:
                a_ref[field * W + plane] = main
                o_ref[field * W + plane] = main
                continue
            aux_ref[(field - FULL) * W + plane] = main
            at = FULL * W + (field - FULL) * AX
            if plane < AX:
                a_ref[at + plane] = main
                o_ref[at + plane] = main
            elif plane >= W - AX:
                i = at + plane - (W - AX)
                down = a_ref[i]
                a_ref[i] = jnp.where(odd, down, main)
                o_ref[i] = jnp.where(odd, main, down)
        if field < FULL:
            a_ref[FULL * W + AUX * AX + field] = ends
            o_ref[FULL * W + AUX * AX + field] = ends
        else:
            f = field - FULL
            aux_ref[AUX * W + f] = ends
            here = lane >= 32 * f
            down_ends = jnp.where(here, lroll(ends, 32 * f), down_ends)
            up_ends = jnp.where(here, lroll(ends, 32 * f - (LANES - 32)), up_ends)
    a_ref[SIDE - 1] = jnp.where(odd, down_ends, up_ends)
    o_ref[SIDE - 1] = jnp.where(odd, up_ends, down_ends)
    low = z_ref[0, ZT - 1]
    for slot in range(1, z_ref.shape[0]):
        low = jnp.minimum(low, z_ref[slot, ZT - 1])
    low = lowest(jnp.where(lane >= SPARE, low, jnp.max(low)))
    low_ref[...] = jnp.broadcast_to(low.reshape(1, 1, 1), low_ref.shape)


def pack_y(own_ref, ownaux_ref, xa_ref, xo_ref, min_ref, a_ref, o_ref, aux_ref, low_ref):
    odd_x, odd_y = is_odd(GX), is_odd("gy")
    lane = lane_ids(W)

    def below(i):
        return jnp.where(odd_x, xa_ref[i], xo_ref[i])

    def above(i):
        return jnp.where(odd_x, xo_ref[i], xa_ref[i])

    sides = (below, own_ref.__getitem__, above)

    def send(i, u):
        a_ref[i] = u
        o_ref[i] = u

    ends_at = FULL * W + AUX * AX
    for field in range(FULL):
        ends = [get(ends_at + field) for get in sides]
        mains = []
        for x in range(XE):
            part, at = divmod(x, W)
            mains.append(sides[part](field * W + at))
            send(field * XE + x, mains[x])
        for k in range(XG):
            strip = None
            for g in range(GROUPS):
                part, at = divmod(g * XG + k, W)
                to = g * WIDE
                new = jnp.where(
                    lane < to + 16,
                    lroll(mains[g * XG + k], to + 16 - LANES),
                    lroll(ends[part], to + 16 - 16 * at),
                )
                strip = jnp.where(lane < to, strip, new) if g else new
            send(FULL * XE + field * XG + k, strip)

    def put(i, u):
        aux_ref[i] = u
        tile, k = Y_FULL + i // 4, AX * (i % 4)
        up, down = u[W - AX : W], u[0:AX]
        a_ref[tile, k : k + AX] = jnp.where(odd_y, down, up)
        o_ref[tile, k : k + AX] = jnp.where(odd_y, up, down)

    outer = below(SIDE - 1), above(SIDE - 1)
    for field in range(AUX):
        mains, ends = [], []
        at = FULL * W + field * AX
        for i in range(XA):
            if i < AX:
                mains.append(below(at + i))
                ends.append((outer[0], field * AX + i))
            elif i < AX + W:
                mains.append(ownaux_ref[field * W + i - AX])
                ends.append((ownaux_ref[AUX * W + field], i - AX))
            else:
                mains.append(above(at + i - AX - W))
                ends.append((outer[1], field * AX + i - AX - W))
            put(field * XA + i, mains[i])
        for k in range(XG):
            strip = None
            for g in range(XA // XG):
                u, (end, at_end) = mains[g * XG + k], ends[g * XG + k]
                to = (g + OFF // XG) * WIDE
                new = lroll(u, to + 16 - LANES)
                strip = jnp.where(lane < to, strip, new) if g else new
                new = lroll(end, to + 16 - 16 * at_end)
                strip = jnp.where((lane >= to + 16) & (lane < to + 32), new, strip)
            put(AUX * XA + field * XG + k, strip)
    low = lowest(jnp.min(min_ref[...], axis=0))
    low_ref[...] = jnp.broadcast_to(low.reshape(1, 1, 1), low_ref.shape)


def sweep(first, last, body, carry, by):
    trips = (last - first) // by

    def several(i, carry):
        for k in range(by):
            carry = body(first + i * by + k, carry)
        return carry

    if trips:
        carry = lax.fori_loop(0, trips, several, carry)
    for x in range(first + trips * by, last):
        carry = body(x, carry)
    return carry


def advance(
    own_ref, aux_ref, ya_ref, yo_ref, low_ref, tout_ref, bout_ref,
    y00, y01, y02, y10, y11, y12, y20, y21, y22, full, aux, coef, coef_up, ecoef, edge, mid,
):
    lane = lane_ids(W)
    dt = lowest(jnp.min(low_ref[...], axis=0))
    odd = is_odd("gy")

    sides = (
        lambda i: jnp.where(odd, ya_ref[i], yo_ref[i]),
        own_ref.__getitem__,
        lambda i: jnp.where(odd, yo_ref[i], ya_ref[i]),
    )
    for field in range(FULL):
        to = y00 if field == 0 else full.at[field - 1]
        for x in range(XE + XG):
            i, plane = field * XE + x, x
            if x >= XE:
                i, plane = FULL * XE + field * XG + x - XE, x + 1
            for part in range(3):
                to[plane, part * W : part * W + W] = sides[part](i)
    for field in range(AUX):
        for x in range(XA + XG):
            i, plane = field * XA + x, x
            if x >= XA:
                i, plane = AUX * XA + field * XG + x - XA, x + 1
            tile, k = Y_FULL + i // 4, AX * (i % 4)
            for part in range(3):
                u = aux_ref[i] if part == 1 else jnp.tile(sides[part](tile)[k : k + AX], (4, 1))
                aux[field, plane, part * W : part * W + W] = u

    def beside(ref, low, high):
        ref[low] = lroll(ref[high - 1], WIDE)
        ref[high] = lroll(ref[low + 1], -WIDE)

    beside(y00, LOW, HIGH)
    for k in range(FULL - 1):
        beside(full.at[k], LOW, HIGH)

    def sums(x, x_p):
        bx, by, bz = full[1, x], full[2, x], full[3, x]
        sx = bx + full[1, x_p]
        sy = by + rroll(by, -1)
        sz = bz + lroll(bz, -1)
        return bx, by, bz, sx, sy, sz

    def face(n, x, kk, bn, b1, b2):
        b1, b2 = 0.25 * b1, 0.25 * b2
        q = bn * bn + b1 * b1 + b2 * b2
        s = (0.5 * FIRST_RATE * dt) * kk / jnp.maximum(q, FACE_FLOOR) * bn
        coef[3 * n, x] = s * bn
        coef[3 * n + 1, x] = 0.25 * (s * b1)
        coef[3 * n + 2, x] = 0.25 * (s * b2)

    def faces(x, carry):
        k_m, sy_m, sz_m = carry
        kap = full[0, x]
        u = y00[x]
        y01[x] = lroll(u, -1)
        y02[x] = lroll(u, 1)
        x_p = jnp.minimum(x + 1, PLANES - 1)
        bx, by, bz, sx, sy, sz = sums(x, x_p)
        face(0, x, kap + k_m, bx, sy + sy_m, sz + sz_m)
        face(1, x, kap + rroll(kap, 1), by, sz + rroll(sz, 1), sx + rroll(sx, 1))
        face(2, x, kap + lroll(kap, 1), bz, sx + lroll(sx, 1), sy + lroll(sy, 1))
        return kap, sy, sz

    for first, last in ((0, XE), (LOW, PLANES)):
        _, _, _, _, sy, sz = sums(first, first + 1)
        sweep(first, last, faces, (full[0, first], sy, sz), 4)

    def upper(x, carry):
        for k in range(3):
            coef_up[k, x] = lroll(coef[6 + k, x], -1)
        return carry

    sweep(0, PLANES, upper, 0, 8)

    arrays = ((y00, y01, y02), (y10, y11, y12), (y20, y21, y22))
    source, older = arrays[0], None
    for j in range(1, SECTIONS + 1):
        target = arrays[2 - j % 2]
        grow = (2.0 * j - 1.0) / j
        back = (j - 1.0) / j

        def rolled(u, u_p, u_m):
            down = rroll(u, 1)
            return down, rroll(u, -1) - down, u_p - u_m

        def flux_x(x, du, sum_y, sum_z):
            return coef[0, x] * du + coef[1, x] * sum_y + coef[2, x] * sum_z

        def plane(x, carry, source=source, older=older, target=target, grow=grow, back=back, j=j):
            dy, dz, fx, down = carry
            u, p, m = source[0][x], source[1][x], source[2][x]
            u_p, p_p, m_p = source[0][x + 1], source[1][x + 1], source[2][x + 1]
            down_p, dy_p, dz_p = rolled(u_p, p_p, m_p)
            fx_p = flux_x(x + 1, u_p - u, dy_p + dy, dz_p + dz)
            dx = u_p - source[0][x - 1]
            dx_zp = p_p - source[1][x - 1]
            dx_zm = m_p - source[2][x - 1]
            p_down, m_down = rroll(p, 1), rroll(m, 1)
            dy_zp = rroll(p, -1) - p_down
            dy_zm = rroll(m, -1) - m_down
            fy = (
                coef[3, x] * (u - down)
                + coef[4, x] * (dz + (p_down - m_down))
                + coef[5, x] * (dx + rroll(dx, 1))
            )
            fz = coef[6, x] * (u - m) + coef[7, x] * (dx + dx_zm) + coef[8, x] * (dy + dy_zm)
            fz_p = coef_up[0, x] * (p - u) + coef_up[1, x] * (dx_zp + dx) + coef_up[2, x] * (dy_zp + dy)
            rate = (fx_p - fx) + (rroll(fy, -1) - fy) + (fz_p - fz)
            new = u + rate
            if j > 1:
                new = grow * new - back * older[0][x]
            if j == SECTIONS:
                b = (SECTIONS * SECTIONS + SECTIONS - 2) / (2.0 * SECTIONS * (SECTIONS + 1))
                new = (1.0 - b) * y00[x] + b * new
            target[0][x] = new
            return (dy_p, dz_p, fx_p, down_p), new

        def start(x, source=source):
            u_m, u = source[0][x - 1], source[0][x]
            _, dy_m, dz_m = rolled(u_m, source[1][x - 1], source[2][x - 1])
            down, dy, dz = rolled(u, source[1][x], source[2][x])
            return dy, dz, flux_x(x, u - u_m, dy + dy_m, dz + dz_m), down

        def two(i, carry, target=target, plane=plane, j=j):
            x = j + 2 * i
            carry, *made = carry
            turned = [(lroll(u, -1), lroll(u, 1)) for u in made]
            carry, first = plane(x, carry)
            carry, second = plane(x + 1, carry)
            if j < SECTIONS:
                for k, (up, down) in enumerate(turned):
                    at = jnp.maximum(x - 2 + k, 0)
                    target[1][at] = up
                    target[2][at] = down
            return carry, first, second

        carry = start(j)
        _, *made = lax.fori_loop(0, (XE - 2 * j) // 2, two, (carry, carry[3], carry[3]))
        carry = start(LOW + 1)
        strip = []
        for x in range(LOW + 1, HIGH):
            carry, new = plane(x, carry)
            strip.append(new)
        if j < SECTIONS:
            for k, u in enumerate(made):
                target[1][XE - j - 2 + k] = lroll(u, -1)
                target[2][XE - j - 2 + k] = lroll(u, 1)
            for at, u, by in ((HIGH, strip[0], -WIDE), (LOW, strip[-1], WIDE)):
                target[0][at] = lroll(u, by)
                target[1][at] = lroll(u, by - 1)
                target[2][at] = lroll(u, by + 1)
            for k, u in enumerate(strip):
                target[1][LOW + 1 + k] = lroll(u, -1)
                target[2][LOW + 1 + k] = lroll(u, 1)
        source, older = target, source

    def seam(main, strip, g):
        return jnp.where(
            lane < LANES - 16, lroll(main, -8), lroll(strip, LANES - 16 - 8 - WIDE * g)
        )

    for x in range(W):
        g, k = divmod(W + x, XG)
        tout_ref[x] = seam(source[0][W + x, W : 2 * W], source[0][LOW + 1 + k, W : 2 * W], g)

    SPEED = 3
    strip = range(A_LOW + 1, A_HIGH)

    def within(i):
        return i + OFF if i < XA else i - A_LOW + LOW

    for i in (*range(XA), *strip):
        x = within(i)
        _, _, _, sx, sy, sz = sums(x, x + 1)
        field = 0.25 * (sx * sx + sy * sy + sz * sz)
        vx, vy, vz = aux[0, i], aux[1, i], aux[2, i]
        flow = jnp.sqrt(vx * vx + vy * vy + vz * vz)
        aux[SPEED, i] = flow + jnp.sqrt(GAMMA * y00[x] + field / aux[SPEED, i])
    for k in range(AUX):
        aux[k, A_LOW] = lroll(aux[k, A_HIGH - 1], WIDE)

    def by_axis(u, u_m, axis):
        if axis == 0:
            return u_m
        return rroll(u, 1) if axis == 1 else lroll(u, 1)

    for i in (*range(1, XA), *strip):
        for c in range(3):
            a, b = (c + 1) % 3, (c + 2) % 3

            def mean(f, i=i, a=a, b=b):
                if 0 in (a, b):
                    other = a + b
                    u = aux[f, i] + aux[f, i - 1]
                else:
                    other = 2
                    u = aux[f, i]
                    u = u + by_axis(u, None, 1)
                return 0.125 * (u + by_axis(u, None, other))

            va, vb, s = mean(a), mean(b), mean(SPEED)
            ecoef[4 * c, i] = vb - s
            ecoef[4 * c + 1, i] = vb + s
            ecoef[4 * c + 2, i] = s - va
            ecoef[4 * c + 3, i] = -s - va

    def fields(get, first, last):
        for i in (*range(first, last), *strip):
            for c in range(3):
                a, b = (c + 1) % 3, (c + 2) % 3
                ua, ub = get(a, i), get(b, i)
                ua_b = by_axis(ua, get(a, i - 1) if b == 0 else None, b)
                ub_a = by_axis(ub, get(b, i - 1) if a == 0 else None, a)
                edge[c, i] = (ecoef[4 * c, i] * ua + ecoef[4 * c + 1, i] * ua_b) + (
                    ecoef[4 * c + 2, i] * ub + ecoef[4 * c + 3, i] * ub_a
                )
        for c in range(1, 3):
            edge[c, A_HIGH] = lroll(edge[c, A_LOW + 1], -WIDE)

    def ahead(f, i, axis):
        if axis == 0:
            return edge[f, i + 1]
        u = edge[f, i]
        return rroll(u, -1) if axis == 1 else lroll(u, -1)

    def curl(d, i):
        e, f = (d + 1) % 3, (d + 2) % 3
        return (ahead(f, i, e) - edge[f, i]) - (ahead(e, i, f) - edge[e, i])

    fields(lambda d, i: full[1 + d, within(i)], 1, XA)
    for i in (*range(1, XA - 1), *strip):
        for d in range(3):
            mid[d, i] = full[1 + d, within(i)] - dt * curl(d, i)
    for d in range(1, 3):
        mid[d, A_LOW] = lroll(mid[d, A_HIGH - 1], WIDE)
    fields(lambda d, i: mid[d, i], 2, XA - 1)

    def final(d, i):
        u = 0.5 * (full[1 + d, within(i)] + (mid[d, i] - dt * curl(d, i)))
        return u[W : 2 * W]

    for d in range(3):
        ends = [final(d, i) for i in strip]
        for x in range(W):
            g, k = divmod(W + x, XG)
            bout_ref[d, x] = seam(final(d, x + AX), ends[k], g)


def exchange(first, second, axis):
    count = lax.axis_size(axis)
    swaps = [(i, i + 1) for i in range(0, count, 2)] + [(i + 1, i) for i in range(0, count, 2)]
    others = [((a + 1) % count, (b + 1) % count) for a, b in swaps]
    return lax.ppermute(first, axis, swaps), lax.ppermute(second, axis, others)


def on_core(kernel, out, *args, scratch=(), last=False):
    space = pl.BlockSpec(memory_space=pltpu.VMEM)
    shape = [
        jax.ShapeDtypeStruct(o, jnp.float32) if last else pltpu.VMEM(o, jnp.float32) for o in out
    ]
    return pl.pallas_call(
        kernel,
        out_shape=shape,
        in_specs=[space] * len(args),
        out_specs=[space] * len(out),
        scratch_shapes=[pltpu.VMEM(shape, jnp.float32) for shape in scratch],
        name=kernel.__name__,
    )(*args)


def held(*arrays):
    return [pltpu.with_memory_space_constraint(a, pltpu.VMEM) for a in arrays]


def on_device(t, diffusivity, b, v, rho):
    zs = lax.axis_size("gz")
    outer = lax.axis_size("gx_0") * lax.axis_size("gy")
    inner = lax.axis_size("gx_1") * lax.axis_size("gx_2")
    out = [(W, W, LANES), (zs, ZT, W, LANES)]
    kappa, edges = on_core(pack_z, out, t, diffusivity, b, v, rho)
    edges = lax.all_to_all(edges, "gz", 0, 0, tiled=True)
    kappa, edges = held(kappa, edges)
    out = [(SIDE, W, LANES)] * 2 + [((W + 1) * AUX, W, LANES), (outer, 1, LANES)]
    first, second, aux, low = on_core(pack_x, out, t, kappa, b, v, rho, edges)
    x_first, x_second = exchange(first, second, GX)
    low = lax.all_to_all(low, ("gx_0", "gy"), 0, 0, tiled=True)
    args = held(first, aux, x_first, x_second, low)
    out = [(YT, W, LANES)] * 2 + [(A_TILES, W, LANES), (inner, 1, LANES)]
    first, second, aux, low = on_core(pack_y, out, *args)
    y_first, y_second = exchange(first, second, "gy")
    low = lax.all_to_all(low, ("gx_1", "gx_2"), 0, 0, tiled=True)
    out = [(W, W, LANES), (3, W, W, LANES)]
    args = held(first, aux, y_first, y_second, low)
    return tuple(on_core(advance, out, *args, scratch=SCRATCH, last=True))


def solution(mesh):
    gx, gy, gz = (mesh.shape[axis] for axis in ("gx", "gy", "gz"))
    outer = 3 if gx % 6 == 0 else 1
    finer = Mesh(mesh.devices.reshape(outer, gx // outer // 2, 2, gy, gz), (*GX, "gy", "gz"))
    cell = P(GX, "gy", "gz")
    face = P(None, GX, "gy", "gz")
    return jax.shard_map(
        on_device,
        mesh=finer,
        in_specs=(cell, cell, face, face, cell),
        out_specs=(cell, face),
        check_vma=False,
    )
```

```python
import jax
import jax.numpy as jnp
from jax import lax
from jax.experimental import pallas as pl
from jax.experimental.pallas import tpu as pltpu
from jax.sharding import Mesh
from jax.sharding import PartitionSpec as P

SECTIONS = 8
GAMMA = 5.0 / 3.0
FACE_FLOOR = 0.25

GX = ("gx_0", "gx_1", "gx_2")
W = 8
LANES = 128
XE = 3 * W
WIDE = 4 * W
GROUPS = LANES // WIDE
XG = XE // GROUPS
LOW, HIGH = XE, XE + XG + 1
PLANES = HIGH + 1
ROWS = 3 * W
FULL = 5
AUX = 4
AX = 2
XA = W + 2 * AX
OFF = W - AX
A_LOW, A_HIGH = XA, XA + XG + 1
A_PLANES = A_HIGH + 1
ZT = (FULL + AUX) * W // 16 + 1
SPARE = LANES // 2
SIDE = FULL * W + AUX * AX + FULL + 1
A_TILES = AUX * (XA + XG)
Y_FULL = FULL * (XE + XG)
YT = Y_FULL + A_TILES // 4
SCRATCH = [(PLANES, ROWS, LANES)] * 9 + [
    (FULL - 1, PLANES, ROWS, LANES),
    (AUX, A_PLANES, ROWS, LANES),
    (9, PLANES, ROWS, LANES),
    (3, PLANES, ROWS, LANES),
    (12, A_PLANES, ROWS, LANES),
    (3, A_PLANES, ROWS, LANES),
    (3, A_PLANES, ROWS, LANES),
]
FIRST_RATE = 4.0 / (SECTIONS * SECTIONS + SECTIONS - 2)
LIMIT = (SECTIONS * SECTIONS + SECTIONS - 2) / 16.0


def lane_ids(rows):
    return lax.broadcasted_iota(jnp.int32, (rows, LANES), 1)


def lroll(u, amount):
    return pltpu.roll(u, amount % LANES, 1)


def rroll(u, amount):
    return pltpu.roll(u, amount % u.shape[0], 0)


def lowest(u):
    return jnp.min(jnp.min(u, axis=0, keepdims=True), axis=1, keepdims=True)


def neighbours(axis):
    count = lax.axis_size(axis)
    at = lax.axis_index(axis)
    return lax.rem(at + count - 1, count), lax.rem(at + 1, count)


def is_odd(axis):
    return lax.rem(lax.axis_index(axis), 2) == 1


def piece(field, plane):
    return divmod(field * W + plane, 16)


def pack_z(t_ref, d_ref, b_ref, v_ref, r_ref, kap_ref, out_ref):
    t = t_ref[...]
    kappa = d_ref[...] * (t * t * jnp.sqrt(t))
    kap_ref[...] = kappa
    low = lowest(jnp.min(LIMIT / kappa, axis=0))
    lane = lane_ids(W)
    left, right = [], []
    for tile in range(ZT):
        below = above = jnp.broadcast_to(low, (W, LANES))
        for k in range(16):
            field, plane = divmod(tile * 16 + k, W)
            if field >= FULL + AUX:
                break
            if field == 0:
                u = t[plane]
            elif field == 1:
                u = kappa[plane]
            elif field < FULL:
                u = b_ref[field - 2, plane]
            else:
                u = v_ref[field - FULL, plane] if field < FULL + 3 else r_ref[plane]
            here = (lane >= 8 * k) & (lane < 8 * k + 8)
            below = jnp.where(here, lroll(u, 8 * k), below)
            above = jnp.where(here, lroll(u, 8 * k - (LANES - 8)), above)
        left.append(below)
        right.append(above)
    lo, _ = neighbours("gz")
    for slot in range(out_ref.shape[0]):
        for tile in range(ZT):
            out_ref[slot, tile] = jnp.where(lo == slot, left[tile], right[tile])


def pack_x(t_ref, k_ref, b_ref, v_ref, r_ref, z_ref, a_ref, o_ref, aux_ref, low_ref):
    odd = is_odd(GX)
    lo, hi = neighbours("gz")
    lane = lane_ids(W)
    left = [z_ref[lo, tile] for tile in range(ZT)]
    right = [z_ref[hi, tile] for tile in range(ZT)]
    up_ends = down_ends = jnp.zeros((W, LANES), jnp.float32)
    for field in range(FULL + AUX):
        ends = jnp.zeros((W, LANES), jnp.float32)
        for plane in range(W):
            if field < FULL:
                u = (t_ref, k_ref, b_ref.at[0], b_ref.at[1], b_ref.at[2])[field][plane]
            else:
                u = v_ref[field - FULL, plane] if field < FULL + 3 else r_ref[plane]
            tile, k = piece(field, plane)
            main = jnp.where(lane < 8, lroll(left[tile], -8 * k), lroll(u, 8))
            to = 16 * plane
            end = jnp.where(
                lane < to + 8, lroll(u, to + 8 - LANES), lroll(right[tile], to + 8 - 8 * k)
            )
            ends = jnp.where(lane < to, ends, end)
            if field < FULL:
                a_ref[field * W + plane] = main
                o_ref[field * W + plane] = main
                continue
            aux_ref[(field - FULL) * W + plane] = main
            at = FULL * W + (field - FULL) * AX
            if plane < AX:
                a_ref[at + plane] = main
                o_ref[at + plane] = main
            elif plane >= W - AX:
                i = at + plane - (W - AX)
                down = a_ref[i]
                a_ref[i] = jnp.where(odd, down, main)
                o_ref[i] = jnp.where(odd, main, down)
        if field < FULL:
            a_ref[FULL * W + AUX * AX + field] = ends
            o_ref[FULL * W + AUX * AX + field] = ends
        else:
            f = field - FULL
            aux_ref[AUX * W + f] = ends
            here = lane >= 32 * f
            down_ends = jnp.where(here, lroll(ends, 32 * f), down_ends)
            up_ends = jnp.where(here, lroll(ends, 32 * f - (LANES - 32)), up_ends)
    a_ref[SIDE - 1] = jnp.where(odd, down_ends, up_ends)
    o_ref[SIDE - 1] = jnp.where(odd, up_ends, down_ends)
    low = z_ref[0, ZT - 1]
    for slot in range(1, z_ref.shape[0]):
        low = jnp.minimum(low, z_ref[slot, ZT - 1])
    low = lowest(jnp.where(lane >= SPARE, low, jnp.max(low)))
    low_ref[...] = jnp.broadcast_to(low.reshape(1, 1, 1), low_ref.shape)


def pack_y(own_ref, ownaux_ref, xa_ref, xo_ref, min_ref, a_ref, o_ref, aux_ref, low_ref):
    odd_x, odd_y = is_odd(GX), is_odd("gy")
    lane = lane_ids(W)

    def below(i):
        return jnp.where(odd_x, xa_ref[i], xo_ref[i])

    def above(i):
        return jnp.where(odd_x, xo_ref[i], xa_ref[i])

    sides = (below, own_ref.__getitem__, above)

    def send(i, u):
        a_ref[i] = u
        o_ref[i] = u

    ends_at = FULL * W + AUX * AX
    for field in range(FULL):
        ends = [get(ends_at + field) for get in sides]
        mains = []
        for x in range(XE):
            part, at = divmod(x, W)
            mains.append(sides[part](field * W + at))
            send(field * XE + x, mains[x])
        for k in range(XG):
            strip = None
            for g in range(GROUPS):
                part, at = divmod(g * XG + k, W)
                to = g * WIDE
                new = jnp.where(
                    lane < to + 16,
                    lroll(mains[g * XG + k], to + 16 - LANES),
                    lroll(ends[part], to + 16 - 16 * at),
                )
                strip = jnp.where(lane < to, strip, new) if g else new
            send(FULL * XE + field * XG + k, strip)

    def put(i, u):
        aux_ref[i] = u
        tile, k = Y_FULL + i // 4, AX * (i % 4)
        up, down = u[W - AX : W], u[0:AX]
        a_ref[tile, k : k + AX] = jnp.where(odd_y, down, up)
        o_ref[tile, k : k + AX] = jnp.where(odd_y, up, down)

    outer = below(SIDE - 1), above(SIDE - 1)
    for field in range(AUX):
        mains, ends = [], []
        at = FULL * W + field * AX
        for i in range(XA):
            if i < AX:
                mains.append(below(at + i))
                ends.append((outer[0], field * AX + i))
            elif i < AX + W:
                mains.append(ownaux_ref[field * W + i - AX])
                ends.append((ownaux_ref[AUX * W + field], i - AX))
            else:
                mains.append(above(at + i - AX - W))
                ends.append((outer[1], field * AX + i - AX - W))
            put(field * XA + i, mains[i])
        for k in range(XG):
            strip = None
            for g in range(XA // XG):
                u, (end, at_end) = mains[g * XG + k], ends[g * XG + k]
                to = (g + OFF // XG) * WIDE
                new = lroll(u, to + 16 - LANES)
                strip = jnp.where(lane < to, strip, new) if g else new
                new = lroll(end, to + 16 - 16 * at_end)
                strip = jnp.where((lane >= to + 16) & (lane < to + 32), new, strip)
            put(AUX * XA + field * XG + k, strip)
    low = lowest(jnp.min(min_ref[...], axis=0))
    low_ref[...] = jnp.broadcast_to(low.reshape(1, 1, 1), low_ref.shape)


def sweep(first, last, body, carry, by):
    trips = (last - first) // by

    def several(i, carry):
        for k in range(by):
            carry = body(first + i * by + k, carry)
        return carry

    if trips:
        carry = lax.fori_loop(0, trips, several, carry)
    for x in range(first + trips * by, last):
        carry = body(x, carry)
    return carry


def advance(
    own_ref, aux_ref, ya_ref, yo_ref, low_ref, tout_ref, bout_ref,
    y00, y01, y02, y10, y11, y12, y20, y21, y22, full, aux, coef, coef_up, ecoef, edge, mid,
):
    lane = lane_ids(W)
    dt = lowest(jnp.min(low_ref[...], axis=0))
    odd = is_odd("gy")

    sides = (
        lambda i: jnp.where(odd, ya_ref[i], yo_ref[i]),
        own_ref.__getitem__,
        lambda i: jnp.where(odd, yo_ref[i], ya_ref[i]),
    )
    for field in range(FULL):
        to = y00 if field == 0 else full.at[field - 1]
        for x in range(XE + XG):
            i, plane = field * XE + x, x
            if x >= XE:
                i, plane = FULL * XE + field * XG + x - XE, x + 1
            for part in range(3):
                to[plane, part * W : part * W + W] = sides[part](i)
    for field in range(AUX):
        for x in range(XA + XG):
            i, plane = field * XA + x, x
            if x >= XA:
                i, plane = AUX * XA + field * XG + x - XA, x + 1
            tile, k = Y_FULL + i // 4, AX * (i % 4)
            for part in range(3):
                u = aux_ref[i] if part == 1 else jnp.tile(sides[part](tile)[k : k + AX], (4, 1))
                aux[field, plane, part * W : part * W + W] = u

    def beside(ref, low, high):
        ref[low] = lroll(ref[high - 1], WIDE)
        ref[high] = lroll(ref[low + 1], -WIDE)

    beside(y00, LOW, HIGH)
    for k in range(FULL - 1):
        beside(full.at[k], LOW, HIGH)

    def sums(x, x_p):
        bx, by, bz = full[1, x], full[2, x], full[3, x]
        sx = bx + full[1, x_p]
        sy = by + rroll(by, -1)
        sz = bz + lroll(bz, -1)
        return bx, by, bz, sx, sy, sz

    def face(n, x, kk, bn, b1, b2):
        b1, b2 = 0.25 * b1, 0.25 * b2
        q = bn * bn + b1 * b1 + b2 * b2
        s = (0.5 * FIRST_RATE * dt) * kk / jnp.maximum(q, FACE_FLOOR) * bn
        coef[3 * n, x] = s * bn
        coef[3 * n + 1, x] = 0.25 * (s * b1)
        coef[3 * n + 2, x] = 0.25 * (s * b2)

    def faces(x, carry):
        k_m, sy_m, sz_m = carry
        kap = full[0, x]
        u = y00[x]
        y01[x] = lroll(u, -1)
        y02[x] = lroll(u, 1)
        x_p = jnp.minimum(x + 1, PLANES - 1)
        bx, by, bz, sx, sy, sz = sums(x, x_p)
        face(0, x, kap + k_m, bx, sy + sy_m, sz + sz_m)
        face(1, x, kap + rroll(kap, 1), by, sz + rroll(sz, 1), sx + rroll(sx, 1))
        face(2, x, kap + lroll(kap, 1), bz, sx + lroll(sx, 1), sy + lroll(sy, 1))
        return kap, sy, sz

    for first, last in ((0, XE), (LOW, PLANES)):
        _, _, _, _, sy, sz = sums(first, first + 1)
        sweep(first, last, faces, (full[0, first], sy, sz), 4)

    def upper(x, carry):
        for k in range(3):
            coef_up[k, x] = lroll(coef[6 + k, x], -1)
        return carry

    sweep(0, PLANES, upper, 0, 8)

    arrays = ((y00, y01, y02), (y10, y11, y12), (y20, y21, y22))
    source, older = arrays[0], None
    for j in range(1, SECTIONS + 1):
        target = arrays[2 - j % 2]
        grow = (2.0 * j - 1.0) / j
        back = (j - 1.0) / j

        def rolled(u, u_p, u_m):
            down = rroll(u, 1)
            return down, rroll(u, -1) - down, u_p - u_m

        def flux_x(x, du, sum_y, sum_z):
            return coef[0, x] * du + coef[1, x] * sum_y + coef[2, x] * sum_z

        def plane(x, carry, source=source, older=older, target=target, grow=grow, back=back, j=j):
            dy, dz, fx, down = carry
            u, p, m = source[0][x], source[1][x], source[2][x]
            u_p, p_p, m_p = source[0][x + 1], source[1][x + 1], source[2][x + 1]
            down_p, dy_p, dz_p = rolled(u_p, p_p, m_p)
            fx_p = flux_x(x + 1, u_p - u, dy_p + dy, dz_p + dz)
            dx = u_p - source[0][x - 1]
            dx_zp = p_p - source[1][x - 1]
            dx_zm = m_p - source[2][x - 1]
            p_down, m_down = rroll(p, 1), rroll(m, 1)
            dy_zp = rroll(p, -1) - p_down
            dy_zm = rroll(m, -1) - m_down
            fy = (
                coef[3, x] * (u - down)
                + coef[4, x] * (dz + (p_down - m_down))
                + coef[5, x] * (dx + rroll(dx, 1))
            )
            fz = coef[6, x] * (u - m) + coef[7, x] * (dx + dx_zm) + coef[8, x] * (dy + dy_zm)
            fz_p = coef_up[0, x] * (p - u) + coef_up[1, x] * (dx_zp + dx) + coef_up[2, x] * (dy_zp + dy)
            rate = (fx_p - fx) + (rroll(fy, -1) - fy) + (fz_p - fz)
            new = u + rate
            if j > 1:
                new = grow * new - back * older[0][x]
            if j == SECTIONS:
                b = (SECTIONS * SECTIONS + SECTIONS - 2) / (2.0 * SECTIONS * (SECTIONS + 1))
                new = (1.0 - b) * y00[x] + b * new
            target[0][x] = new
            return (dy_p, dz_p, fx_p, down_p), new

        def start(x, source=source):
            u_m, u = source[0][x - 1], source[0][x]
            _, dy_m, dz_m = rolled(u_m, source[1][x - 1], source[2][x - 1])
            down, dy, dz = rolled(u, source[1][x], source[2][x])
            return dy, dz, flux_x(x, u - u_m, dy + dy_m, dz + dz_m), down

        def two(i, carry, target=target, plane=plane, j=j):
            x = j + 2 * i
            carry, *made = carry
            turned = [(lroll(u, -1), lroll(u, 1)) for u in made]
            carry, first = plane(x, carry)
            carry, second = plane(x + 1, carry)
            if j < SECTIONS:
                for k, (up, down) in enumerate(turned):
                    at = jnp.maximum(x - 2 + k, 0)
                    target[1][at] = up
                    target[2][at] = down
            return carry, first, second

        carry = start(j)
        _, *made = lax.fori_loop(0, (XE - 2 * j) // 2, two, (carry, carry[3], carry[3]))
        carry = start(LOW + 1)
        strip = []
        for x in range(LOW + 1, HIGH):
            carry, new = plane(x, carry)
            strip.append(new)
        if j < SECTIONS:
            for k, u in enumerate(made):
                target[1][XE - j - 2 + k] = lroll(u, -1)
                target[2][XE - j - 2 + k] = lroll(u, 1)
            for at, u, by in ((HIGH, strip[0], -WIDE), (LOW, strip[-1], WIDE)):
                target[0][at] = lroll(u, by)
                target[1][at] = lroll(u, by - 1)
                target[2][at] = lroll(u, by + 1)
            for k, u in enumerate(strip):
                target[1][LOW + 1 + k] = lroll(u, -1)
                target[2][LOW + 1 + k] = lroll(u, 1)
        source, older = target, source

    def seam(main, strip, g):
        return jnp.where(
            lane < LANES - 16, lroll(main, -8), lroll(strip, LANES - 16 - 8 - WIDE * g)
        )

    for x in range(W):
        g, k = divmod(W + x, XG)
        tout_ref[x] = seam(source[0][W + x, W : 2 * W], source[0][LOW + 1 + k, W : 2 * W], g)

    SPEED = 3
    strip = range(A_LOW + 1, A_HIGH)

    def within(i):
        return i + OFF if i < XA else i - A_LOW + LOW

    for i in (*range(XA), *strip):
        x = within(i)
        _, _, _, sx, sy, sz = sums(x, x + 1)
        field = 0.25 * (sx * sx + sy * sy + sz * sz)
        vx, vy, vz = aux[0, i], aux[1, i], aux[2, i]
        flow = jnp.sqrt(vx * vx + vy * vy + vz * vz)
        aux[SPEED, i] = flow + jnp.sqrt(GAMMA * y00[x] + field / aux[SPEED, i])
    for k in range(AUX):
        aux[k, A_LOW] = lroll(aux[k, A_HIGH - 1], WIDE)

    def by_axis(u, u_m, axis):
        if axis == 0:
            return u_m
        return rroll(u, 1) if axis == 1 else lroll(u, 1)

    for i in (*range(1, XA), *strip):
        for c in range(3):
            a, b = (c + 1) % 3, (c + 2) % 3

            def mean(f, i=i, a=a, b=b):
                if 0 in (a, b):
                    other = a + b
                    u = aux[f, i] + aux[f, i - 1]
                else:
                    other = 2
                    u = aux[f, i]
                    u = u + by_axis(u, None, 1)
                return 0.125 * (u + by_axis(u, None, other))

            va, vb, s = mean(a), mean(b), mean(SPEED)
            ecoef[4 * c, i] = vb - s
            ecoef[4 * c + 1, i] = vb + s
            ecoef[4 * c + 2, i] = s - va
            ecoef[4 * c + 3, i] = -s - va

    def fields(get, first, last):
        for i in (*range(first, last), *strip):
            for c in range(3):
                a, b = (c + 1) % 3, (c + 2) % 3
                ua, ub = get(a, i), get(b, i)
                ua_b = by_axis(ua, get(a, i - 1) if b == 0 else None, b)
                ub_a = by_axis(ub, get(b, i - 1) if a == 0 else None, a)
                edge[c, i] = (ecoef[4 * c, i] * ua + ecoef[4 * c + 1, i] * ua_b) + (
                    ecoef[4 * c + 2, i] * ub + ecoef[4 * c + 3, i] * ub_a
                )
        for c in range(1, 3):
            edge[c, A_HIGH] = lroll(edge[c, A_LOW + 1], -WIDE)

    def ahead(f, i, axis):
        if axis == 0:
            return edge[f, i + 1]
        u = edge[f, i]
        return rroll(u, -1) if axis == 1 else lroll(u, -1)

    def curl(d, i):
        e, f = (d + 1) % 3, (d + 2) % 3
        return (ahead(f, i, e) - edge[f, i]) - (ahead(e, i, f) - edge[e, i])

    fields(lambda d, i: full[1 + d, within(i)], 1, XA)
    for i in (*range(1, XA - 1), *strip):
        for d in range(3):
            mid[d, i] = full[1 + d, within(i)] - dt * curl(d, i)
    for d in range(1, 3):
        mid[d, A_LOW] = lroll(mid[d, A_HIGH - 1], WIDE)
    fields(lambda d, i: mid[d, i], 2, XA - 1)

    def final(d, i):
        u = 0.5 * (full[1 + d, within(i)] + (mid[d, i] - dt * curl(d, i)))
        return u[W : 2 * W]

    for d in range(3):
        ends = [final(d, i) for i in strip]
        for x in range(W):
            g, k = divmod(W + x, XG)
            bout_ref[d, x] = seam(final(d, x + AX), ends[k], g)


def exchange(first, second, axis):
    count = lax.axis_size(axis)
    swaps = [(i, i + 1) for i in range(0, count, 2)] + [(i + 1, i) for i in range(0, count, 2)]
    others = [((a + 1) % count, (b + 1) % count) for a, b in swaps]
    return lax.ppermute(first, axis, swaps), lax.ppermute(second, axis, others)


def on_core(kernel, out, *args, scratch=(), last=False):
    space = pl.BlockSpec(memory_space=pltpu.VMEM)
    shape = [
        jax.ShapeDtypeStruct(o, jnp.float32) if last else pltpu.VMEM(o, jnp.float32) for o in out
    ]
    return pl.pallas_call(
        kernel,
        out_shape=shape,
        in_specs=[space] * len(args),
        out_specs=[space] * len(out),
        scratch_shapes=[pltpu.VMEM(shape, jnp.float32) for shape in scratch],
        name=kernel.__name__,
    )(*args)


def held(*arrays):
    return [pltpu.with_memory_space_constraint(a, pltpu.VMEM) for a in arrays]


def on_device(t, diffusivity, b, v, rho):
    zs = lax.axis_size("gz")
    outer = lax.axis_size("gx_2") * lax.axis_size("gy")
    inner = lax.axis_size("gx_0") * lax.axis_size("gx_1")
    out = [(W, W, LANES), (zs, ZT, W, LANES)]
    kappa, edges = on_core(pack_z, out, t, diffusivity, b, v, rho)
    edges = lax.all_to_all(edges, "gz", 0, 0, tiled=True)
    kappa, edges = held(kappa, edges)
    out = [(SIDE, W, LANES)] * 2 + [((W + 1) * AUX, W, LANES), (outer, 1, LANES)]
    first, second, aux, low = on_core(pack_x, out, t, kappa, b, v, rho, edges)
    x_first, x_second = exchange(first, second, GX)
    low = lax.all_to_all(low, ("gx_2", "gy"), 0, 0, tiled=True)
    args = held(first, aux, x_first, x_second, low)
    out = [(YT, W, LANES)] * 2 + [(A_TILES, W, LANES), (inner, 1, LANES)]
    first, second, aux, low = on_core(pack_y, out, *args)
    y_first, y_second = exchange(first, second, "gy")
    low = lax.all_to_all(low, ("gx_0", "gx_1"), 0, 0, tiled=True)
    out = [(W, W, LANES), (3, W, W, LANES)]
    args = held(first, aux, y_first, y_second, low)
    return tuple(on_core(advance, out, *args, scratch=SCRATCH, last=True))


def solution(mesh):
    gx, gy, gz = (mesh.shape[axis] for axis in ("gx", "gy", "gz"))
    outer = 3 if gx % 6 == 0 else 1
    finer = Mesh(mesh.devices.reshape(outer, gx // outer // 2, 2, gy, gz), (*GX, "gy", "gz"))
    cell = P(GX, "gy", "gz")
    face = P(None, GX, "gy", "gz")
    return jax.shard_map(
        on_device,
        mesh=finer,
        in_specs=(cell, cell, face, face, cell),
        out_specs=(cell, face),
        check_vma=False,
    )
```

```python
import jax
import jax.numpy as jnp
from jax import lax
from jax.experimental import pallas as pl
from jax.experimental.pallas import tpu as pltpu
from jax.sharding import Mesh
from jax.sharding import PartitionSpec as P

SECTIONS = 8
GAMMA = 5.0 / 3.0
FACE_FLOOR = 0.25

GX = ("gx_0", "gx_1", "gx_2")
W = 8
LANES = 128
XE = 3 * W
WIDE = 4 * W
GROUPS = LANES // WIDE
XG = XE // GROUPS
LOW, HIGH = XE, XE + XG + 1
PLANES = HIGH + 1
ROWS = 3 * W
FULL = 5
AUX = 4
AX = 2
XA = W + 2 * AX
OFF = W - AX
A_LOW, A_HIGH = XA, XA + XG + 1
A_PLANES = A_HIGH + 1
ZT = (FULL + AUX) * W // 16 + 1
SPARE = LANES // 2
SIDE = FULL * W + AUX * AX + FULL + 1
A_TILES = AUX * (XA + XG)
Y_FULL = FULL * (XE + XG)
YT = Y_FULL + A_TILES // 4
SCRATCH = [(PLANES, ROWS, LANES)] * 9 + [
    (FULL - 1, PLANES, ROWS, LANES),
    (AUX, A_PLANES, ROWS, LANES),
    (9, PLANES, ROWS, LANES),
    (3, PLANES, ROWS, LANES),
    (12, A_PLANES, ROWS, LANES),
    (3, A_PLANES, ROWS, LANES),
    (3, A_PLANES, ROWS, LANES),
]
LATE = 5
FIRST_RATE = 4.0 / (SECTIONS * SECTIONS + SECTIONS - 2)
LIMIT = (SECTIONS * SECTIONS + SECTIONS - 2) / 16.0


def lane_ids(rows):
    return lax.broadcasted_iota(jnp.int32, (rows, LANES), 1)


def lroll(u, amount):
    return pltpu.roll(u, amount % LANES, 1)


def rroll(u, amount):
    return pltpu.roll(u, amount % u.shape[0], 0)


def lowest(u):
    return jnp.min(jnp.min(u, axis=0, keepdims=True), axis=1, keepdims=True)


def neighbours(axis):
    count = lax.axis_size(axis)
    at = lax.axis_index(axis)
    return lax.rem(at + count - 1, count), lax.rem(at + 1, count)


def is_odd(axis):
    return lax.rem(lax.axis_index(axis), 2) == 1


def piece(field, plane):
    return divmod(field * W + plane, 16)


def pack_z(t_ref, d_ref, b_ref, v_ref, r_ref, kap_ref, out_ref):
    t = t_ref[...]
    kappa = d_ref[...] * (t * t * jnp.sqrt(t))
    kap_ref[...] = kappa
    low = lowest(jnp.min(LIMIT / kappa, axis=0))
    lane = lane_ids(W)
    left, right = [], []
    for tile in range(ZT):
        below = above = jnp.broadcast_to(low, (W, LANES))
        for k in range(16):
            field, plane = divmod(tile * 16 + k, W)
            if field >= FULL + AUX:
                break
            if field == 0:
                u = t[plane]
            elif field == 1:
                u = kappa[plane]
            elif field < FULL:
                u = b_ref[field - 2, plane]
            else:
                u = v_ref[field - FULL, plane] if field < FULL + 3 else r_ref[plane]
            here = (lane >= 8 * k) & (lane < 8 * k + 8)
            below = jnp.where(here, lroll(u, 8 * k), below)
            above = jnp.where(here, lroll(u, 8 * k - (LANES - 8)), above)
        left.append(below)
        right.append(above)
    lo, _ = neighbours("gz")
    for slot in range(out_ref.shape[0]):
        for tile in range(ZT):
            out_ref[slot, tile] = jnp.where(lo == slot, left[tile], right[tile])


def pack_x(t_ref, k_ref, b_ref, v_ref, r_ref, z_ref, a_ref, o_ref, aux_ref, low_ref):
    odd = is_odd(GX)
    lo, hi = neighbours("gz")
    lane = lane_ids(W)
    left = [z_ref[lo, tile] for tile in range(ZT)]
    right = [z_ref[hi, tile] for tile in range(ZT)]
    up_ends = down_ends = jnp.zeros((W, LANES), jnp.float32)
    for field in range(FULL + AUX):
        ends = jnp.zeros((W, LANES), jnp.float32)
        for plane in range(W):
            if field < FULL:
                u = (t_ref, k_ref, b_ref.at[0], b_ref.at[1], b_ref.at[2])[field][plane]
            else:
                u = v_ref[field - FULL, plane] if field < FULL + 3 else r_ref[plane]
            tile, k = piece(field, plane)
            main = jnp.where(lane < 8, lroll(left[tile], -8 * k), lroll(u, 8))
            to = 16 * plane
            end = jnp.where(
                lane < to + 8, lroll(u, to + 8 - LANES), lroll(right[tile], to + 8 - 8 * k)
            )
            ends = jnp.where(lane < to, ends, end)
            if field < FULL:
                a_ref[field * W + plane] = main
                o_ref[field * W + plane] = main
                continue
            aux_ref[(field - FULL) * W + plane] = main
            at = FULL * W + (field - FULL) * AX
            if plane < AX:
                a_ref[at + plane] = main
                o_ref[at + plane] = main
            elif plane >= W - AX:
                i = at + plane - (W - AX)
                down = a_ref[i]
                a_ref[i] = jnp.where(odd, down, main)
                o_ref[i] = jnp.where(odd, main, down)
        if field < FULL:
            a_ref[FULL * W + AUX * AX + field] = ends
            o_ref[FULL * W + AUX * AX + field] = ends
        else:
            f = field - FULL
            aux_ref[AUX * W + f] = ends
            here = lane >= 32 * f
            down_ends = jnp.where(here, lroll(ends, 32 * f), down_ends)
            up_ends = jnp.where(here, lroll(ends, 32 * f - (LANES - 32)), up_ends)
    a_ref[SIDE - 1] = jnp.where(odd, down_ends, up_ends)
    o_ref[SIDE - 1] = jnp.where(odd, up_ends, down_ends)
    low = z_ref[0, ZT - 1]
    for slot in range(1, z_ref.shape[0]):
        low = jnp.minimum(low, z_ref[slot, ZT - 1])
    low = lowest(jnp.where(lane >= SPARE, low, jnp.max(low)))
    low_ref[...] = jnp.broadcast_to(low.reshape(1, 1, 1), low_ref.shape)


def pack_y(own_ref, ownaux_ref, xa_ref, xo_ref, min_ref, a_ref, o_ref, aux_ref, low_ref):
    odd_x, odd_y = is_odd(GX), is_odd("gy")
    lane = lane_ids(W)

    def below(i):
        return jnp.where(odd_x, xa_ref[i], xo_ref[i])

    def above(i):
        return jnp.where(odd_x, xo_ref[i], xa_ref[i])

    sides = (below, own_ref.__getitem__, above)

    def send(i, u):
        a_ref[i] = u
        o_ref[i] = u

    ends_at = FULL * W + AUX * AX
    for field in range(FULL):
        ends = [get(ends_at + field) for get in sides]
        mains = []
        for x in range(XE):
            part, at = divmod(x, W)
            mains.append(sides[part](field * W + at))
            send(field * XE + x, mains[x])
        for k in range(XG):
            strip = None
            for g in range(GROUPS):
                part, at = divmod(g * XG + k, W)
                to = g * WIDE
                new = jnp.where(
                    lane < to + 16,
                    lroll(mains[g * XG + k], to + 16 - LANES),
                    lroll(ends[part], to + 16 - 16 * at),
                )
                strip = jnp.where(lane < to, strip, new) if g else new
            send(FULL * XE + field * XG + k, strip)

    def put(i, u):
        aux_ref[i] = u
        tile, k = Y_FULL + i // 4, AX * (i % 4)
        up, down = u[W - AX : W], u[0:AX]
        a_ref[tile, k : k + AX] = jnp.where(odd_y, down, up)
        o_ref[tile, k : k + AX] = jnp.where(odd_y, up, down)

    outer = below(SIDE - 1), above(SIDE - 1)
    for field in range(AUX):
        mains, ends = [], []
        at = FULL * W + field * AX
        for i in range(XA):
            if i < AX:
                mains.append(below(at + i))
                ends.append((outer[0], field * AX + i))
            elif i < AX + W:
                mains.append(ownaux_ref[field * W + i - AX])
                ends.append((ownaux_ref[AUX * W + field], i - AX))
            else:
                mains.append(above(at + i - AX - W))
                ends.append((outer[1], field * AX + i - AX - W))
            put(field * XA + i, mains[i])
        for k in range(XG):
            strip = None
            for g in range(XA // XG):
                u, (end, at_end) = mains[g * XG + k], ends[g * XG + k]
                to = (g + OFF // XG) * WIDE
                new = lroll(u, to + 16 - LANES)
                strip = jnp.where(lane < to, strip, new) if g else new
                new = lroll(end, to + 16 - 16 * at_end)
                strip = jnp.where((lane >= to + 16) & (lane < to + 32), new, strip)
            put(AUX * XA + field * XG + k, strip)
    low = lowest(jnp.min(min_ref[...], axis=0))
    low_ref[...] = jnp.broadcast_to(low.reshape(1, 1, 1), low_ref.shape)


def sweep(first, last, body, carry, by):
    trips = (last - first) // by

    def several(i, carry):
        for k in range(by):
            carry = body(first + i * by + k, carry)
        return carry

    if trips:
        carry = lax.fori_loop(0, trips, several, carry)
    for x in range(first + trips * by, last):
        carry = body(x, carry)
    return carry


def advance(
    own_ref, aux_ref, ya_ref, yo_ref, low_ref, tout_ref, bout_ref,
    y00, y01, y02, y10, y11, y12, y20, y21, y22, full, aux, coef, coef_up, ecoef, edge, mid,
):
    lane = lane_ids(W)
    dt = lowest(jnp.min(low_ref[...], axis=0))
    odd = is_odd("gy")

    sides = (
        lambda i: jnp.where(odd, ya_ref[i], yo_ref[i]),
        own_ref.__getitem__,
        lambda i: jnp.where(odd, yo_ref[i], ya_ref[i]),
    )
    for field in range(FULL):
        to = y00 if field == 0 else full.at[field - 1]
        for x in range(XE + XG):
            i, plane = field * XE + x, x
            if x >= XE:
                i, plane = FULL * XE + field * XG + x - XE, x + 1
            for part in range(3):
                to[plane, part * W : part * W + W] = sides[part](i)
    for field in range(AUX):
        for x in range(XA + XG):
            i, plane = field * XA + x, x
            if x >= XA:
                i, plane = AUX * XA + field * XG + x - XA, x + 1
            tile, k = Y_FULL + i // 4, AX * (i % 4)
            for part in range(3):
                u = aux_ref[i] if part == 1 else jnp.tile(sides[part](tile)[k : k + AX], (4, 1))
                aux[field, plane, part * W : part * W + W] = u

    def beside(ref, low, high):
        ref[low] = lroll(ref[high - 1], WIDE)
        ref[high] = lroll(ref[low + 1], -WIDE)

    beside(y00, LOW, HIGH)
    for k in range(FULL - 1):
        beside(full.at[k], LOW, HIGH)

    def sums(x, x_p):
        bx, by, bz = full[1, x], full[2, x], full[3, x]
        sx = bx + full[1, x_p]
        sy = by + rroll(by, -1)
        sz = bz + lroll(bz, -1)
        return bx, by, bz, sx, sy, sz

    def face(n, x, kk, bn, b1, b2):
        b1, b2 = 0.25 * b1, 0.25 * b2
        q = bn * bn + b1 * b1 + b2 * b2
        s = (0.5 * FIRST_RATE * dt) * kk / jnp.maximum(q, FACE_FLOOR) * bn
        coef[3 * n, x] = s * bn
        coef[3 * n + 1, x] = 0.25 * (s * b1)
        coef[3 * n + 2, x] = 0.25 * (s * b2)

    def faces(x, carry):
        k_m, sy_m, sz_m = carry
        kap = full[0, x]
        u = y00[x]
        y01[x] = lroll(u, -1)
        y02[x] = lroll(u, 1)
        x_p = min(x + 1, PLANES - 1)
        bx, by, bz, sx, sy, sz = sums(x, x_p)
        face(0, x, kap + k_m, bx, sy + sy_m, sz + sz_m)
        face(1, x, kap + rroll(kap, 1), by, sz + rroll(sz, 1), sx + rroll(sx, 1))
        face(2, x, kap + lroll(kap, 1), bz, sx + lroll(sx, 1), sy + lroll(sy, 1))
        return kap, sy, sz

    for first, last in ((0, XE), (LOW, PLANES)):
        _, _, _, _, sy, sz = sums(first, first + 1)
        carry = full[0, first], sy, sz
        for x in range(first, last):
            carry = faces(x, carry)

    arrays = ((y00, y01, y02), (y10, y11, y12), (y20, y21, y22))
    source, older = arrays[0], None
    begun = []
    for j in range(1, SECTIONS + 1):
        target = arrays[2 - j % 2]
        grow = (2.0 * j - 1.0) / j
        back = (j - 1.0) / j

        def rolled(u, u_p, u_m):
            down = rroll(u, 1)
            return down, rroll(u, -1) - down, u_p - u_m

        def flux_x(x, du, sum_y, sum_z):
            return coef[0, x] * du + coef[1, x] * sum_y + coef[2, x] * sum_z

        def plane(x, carry, source=source):
            dy, dz, fx, down = carry
            u, p, m = source[0][x], source[1][x], source[2][x]
            u_p, p_p, m_p = source[0][x + 1], source[1][x + 1], source[2][x + 1]
            down_p, dy_p, dz_p = rolled(u_p, p_p, m_p)
            fx_p = flux_x(x + 1, u_p - u, dy_p + dy, dz_p + dz)
            dx = u_p - source[0][x - 1]
            dx_zm = m_p - source[2][x - 1]
            m_down = rroll(m, 1)
            dy_zm = rroll(m, -1) - m_down
            fy = (
                coef[3, x] * (u - down)
                + coef[4, x] * (dz + rroll(dz, 1))
                + coef[5, x] * (dx + rroll(dx, 1))
            )
            fz = coef[6, x] * (u - m) + coef[7, x] * (dx + dx_zm) + coef[8, x] * (dy + dy_zm)
            ahead_z = lroll(fz, -1)
            rate = (fx_p - fx) + (rroll(fy, -1) - fy) - fz
            return (dy_p, dz_p, fx_p, down_p), u + rate, ahead_z

        def finish(x, new, ahead_z, target=target, older=older, grow=grow, back=back, j=j):
            new = new + ahead_z
            if j > 1:
                new = grow * new - back * older[0][x]
            if j == SECTIONS:
                b = (SECTIONS * SECTIONS + SECTIONS - 2) / (2.0 * SECTIONS * (SECTIONS + 1))
                new = (1.0 - b) * y00[x] + b * new
            target[0][x] = new
            if j < SECTIONS:
                target[1][x] = lroll(new, -1)
                target[2][x] = lroll(new, 1)
            return new

        def start(x, source=source):
            u_m, u = source[0][x - 1], source[0][x]
            _, dy_m, dz_m = rolled(u_m, source[1][x - 1], source[2][x - 1])
            down, dy, dz = rolled(u, source[1][x], source[2][x])
            return dy, dz, flux_x(x, u - u_m, dy + dy_m, dz + dz_m), down

        strip = []

        def finish_strip(x, new, ahead_z, finish=finish, strip=strip, target=target, j=j):
            strip.append(finish(x, new, ahead_z))
            if x == HIGH - 1 and j < SECTIONS:
                for at, u, by in ((HIGH, strip[0], -WIDE), (LOW, strip[-1], WIDE)):
                    target[0][at] = lroll(u, by)
                    target[1][at] = lroll(u, by - 1)
                    target[2][at] = lroll(u, by + 1)

        for first, last, then in ((LOW + 1, HIGH, finish_strip), (j, XE - j, finish)):
            carry = start(first)
            for x in range(first, last):
                carry, *parts = plane(x, carry)
                begun.append((then, x, *parts))
                if len(begun) > LATE:
                    then_, *parts = begun.pop(0)
                    then_(*parts)
        source, older = target, source
    for then, *parts in begun:
        then(*parts)

    def seam(main, strip, g):
        return jnp.where(
            lane < LANES - 16, lroll(main, -8), lroll(strip, LANES - 16 - 8 - WIDE * g)
        )

    for x in range(W):
        g, k = divmod(W + x, XG)
        tout_ref[x] = seam(source[0][W + x, W : 2 * W], source[0][LOW + 1 + k, W : 2 * W], g)

    SPEED = 3
    strip = range(A_LOW + 1, A_HIGH)

    def within(i):
        return i + OFF if i < XA else i - A_LOW + LOW

    for i in (*range(XA), *strip):
        x = within(i)
        _, _, _, sx, sy, sz = sums(x, x + 1)
        field = 0.25 * (sx * sx + sy * sy + sz * sz)
        vx, vy, vz = aux[0, i], aux[1, i], aux[2, i]
        flow = jnp.sqrt(vx * vx + vy * vy + vz * vz)
        aux[SPEED, i] = flow + jnp.sqrt(GAMMA * y00[x] + field / aux[SPEED, i])
    for k in range(AUX):
        aux[k, A_LOW] = lroll(aux[k, A_HIGH - 1], WIDE)

    def by_axis(u, u_m, axis):
        if axis == 0:
            return u_m
        return rroll(u, 1) if axis == 1 else lroll(u, 1)

    for i in (*range(1, XA), *strip):
        for c in range(3):
            a, b = (c + 1) % 3, (c + 2) % 3

            def mean(f, i=i, a=a, b=b):
                if 0 in (a, b):
                    other = a + b
                    u = aux[f, i] + aux[f, i - 1]
                else:
                    other = 2
                    u = aux[f, i]
                    u = u + by_axis(u, None, 1)
                return 0.125 * (u + by_axis(u, None, other))

            va, vb, s = mean(a), mean(b), mean(SPEED)
            ecoef[4 * c, i] = vb - s
            ecoef[4 * c + 1, i] = vb + s
            ecoef[4 * c + 2, i] = s - va
            ecoef[4 * c + 3, i] = -s - va

    def fields(get, first, last):
        for i in (*range(first, last), *strip):
            for c in range(3):
                a, b = (c + 1) % 3, (c + 2) % 3
                ua, ub = get(a, i), get(b, i)
                ua_b = by_axis(ua, get(a, i - 1) if b == 0 else None, b)
                ub_a = by_axis(ub, get(b, i - 1) if a == 0 else None, a)
                edge[c, i] = (ecoef[4 * c, i] * ua + ecoef[4 * c + 1, i] * ua_b) + (
                    ecoef[4 * c + 2, i] * ub + ecoef[4 * c + 3, i] * ub_a
                )
        for c in range(1, 3):
            edge[c, A_HIGH] = lroll(edge[c, A_LOW + 1], -WIDE)

    def ahead(f, i, axis):
        if axis == 0:
            return edge[f, i + 1]
        u = edge[f, i]
        return rroll(u, -1) if axis == 1 else lroll(u, -1)

    def curl(d, i):
        e, f = (d + 1) % 3, (d + 2) % 3
        return (ahead(f, i, e) - edge[f, i]) - (ahead(e, i, f) - edge[e, i])

    fields(lambda d, i: full[1 + d, within(i)], 1, XA)
    for i in (*range(1, XA - 1), *strip):
        for d in range(3):
            mid[d, i] = full[1 + d, within(i)] - dt * curl(d, i)
    for d in range(1, 3):
        mid[d, A_LOW] = lroll(mid[d, A_HIGH - 1], WIDE)
    fields(lambda d, i: mid[d, i], 2, XA - 1)

    def final(d, i):
        u = 0.5 * (full[1 + d, within(i)] + (mid[d, i] - dt * curl(d, i)))
        return u[W : 2 * W]

    for d in range(3):
        ends = [final(d, i) for i in strip]
        for x in range(W):
            g, k = divmod(W + x, XG)
            bout_ref[d, x] = seam(final(d, x + AX), ends[k], g)


def exchange(first, second, axis):
    count = lax.axis_size(axis)
    swaps = [(i, i + 1) for i in range(0, count, 2)] + [(i + 1, i) for i in range(0, count, 2)]
    others = [((a + 1) % count, (b + 1) % count) for a, b in swaps]
    return lax.ppermute(first, axis, swaps), lax.ppermute(second, axis, others)


def on_core(kernel, out, *args, scratch=(), last=False):
    space = pl.BlockSpec(memory_space=pltpu.VMEM)
    shape = [
        jax.ShapeDtypeStruct(o, jnp.float32) if last else pltpu.VMEM(o, jnp.float32) for o in out
    ]
    return pl.pallas_call(
        kernel,
        out_shape=shape,
        in_specs=[space] * len(args),
        out_specs=[space] * len(out),
        scratch_shapes=[pltpu.VMEM(shape, jnp.float32) for shape in scratch],
        name=kernel.__name__,
    )(*args)


def held(*arrays):
    return [pltpu.with_memory_space_constraint(a, pltpu.VMEM) for a in arrays]


def on_device(t, diffusivity, b, v, rho):
    zs = lax.axis_size("gz")
    outer = lax.axis_size("gx_2") * lax.axis_size("gy")
    inner = lax.axis_size("gx_0") * lax.axis_size("gx_1")
    out = [(W, W, LANES), (zs, ZT, W, LANES)]
    kappa, edges = on_core(pack_z, out, t, diffusivity, b, v, rho)
    edges = lax.all_to_all(edges, "gz", 0, 0, tiled=True)
    kappa, edges = held(kappa, edges)
    out = [(SIDE, W, LANES)] * 2 + [((W + 1) * AUX, W, LANES), (outer, 1, LANES)]
    first, second, aux, low = on_core(pack_x, out, t, kappa, b, v, rho, edges)
    x_first, x_second = exchange(first, second, GX)
    low = lax.all_to_all(low, ("gx_2", "gy"), 0, 0, tiled=True)
    args = held(first, aux, x_first, x_second, low)
    out = [(YT, W, LANES)] * 2 + [(A_TILES, W, LANES), (inner, 1, LANES)]
    first, second, aux, low = on_core(pack_y, out, *args)
    y_first, y_second = exchange(first, second, "gy")
    low = lax.all_to_all(low, ("gx_0", "gx_1"), 0, 0, tiled=True)
    out = [(W, W, LANES), (3, W, W, LANES)]
    args = held(first, aux, y_first, y_second, low)
    return tuple(on_core(advance, out, *args, scratch=SCRATCH, last=True))


def solution(mesh):
    gx, gy, gz = (mesh.shape[axis] for axis in ("gx", "gy", "gz"))
    outer = 3 if gx % 6 == 0 else 1
    finer = Mesh(mesh.devices.reshape(outer, gx // outer // 2, 2, gy, gz), (*GX, "gy", "gz"))
    cell = P(GX, "gy", "gz")
    face = P(None, GX, "gy", "gz")
    return jax.shard_map(
        on_device,
        mesh=finer,
        in_specs=(cell, cell, face, face, cell),
        out_specs=(cell, face),
        check_vma=False,
    )
```

```python
import jax
import jax.numpy as jnp
from jax import lax
from jax.experimental import pallas as pl
from jax.experimental.pallas import tpu as pltpu
from jax.sharding import Mesh
from jax.sharding import PartitionSpec as P

SECTIONS = 8
GAMMA = 5.0 / 3.0
FACE_FLOOR = 0.25

GX = ("gx_0", "gx_1", "gx_2")
W = 8
LANES = 128
XE = 3 * W
WIDE = 4 * W
GROUPS = LANES // WIDE
XG = XE // GROUPS
LOW, HIGH = XE, XE + XG + 1
PLANES = HIGH + 1
ROWS = 3 * W
FULL = 5
AUX = 4
AX = 2
XA = W + 2 * AX
OFF = W - AX
A_LOW, A_HIGH = XA, XA + XG + 1
A_PLANES = A_HIGH + 1
ZT = (FULL + AUX) * W // 16 + 1
SPARE = LANES // 2
SIDE = FULL * W + AUX * AX + FULL + 1
A_TILES = AUX * (XA + XG)
Y_FULL = FULL * (XE + XG)
YT = Y_FULL + A_TILES // 4
SCRATCH = [(PLANES, ROWS, LANES)] * 12 + [
    (FULL - 1, PLANES, ROWS, LANES),
    (AUX, A_PLANES, ROWS, LANES),
    (9, PLANES, ROWS, LANES),
    (3, PLANES, ROWS, LANES),
    (12, A_PLANES, ROWS, LANES),
    (3, A_PLANES, ROWS, LANES),
    (3, A_PLANES, ROWS, LANES),
]
LATE = 5
FIRST_RATE = 4.0 / (SECTIONS * SECTIONS + SECTIONS - 2)
LIMIT = (SECTIONS * SECTIONS + SECTIONS - 2) / 16.0


def lane_ids(rows):
    return lax.broadcasted_iota(jnp.int32, (rows, LANES), 1)


def lroll(u, amount):
    return pltpu.roll(u, amount % LANES, 1)


def rroll(u, amount):
    return pltpu.roll(u, amount % u.shape[0], 0)


def lowest(u):
    return jnp.min(jnp.min(u, axis=0, keepdims=True), axis=1, keepdims=True)


def neighbours(axis):
    count = lax.axis_size(axis)
    at = lax.axis_index(axis)
    return lax.rem(at + count - 1, count), lax.rem(at + 1, count)


def is_odd(axis):
    return lax.rem(lax.axis_index(axis), 2) == 1


def piece(field, plane):
    return divmod(field * W + plane, 16)


def pack_z(t_ref, d_ref, b_ref, v_ref, r_ref, all_ref, out_ref):
    t = t_ref[...]
    kappa = d_ref[...] * (t * t * jnp.sqrt(t))
    low = lowest(jnp.min(LIMIT / kappa, axis=0))
    lane = lane_ids(W)
    left, right = [], []
    for tile in range(ZT):
        below = above = jnp.broadcast_to(low, (W, LANES))
        for k in range(16):
            field, plane = divmod(tile * 16 + k, W)
            if field >= FULL + AUX:
                break
            if field == 0:
                u = t[plane]
            elif field == 1:
                u = kappa[plane]
            elif field < FULL:
                u = b_ref[field - 2, plane]
            else:
                u = v_ref[field - FULL, plane] if field < FULL + 3 else r_ref[plane]
            all_ref[field * W + plane] = u
            here = (lane >= 8 * k) & (lane < 8 * k + 8)
            below = jnp.where(here, lroll(u, 8 * k), below)
            above = jnp.where(here, lroll(u, 8 * k - (LANES - 8)), above)
        left.append(below)
        right.append(above)
    lo, _ = neighbours("gz")
    for slot in range(out_ref.shape[0]):
        for tile in range(ZT):
            out_ref[slot, tile] = jnp.where(lo == slot, left[tile], right[tile])


def pack_x(all_ref, z_ref, a_ref, o_ref, aux_ref, low_ref):
    odd = is_odd(GX)
    lo, hi = neighbours("gz")
    lane = lane_ids(W)
    left = [z_ref[lo, tile] for tile in range(ZT)]
    right = [z_ref[hi, tile] for tile in range(ZT)]
    up_ends = down_ends = jnp.zeros((W, LANES), jnp.float32)
    for field in range(FULL + AUX):
        ends = jnp.zeros((W, LANES), jnp.float32)
        for plane in range(W):
            u = all_ref[field * W + plane]
            tile, k = piece(field, plane)
            main = jnp.where(lane < 8, lroll(left[tile], -8 * k), lroll(u, 8))
            to = 16 * plane
            end = jnp.where(
                lane < to + 8, lroll(u, to + 8 - LANES), lroll(right[tile], to + 8 - 8 * k)
            )
            ends = jnp.where(lane < to, ends, end)
            if field < FULL:
                a_ref[field * W + plane] = main
                o_ref[field * W + plane] = main
                continue
            aux_ref[(field - FULL) * W + plane] = main
            at = FULL * W + (field - FULL) * AX
            if plane < AX:
                a_ref[at + plane] = main
                o_ref[at + plane] = main
            elif plane >= W - AX:
                i = at + plane - (W - AX)
                down = a_ref[i]
                a_ref[i] = jnp.where(odd, down, main)
                o_ref[i] = jnp.where(odd, main, down)
        if field < FULL:
            a_ref[FULL * W + AUX * AX + field] = ends
            o_ref[FULL * W + AUX * AX + field] = ends
        else:
            f = field - FULL
            aux_ref[AUX * W + f] = ends
            here = lane >= 32 * f
            down_ends = jnp.where(here, lroll(ends, 32 * f), down_ends)
            up_ends = jnp.where(here, lroll(ends, 32 * f - (LANES - 32)), up_ends)
    a_ref[SIDE - 1] = jnp.where(odd, down_ends, up_ends)
    o_ref[SIDE - 1] = jnp.where(odd, up_ends, down_ends)
    low = z_ref[0, ZT - 1]
    for slot in range(1, z_ref.shape[0]):
        low = jnp.minimum(low, z_ref[slot, ZT - 1])
    low = lowest(jnp.where(lane >= SPARE, low, jnp.max(low)))
    low_ref[...] = jnp.broadcast_to(low.reshape(1, 1, 1), low_ref.shape)


def pack_y(own_ref, ownaux_ref, xa_ref, xo_ref, min_ref, a_ref, o_ref, aux_ref, low_ref):
    odd_x, odd_y = is_odd(GX), is_odd("gy")
    lane = lane_ids(W)

    def below(i):
        return jnp.where(odd_x, xa_ref[i], xo_ref[i])

    def above(i):
        return jnp.where(odd_x, xo_ref[i], xa_ref[i])

    sides = (below, own_ref.__getitem__, above)

    def send(i, u):
        a_ref[i] = u
        o_ref[i] = u

    ends_at = FULL * W + AUX * AX
    for field in range(FULL):
        ends = [get(ends_at + field) for get in sides]
        mains = []
        for x in range(XE):
            part, at = divmod(x, W)
            mains.append(sides[part](field * W + at))
            send(field * XE + x, mains[x])
        for k in range(XG):
            strip = None
            for g in range(GROUPS):
                part, at = divmod(g * XG + k, W)
                to = g * WIDE
                new = jnp.where(
                    lane < to + 16,
                    lroll(mains[g * XG + k], to + 16 - LANES),
                    lroll(ends[part], to + 16 - 16 * at),
                )
                strip = jnp.where(lane < to, strip, new) if g else new
            send(FULL * XE + field * XG + k, strip)

    def put(i, u):
        aux_ref[i] = u
        tile, k = Y_FULL + i // 4, AX * (i % 4)
        up, down = u[W - AX : W], u[0:AX]
        a_ref[tile, k : k + AX] = jnp.where(odd_y, down, up)
        o_ref[tile, k : k + AX] = jnp.where(odd_y, up, down)

    outer = below(SIDE - 1), above(SIDE - 1)
    for field in range(AUX):
        mains, ends = [], []
        at = FULL * W + field * AX
        for i in range(XA):
            if i < AX:
                mains.append(below(at + i))
                ends.append((outer[0], field * AX + i))
            elif i < AX + W:
                mains.append(ownaux_ref[field * W + i - AX])
                ends.append((ownaux_ref[AUX * W + field], i - AX))
            else:
                mains.append(above(at + i - AX - W))
                ends.append((outer[1], field * AX + i - AX - W))
            put(field * XA + i, mains[i])
        for k in range(XG):
            strip = None
            for g in range(XA // XG):
                u, (end, at_end) = mains[g * XG + k], ends[g * XG + k]
                to = (g + OFF // XG) * WIDE
                new = lroll(u, to + 16 - LANES)
                strip = jnp.where(lane < to, strip, new) if g else new
                new = lroll(end, to + 16 - 16 * at_end)
                strip = jnp.where((lane >= to + 16) & (lane < to + 32), new, strip)
            put(AUX * XA + field * XG + k, strip)
    low = lowest(jnp.min(min_ref[...], axis=0))
    low_ref[...] = jnp.broadcast_to(low.reshape(1, 1, 1), low_ref.shape)


def sweep(first, last, body, carry, by):
    trips = (last - first) // by

    def several(i, carry):
        for k in range(by):
            carry = body(first + i * by + k, carry)
        return carry

    if trips:
        carry = lax.fori_loop(0, trips, several, carry)
    for x in range(first + trips * by, last):
        carry = body(x, carry)
    return carry


def advance(
    own_ref, aux_ref, ya_ref, yo_ref, low_ref, tout_ref, bout_ref,
    y00, y01, y02, y03, y10, y11, y12, y13, y20, y21, y22, y23, full, aux, coef, coef_up, ecoef, edge, mid,
):
    lane = lane_ids(W)
    dt = lowest(jnp.min(low_ref[...], axis=0))
    odd = is_odd("gy")

    sides = (
        lambda i: jnp.where(odd, ya_ref[i], yo_ref[i]),
        own_ref.__getitem__,
        lambda i: jnp.where(odd, yo_ref[i], ya_ref[i]),
    )
    for field in range(FULL):
        to = y00 if field == 0 else full.at[field - 1]
        for x in range(XE + XG):
            i, plane = field * XE + x, x
            if x >= XE:
                i, plane = FULL * XE + field * XG + x - XE, x + 1
            for part in range(3):
                to[plane, part * W : part * W + W] = sides[part](i)
    for field in range(AUX):
        for x in range(XA + XG):
            i, plane = field * XA + x, x
            if x >= XA:
                i, plane = AUX * XA + field * XG + x - XA, x + 1
            tile, k = Y_FULL + i // 4, AX * (i % 4)
            for part in range(3):
                u = aux_ref[i] if part == 1 else jnp.tile(sides[part](tile)[k : k + AX], (4, 1))
                aux[field, plane, part * W : part * W + W] = u

    def beside(ref, low, high):
        ref[low] = lroll(ref[high - 1], WIDE)
        ref[high] = lroll(ref[low + 1], -WIDE)

    beside(y00, LOW, HIGH)
    for k in range(FULL - 1):
        beside(full.at[k], LOW, HIGH)

    def sums(x, x_p):
        bx, by, bz = full[1, x], full[2, x], full[3, x]
        sx = bx + full[1, x_p]
        sy = by + rroll(by, -1)
        sz = bz + lroll(bz, -1)
        return bx, by, bz, sx, sy, sz

    def face(n, x, kk, bn, b1, b2):
        b1, b2 = 0.25 * b1, 0.25 * b2
        q = bn * bn + b1 * b1 + b2 * b2
        s = (0.5 * FIRST_RATE * dt) * kk / jnp.maximum(q, FACE_FLOOR) * bn
        coef[3 * n, x] = s * bn
        coef[3 * n + 1, x] = 0.25 * (s * b1)
        coef[3 * n + 2, x] = 0.25 * (s * b2)

    def faces(x, carry):
        k_m, sy_m, sz_m = carry
        kap = full[0, x]
        u = y00[x]
        y01[x] = lroll(u, -1)
        y02[x] = lroll(u, 1)
        y03[x] = lroll(rroll(u, -1) - rroll(u, 1), 1)
        x_p = min(x + 1, PLANES - 1)
        bx, by, bz, sx, sy, sz = sums(x, x_p)
        face(0, x, kap + k_m, bx, sy + sy_m, sz + sz_m)
        face(1, x, kap + rroll(kap, 1), by, sz + rroll(sz, 1), sx + rroll(sx, 1))
        face(2, x, kap + lroll(kap, 1), bz, sx + lroll(sx, 1), sy + lroll(sy, 1))
        return kap, sy, sz

    for first, last in ((0, XE), (LOW, PLANES)):
        _, _, _, _, sy, sz = sums(first, first + 1)
        carry = full[0, first], sy, sz
        for x in range(first, last):
            carry = faces(x, carry)

    arrays = ((y00, y01, y02, y03), (y10, y11, y12, y13), (y20, y21, y22, y23))
    source, older = arrays[0], None
    begun = []
    for j in range(1, SECTIONS + 1):
        target = arrays[2 - j % 2]
        grow = (2.0 * j - 1.0) / j
        back = (j - 1.0) / j

        def rolled(u, u_p, u_m):
            down = rroll(u, 1)
            return down, rroll(u, -1) - down, u_p - u_m

        def flux_x(x, du, sum_y, sum_z):
            return coef[0, x] * du + coef[1, x] * sum_y + coef[2, x] * sum_z

        def plane(x, carry, source=source):
            dy, dz, fx, down = carry
            u, p, m = source[0][x], source[1][x], source[2][x]
            u_p, p_p, m_p = source[0][x + 1], source[1][x + 1], source[2][x + 1]
            down_p, dy_p, dz_p = rolled(u_p, p_p, m_p)
            fx_p = flux_x(x + 1, u_p - u, dy_p + dy, dz_p + dz)
            dx = u_p - source[0][x - 1]
            dx_zm = m_p - source[2][x - 1]
            dy_zm = source[3][x]
            fy = (
                coef[3, x] * (u - down)
                + coef[4, x] * (dz + rroll(dz, 1))
                + coef[5, x] * (dx + rroll(dx, 1))
            )
            fz = coef[6, x] * (u - m) + coef[7, x] * (dx + dx_zm) + coef[8, x] * (dy + dy_zm)
            ahead_z = lroll(fz, -1)
            rate = (fx_p - fx) + (rroll(fy, -1) - fy) - fz
            return (dy_p, dz_p, fx_p, down_p), u + rate, ahead_z

        def finish(x, new, ahead_z, target=target, older=older, grow=grow, back=back, j=j):
            new = new + ahead_z
            if j > 1:
                new = grow * new - back * older[0][x]
            if j == SECTIONS:
                b = (SECTIONS * SECTIONS + SECTIONS - 2) / (2.0 * SECTIONS * (SECTIONS + 1))
                new = (1.0 - b) * y00[x] + b * new
            if j == SECTIONS:
                target[0][x, W : 2 * W] = new[W : 2 * W]
            else:
                target[0][x] = new
                target[1][x] = lroll(new, -1)
                target[2][x] = lroll(new, 1)
                target[3][x] = lroll(rroll(new, -1) - rroll(new, 1), 1)
            return new

        def start(x, source=source):
            u_m, u = source[0][x - 1], source[0][x]
            _, dy_m, dz_m = rolled(u_m, source[1][x - 1], source[2][x - 1])
            down, dy, dz = rolled(u, source[1][x], source[2][x])
            return dy, dz, flux_x(x, u - u_m, dy + dy_m, dz + dz_m), down

        strip = []

        def finish_strip(x, new, ahead_z, finish=finish, strip=strip, target=target, j=j):
            strip.append(finish(x, new, ahead_z))
            if x == HIGH - 1 and j < SECTIONS:
                for at, u, by in ((HIGH, strip[0], -WIDE), (LOW, strip[-1], WIDE)):
                    target[0][at] = lroll(u, by)
                    target[1][at] = lroll(u, by - 1)
                    target[2][at] = lroll(u, by + 1)

        for first, last, then in ((LOW + 1, HIGH, finish_strip), (j, XE - j, finish)):
            carry = start(first)
            for x in range(first, last):
                carry, *parts = plane(x, carry)
                begun.append((then, x, *parts))
                if len(begun) > LATE:
                    then_, *parts = begun.pop(0)
                    then_(*parts)
        source, older = target, source
    for then, *parts in begun:
        then(*parts)

    def seam(main, strip, g):
        return jnp.where(
            lane < LANES - 16, lroll(main, -8), lroll(strip, LANES - 16 - 8 - WIDE * g)
        )

    for x in range(W):
        g, k = divmod(W + x, XG)
        tout_ref[x] = seam(source[0][W + x, W : 2 * W], source[0][LOW + 1 + k, W : 2 * W], g)

    SPEED = 3
    strip = range(A_LOW + 1, A_HIGH)

    def within(i):
        return i + OFF if i < XA else i - A_LOW + LOW

    for i in (*range(XA), *strip):
        x = within(i)
        _, _, _, sx, sy, sz = sums(x, x + 1)
        field = 0.25 * (sx * sx + sy * sy + sz * sz)
        vx, vy, vz = aux[0, i], aux[1, i], aux[2, i]
        flow = jnp.sqrt(vx * vx + vy * vy + vz * vz)
        aux[SPEED, i] = flow + jnp.sqrt(GAMMA * y00[x] + field / aux[SPEED, i])
    for k in range(AUX):
        aux[k, A_LOW] = lroll(aux[k, A_HIGH - 1], WIDE)

    def by_axis(u, u_m, axis):
        if axis == 0:
            return u_m
        return rroll(u, 1) if axis == 1 else lroll(u, 1)

    for i in (*range(1, XA), *strip):
        for c in range(3):
            a, b = (c + 1) % 3, (c + 2) % 3

            def mean(f, i=i, a=a, b=b):
                if 0 in (a, b):
                    other = a + b
                    u = aux[f, i] + aux[f, i - 1]
                else:
                    other = 2
                    u = aux[f, i]
                    u = u + by_axis(u, None, 1)
                return 0.125 * (u + by_axis(u, None, other))

            va, vb, s = mean(a), mean(b), mean(SPEED)
            ecoef[4 * c, i] = vb - s
            ecoef[4 * c + 1, i] = vb + s
            ecoef[4 * c + 2, i] = s - va
            ecoef[4 * c + 3, i] = -s - va

    def fields(get, first, last):
        for i in (*range(first, last), *strip):
            for c in range(3):
                a, b = (c + 1) % 3, (c + 2) % 3
                ua, ub = get(a, i), get(b, i)
                ua_b = by_axis(ua, get(a, i - 1) if b == 0 else None, b)
                ub_a = by_axis(ub, get(b, i - 1) if a == 0 else None, a)
                edge[c, i] = (ecoef[4 * c, i] * ua + ecoef[4 * c + 1, i] * ua_b) + (
                    ecoef[4 * c + 2, i] * ub + ecoef[4 * c + 3, i] * ub_a
                )
        for c in range(1, 3):
            edge[c, A_HIGH] = lroll(edge[c, A_LOW + 1], -WIDE)

    def ahead(f, i, axis):
        if axis == 0:
            return edge[f, i + 1]
        u = edge[f, i]
        return rroll(u, -1) if axis == 1 else lroll(u, -1)

    def curl(d, i):
        e, f = (d + 1) % 3, (d + 2) % 3
        return (ahead(f, i, e) - edge[f, i]) - (ahead(e, i, f) - edge[e, i])

    fields(lambda d, i: full[1 + d, within(i)], 1, XA)
    for i in (*range(1, XA - 1), *strip):
        for d in range(3):
            mid[d, i] = full[1 + d, within(i)] - dt * curl(d, i)
    for d in range(1, 3):
        mid[d, A_LOW] = lroll(mid[d, A_HIGH - 1], WIDE)
    fields(lambda d, i: mid[d, i], 2, XA - 1)

    def final(d, i):
        u = 0.5 * (full[1 + d, within(i)] + (mid[d, i] - dt * curl(d, i)))
        return u[W : 2 * W]

    for d in range(3):
        ends = [final(d, i) for i in strip]
        for x in range(W):
            g, k = divmod(W + x, XG)
            bout_ref[d, x] = seam(final(d, x + AX), ends[k], g)


def exchange(first, second, axis):
    count = lax.axis_size(axis)
    swaps = [(i, i + 1) for i in range(0, count, 2)] + [(i + 1, i) for i in range(0, count, 2)]
    others = [((a + 1) % count, (b + 1) % count) for a, b in swaps]
    return lax.ppermute(first, axis, swaps), lax.ppermute(second, axis, others)


def on_core(kernel, out, *args, scratch=(), last=False):
    space = pl.BlockSpec(memory_space=pltpu.VMEM)
    shape = [
        jax.ShapeDtypeStruct(o, jnp.float32) if last else pltpu.VMEM(o, jnp.float32) for o in out
    ]
    return pl.pallas_call(
        kernel,
        out_shape=shape,
        in_specs=[space] * len(args),
        out_specs=[space] * len(out),
        scratch_shapes=[pltpu.VMEM(shape, jnp.float32) for shape in scratch],
        name=kernel.__name__,
    )(*args)


def held(*arrays):
    return [pltpu.with_memory_space_constraint(a, pltpu.VMEM) for a in arrays]


def on_device(t, diffusivity, b, v, rho):
    zs = lax.axis_size("gz")
    outer = lax.axis_size("gx_2") * lax.axis_size("gy")
    inner = lax.axis_size("gx_0") * lax.axis_size("gx_1")
    out = [((FULL + AUX) * W, W, LANES), (zs, ZT, W, LANES)]
    cells, edges = on_core(pack_z, out, t, diffusivity, b, v, rho)
    edges = lax.all_to_all(edges, "gz", 0, 0, tiled=True)
    cells, edges = held(cells, edges)
    out = [(SIDE, W, LANES)] * 2 + [((W + 1) * AUX, W, LANES), (outer, 1, LANES)]
    first, second, aux, low = on_core(pack_x, out, cells, edges)
    x_first, x_second = exchange(first, second, GX)
    low = lax.all_to_all(low, ("gx_2", "gy"), 0, 0, tiled=True)
    args = held(first, aux, x_first, x_second, low)
    out = [(YT, W, LANES)] * 2 + [(A_TILES, W, LANES), (inner, 1, LANES)]
    first, second, aux, low = on_core(pack_y, out, *args)
    y_first, y_second = exchange(first, second, "gy")
    low = lax.all_to_all(low, ("gx_0", "gx_1"), 0, 0, tiled=True)
    out = [(W, W, LANES), (3, W, W, LANES)]
    args = held(first, aux, y_first, y_second, low)
    return tuple(on_core(advance, out, *args, scratch=SCRATCH, last=True))


def solution(mesh):
    gx, gy, gz = (mesh.shape[axis] for axis in ("gx", "gy", "gz"))
    outer = 3 if gx % 6 == 0 else 1
    finer = Mesh(mesh.devices.reshape(outer, gx // outer // 2, 2, gy, gz), (*GX, "gy", "gz"))
    cell = P(GX, "gy", "gz")
    face = P(None, GX, "gy", "gz")
    return jax.shard_map(
        on_device,
        mesh=finer,
        in_specs=(cell, cell, face, face, cell),
        out_specs=(cell, face),
        check_vma=False,
    )
```

```python
import jax
import jax.numpy as jnp
from jax import lax
from jax.experimental import pallas as pl
from jax.experimental.pallas import tpu as pltpu
from jax.sharding import Mesh
from jax.sharding import PartitionSpec as P

SECTIONS = 8
GAMMA = 5.0 / 3.0
FACE_FLOOR = 0.25

GX = ("gx_0", "gx_1", "gx_2")
W = 8
LANES = 128
XE = 3 * W
WIDE = 4 * W
GROUPS = LANES // WIDE
XG = XE // GROUPS
LOW, HIGH = XE, XE + XG + 1
PLANES = HIGH + 1
ROWS = 3 * W
FULL = 5
AUX = 4
AX = 2
XA = W + 2 * AX
OFF = W - AX
A_LOW, A_HIGH = XA, XA + XG + 1
A_PLANES = A_HIGH + 1
ZT = (FULL + AUX) * W // 16 + 1
SPARE = LANES // 2
SIDE = FULL * W + AUX * AX + FULL + 1
A_TILES = AUX * (XA + XG)
Y_FULL = FULL * (XE + XG)
YT = Y_FULL + A_TILES // 4
GRANT = 28 << 20
SCRATCH = [(PLANES, ROWS, LANES)] * 12 + [
    (FULL - 1, PLANES, ROWS, LANES),
    (AUX, A_PLANES, ROWS, LANES),
    (9, PLANES, ROWS, LANES),
    (3, PLANES, ROWS, LANES),
    (12, A_PLANES, ROWS, LANES),
    (3, A_PLANES, ROWS, LANES),
    (3, A_PLANES, ROWS, LANES),
]
LATE = 5
FIRST_RATE = 4.0 / (SECTIONS * SECTIONS + SECTIONS - 2)
LIMIT = (SECTIONS * SECTIONS + SECTIONS - 2) / 16.0


def lane_ids(rows):
    return lax.broadcasted_iota(jnp.int32, (rows, LANES), 1)


def lroll(u, amount):
    return pltpu.roll(u, amount % LANES, 1)


def rroll(u, amount):
    return pltpu.roll(u, amount % u.shape[0], 0)


def lowest(u):
    return jnp.min(jnp.min(u, axis=0, keepdims=True), axis=1, keepdims=True)


def neighbours(axis):
    count = lax.axis_size(axis)
    at = lax.axis_index(axis)
    return lax.rem(at + count - 1, count), lax.rem(at + 1, count)


def is_odd(axis):
    return lax.rem(lax.axis_index(axis), 2) == 1


def piece(field, plane):
    return divmod(field * W + plane, 16)


def pack_z(t_ref, d_ref, b_ref, v_ref, r_ref, all_ref, out_ref):
    t = t_ref[...]
    kappa = d_ref[...] * (t * t * jnp.sqrt(t))
    low = lowest(jnp.min(LIMIT / kappa, axis=0))
    lane = lane_ids(W)
    left, right = [], []
    for tile in range(ZT):
        below = above = jnp.broadcast_to(low, (W, LANES))
        for k in range(16):
            field, plane = divmod(tile * 16 + k, W)
            if field >= FULL + AUX:
                break
            if field == 0:
                u = t[plane]
            elif field == 1:
                u = kappa[plane]
            elif field < FULL:
                u = b_ref[field - 2, plane]
            else:
                u = v_ref[field - FULL, plane] if field < FULL + 3 else r_ref[plane]
            all_ref[field * W + plane] = u
            here = (lane >= 8 * k) & (lane < 8 * k + 8)
            below = jnp.where(here, lroll(u, 8 * k), below)
            above = jnp.where(here, lroll(u, 8 * k - (LANES - 8)), above)
        left.append(below)
        right.append(above)
    lo, _ = neighbours("gz")
    for slot in range(out_ref.shape[0]):
        for tile in range(ZT):
            out_ref[slot, tile] = jnp.where(lo == slot, left[tile], right[tile])


def pack_x(all_ref, z_ref, a_ref, o_ref, aux_ref, low_ref):
    odd = is_odd(GX)
    lo, hi = neighbours("gz")
    lane = lane_ids(W)
    left = [z_ref[lo, tile] for tile in range(ZT)]
    right = [z_ref[hi, tile] for tile in range(ZT)]
    up_ends = down_ends = jnp.zeros((W, LANES), jnp.float32)
    for field in range(FULL + AUX):
        ends = jnp.zeros((W, LANES), jnp.float32)
        for plane in range(W):
            u = all_ref[field * W + plane]
            tile, k = piece(field, plane)
            main = jnp.where(lane < 8, lroll(left[tile], -8 * k), lroll(u, 8))
            to = 16 * plane
            end = jnp.where(
                lane < to + 8, lroll(u, to + 8 - LANES), lroll(right[tile], to + 8 - 8 * k)
            )
            ends = jnp.where(lane < to, ends, end)
            if field < FULL:
                a_ref[field * W + plane] = main
                o_ref[field * W + plane] = main
                continue
            aux_ref[(field - FULL) * W + plane] = main
            at = FULL * W + (field - FULL) * AX
            if plane < AX:
                a_ref[at + plane] = main
                o_ref[at + plane] = main
            elif plane >= W - AX:
                i = at + plane - (W - AX)
                down = a_ref[i]
                a_ref[i] = jnp.where(odd, down, main)
                o_ref[i] = jnp.where(odd, main, down)
        if field < FULL:
            a_ref[FULL * W + AUX * AX + field] = ends
            o_ref[FULL * W + AUX * AX + field] = ends
        else:
            f = field - FULL
            aux_ref[AUX * W + f] = ends
            here = lane >= 32 * f
            down_ends = jnp.where(here, lroll(ends, 32 * f), down_ends)
            up_ends = jnp.where(here, lroll(ends, 32 * f - (LANES - 32)), up_ends)
    a_ref[SIDE - 1] = jnp.where(odd, down_ends, up_ends)
    o_ref[SIDE - 1] = jnp.where(odd, up_ends, down_ends)
    low = z_ref[0, ZT - 1]
    for slot in range(1, z_ref.shape[0]):
        low = jnp.minimum(low, z_ref[slot, ZT - 1])
    low = lowest(jnp.where(lane >= SPARE, low, jnp.max(low)))
    low_ref[...] = jnp.broadcast_to(low.reshape(1, 1, 1), low_ref.shape)


def pack_y(own_ref, ownaux_ref, xa_ref, xo_ref, min_ref, a_ref, o_ref, aux_ref, low_ref):
    odd_x, odd_y = is_odd(GX), is_odd("gy")
    lane = lane_ids(W)

    def below(i):
        return jnp.where(odd_x, xa_ref[i], xo_ref[i])

    def above(i):
        return jnp.where(odd_x, xo_ref[i], xa_ref[i])

    sides = (below, own_ref.__getitem__, above)

    def send(i, u):
        a_ref[i] = u
        o_ref[i] = u

    ends_at = FULL * W + AUX * AX
    for field in range(FULL):
        ends = [get(ends_at + field) for get in sides]
        mains = []
        for x in range(XE):
            part, at = divmod(x, W)
            mains.append(sides[part](field * W + at))
            send(field * XE + x, mains[x])
        for k in range(XG):
            strip = None
            for g in range(GROUPS):
                part, at = divmod(g * XG + k, W)
                to = g * WIDE
                new = jnp.where(
                    lane < to + 16,
                    lroll(mains[g * XG + k], to + 16 - LANES),
                    lroll(ends[part], to + 16 - 16 * at),
                )
                strip = jnp.where(lane < to, strip, new) if g else new
            send(FULL * XE + field * XG + k, strip)

    def put(i, u):
        aux_ref[i] = u
        tile, k = Y_FULL + i // 4, AX * (i % 4)
        up, down = u[W - AX : W], u[0:AX]
        a_ref[tile, k : k + AX] = jnp.where(odd_y, down, up)
        o_ref[tile, k : k + AX] = jnp.where(odd_y, up, down)

    outer = below(SIDE - 1), above(SIDE - 1)
    for field in range(AUX):
        mains, ends = [], []
        at = FULL * W + field * AX
        for i in range(XA):
            if i < AX:
                mains.append(below(at + i))
                ends.append((outer[0], field * AX + i))
            elif i < AX + W:
                mains.append(ownaux_ref[field * W + i - AX])
                ends.append((ownaux_ref[AUX * W + field], i - AX))
            else:
                mains.append(above(at + i - AX - W))
                ends.append((outer[1], field * AX + i - AX - W))
            put(field * XA + i, mains[i])
        for k in range(XG):
            strip = None
            for g in range(XA // XG):
                u, (end, at_end) = mains[g * XG + k], ends[g * XG + k]
                to = (g + OFF // XG) * WIDE
                new = lroll(u, to + 16 - LANES)
                strip = jnp.where(lane < to, strip, new) if g else new
                new = lroll(end, to + 16 - 16 * at_end)
                strip = jnp.where((lane >= to + 16) & (lane < to + 32), new, strip)
            put(AUX * XA + field * XG + k, strip)
    low = lowest(jnp.min(min_ref[...], axis=0))
    low_ref[...] = jnp.broadcast_to(low.reshape(1, 1, 1), low_ref.shape)


def sweep(first, last, body, carry, by):
    trips = (last - first) // by

    def several(i, carry):
        for k in range(by):
            carry = body(first + i * by + k, carry)
        return carry

    if trips:
        carry = lax.fori_loop(0, trips, several, carry)
    for x in range(first + trips * by, last):
        carry = body(x, carry)
    return carry


def advance(
    own_ref, aux_ref, ya_ref, yo_ref, low_ref, tout_ref, bout_ref,
    y00, y01, y02, y03, y10, y11, y12, y13, y20, y21, y22, y23, full, aux, coef, coef_up, ecoef, edge, mid,
):
    lane = lane_ids(W)
    dt = lowest(jnp.min(low_ref[...], axis=0))
    odd = is_odd("gy")

    sides = (
        lambda i: jnp.where(odd, ya_ref[i], yo_ref[i]),
        own_ref.__getitem__,
        lambda i: jnp.where(odd, yo_ref[i], ya_ref[i]),
    )
    for field in range(FULL):
        to = y00 if field == 0 else full.at[field - 1]
        for x in range(XE + XG):
            i, plane = field * XE + x, x
            if x >= XE:
                i, plane = FULL * XE + field * XG + x - XE, x + 1
            for part in range(3):
                to[plane, part * W : part * W + W] = sides[part](i)
    for field in range(AUX):
        for x in range(XA + XG):
            i, plane = field * XA + x, x
            if x >= XA:
                i, plane = AUX * XA + field * XG + x - XA, x + 1
            tile, k = Y_FULL + i // 4, AX * (i % 4)
            for part in range(3):
                u = aux_ref[i] if part == 1 else jnp.tile(sides[part](tile)[k : k + AX], (4, 1))
                aux[field, plane, part * W : part * W + W] = u

    def beside(ref, low, high):
        ref[low] = lroll(ref[high - 1], WIDE)
        ref[high] = lroll(ref[low + 1], -WIDE)

    beside(y00, LOW, HIGH)
    for k in range(FULL - 1):
        beside(full.at[k], LOW, HIGH)

    def sums(x, x_p):
        bx, by, bz = full[1, x], full[2, x], full[3, x]
        sx = bx + full[1, x_p]
        sy = by + rroll(by, -1)
        sz = bz + lroll(bz, -1)
        return bx, by, bz, sx, sy, sz

    def face(n, x, kk, bn, b1, b2):
        b1, b2 = 0.25 * b1, 0.25 * b2
        q = bn * bn + b1 * b1 + b2 * b2
        s = (0.5 * FIRST_RATE * dt) * kk / jnp.maximum(q, FACE_FLOOR) * bn
        coef[3 * n, x] = s * bn
        coef[3 * n + 1, x] = 0.25 * (s * b1)
        coef[3 * n + 2, x] = 0.25 * (s * b2)

    def faces(x, carry):
        k_m, sy_m, sz_m = carry
        kap = full[0, x]
        u = y00[x]
        y01[x] = lroll(u, -1)
        y02[x] = lroll(u, 1)
        y03[x] = lroll(rroll(u, -1) - rroll(u, 1), 1)
        x_p = min(x + 1, PLANES - 1)
        bx, by, bz, sx, sy, sz = sums(x, x_p)
        face(0, x, kap + k_m, bx, sy + sy_m, sz + sz_m)
        face(1, x, kap + rroll(kap, 1), by, sz + rroll(sz, 1), sx + rroll(sx, 1))
        face(2, x, kap + lroll(kap, 1), bz, sx + lroll(sx, 1), sy + lroll(sy, 1))
        return kap, sy, sz

    for first, last in ((0, XE), (LOW, PLANES)):
        _, _, _, _, sy, sz = sums(first, first + 1)
        carry = full[0, first], sy, sz
        for x in range(first, last):
            carry = faces(x, carry)

    arrays = ((y00, y01, y02, y03), (y10, y11, y12, y13), (y20, y21, y22, y23))
    source, older = arrays[0], None
    begun = []
    for j in range(1, SECTIONS + 1):
        target = arrays[2 - j % 2]
        grow = (2.0 * j - 1.0) / j
        back = (j - 1.0) / j

        def rolled(u, u_p, u_m):
            down = rroll(u, 1)
            return down, rroll(u, -1) - down, u_p - u_m

        def flux_x(x, du, sum_y, sum_z):
            return coef[0, x] * du + coef[1, x] * sum_y + coef[2, x] * sum_z

        def plane(x, carry, source=source):
            dy, dz, fx, down = carry
            u, p, m = source[0][x], source[1][x], source[2][x]
            u_p, p_p, m_p = source[0][x + 1], source[1][x + 1], source[2][x + 1]
            down_p, dy_p, dz_p = rolled(u_p, p_p, m_p)
            fx_p = flux_x(x + 1, u_p - u, dy_p + dy, dz_p + dz)
            dx = u_p - source[0][x - 1]
            dx_zm = m_p - source[2][x - 1]
            dy_zm = source[3][x]
            fy = (
                coef[3, x] * (u - down)
                + coef[4, x] * (dz + rroll(dz, 1))
                + coef[5, x] * (dx + rroll(dx, 1))
            )
            fz = coef[6, x] * (u - m) + coef[7, x] * (dx + dx_zm) + coef[8, x] * (dy + dy_zm)
            ahead_z = lroll(fz, -1)
            rate = (fx_p - fx) + (rroll(fy, -1) - fy) - fz
            return (dy_p, dz_p, fx_p, down_p), u + rate, ahead_z

        def finish(x, new, ahead_z, target=target, older=older, grow=grow, back=back, j=j):
            new = new + ahead_z
            if j > 1:
                new = grow * new - back * older[0][x]
            if j == SECTIONS:
                b = (SECTIONS * SECTIONS + SECTIONS - 2) / (2.0 * SECTIONS * (SECTIONS + 1))
                new = (1.0 - b) * y00[x] + b * new
            if j == SECTIONS:
                target[0][x, W : 2 * W] = new[W : 2 * W]
            else:
                target[0][x] = new
                target[1][x] = lroll(new, -1)
                target[2][x] = lroll(new, 1)
                target[3][x] = lroll(rroll(new, -1) - rroll(new, 1), 1)
            return new

        def start(x, source=source):
            u_m, u = source[0][x - 1], source[0][x]
            _, dy_m, dz_m = rolled(u_m, source[1][x - 1], source[2][x - 1])
            down, dy, dz = rolled(u, source[1][x], source[2][x])
            return dy, dz, flux_x(x, u - u_m, dy + dy_m, dz + dz_m), down

        strip = []

        def finish_strip(x, new, ahead_z, finish=finish, strip=strip, target=target, j=j):
            strip.append(finish(x, new, ahead_z))
            if x == HIGH - 1 and j < SECTIONS:
                for at, u, by in ((HIGH, strip[0], -WIDE), (LOW, strip[-1], WIDE)):
                    target[0][at] = lroll(u, by)
                    target[1][at] = lroll(u, by - 1)
                    target[2][at] = lroll(u, by + 1)

        for first, last, then in ((LOW + 1, HIGH, finish_strip), (j, XE - j, finish)):
            carry = start(first)
            for x in range(first, last):
                carry, *parts = plane(x, carry)
                begun.append((then, x, *parts))
                if len(begun) > LATE:
                    then_, *parts = begun.pop(0)
                    then_(*parts)
        source, older = target, source
    for then, *parts in begun:
        then(*parts)

    def seam(main, strip, g):
        return jnp.where(
            lane < LANES - 16, lroll(main, -8), lroll(strip, LANES - 16 - 8 - WIDE * g)
        )

    for x in range(W):
        g, k = divmod(W + x, XG)
        tout_ref[x] = seam(source[0][W + x, W : 2 * W], source[0][LOW + 1 + k, W : 2 * W], g)

    SPEED = 3
    strip = range(A_LOW + 1, A_HIGH)

    def within(i):
        return i + OFF if i < XA else i - A_LOW + LOW

    for i in (*range(XA), *strip):
        x = within(i)
        _, _, _, sx, sy, sz = sums(x, x + 1)
        field = 0.25 * (sx * sx + sy * sy + sz * sz)
        vx, vy, vz = aux[0, i], aux[1, i], aux[2, i]
        flow = jnp.sqrt(vx * vx + vy * vy + vz * vz)
        aux[SPEED, i] = flow + jnp.sqrt(GAMMA * y00[x] + field / aux[SPEED, i])
    for k in range(AUX):
        aux[k, A_LOW] = lroll(aux[k, A_HIGH - 1], WIDE)

    def by_axis(u, u_m, axis):
        if axis == 0:
            return u_m
        return rroll(u, 1) if axis == 1 else lroll(u, 1)

    for i in (*range(1, XA), *strip):
        for c in range(3):
            a, b = (c + 1) % 3, (c + 2) % 3

            def mean(f, i=i, a=a, b=b):
                if 0 in (a, b):
                    other = a + b
                    u = aux[f, i] + aux[f, i - 1]
                else:
                    other = 2
                    u = aux[f, i]
                    u = u + by_axis(u, None, 1)
                return 0.125 * (u + by_axis(u, None, other))

            va, vb, s = mean(a), mean(b), mean(SPEED)
            ecoef[4 * c, i] = vb - s
            ecoef[4 * c + 1, i] = vb + s
            ecoef[4 * c + 2, i] = s - va
            ecoef[4 * c + 3, i] = -s - va

    def fields(get, first, last):
        for i in (*range(first, last), *strip):
            for c in range(3):
                a, b = (c + 1) % 3, (c + 2) % 3
                ua, ub = get(a, i), get(b, i)
                ua_b = by_axis(ua, get(a, i - 1) if b == 0 else None, b)
                ub_a = by_axis(ub, get(b, i - 1) if a == 0 else None, a)
                edge[c, i] = (ecoef[4 * c, i] * ua + ecoef[4 * c + 1, i] * ua_b) + (
                    ecoef[4 * c + 2, i] * ub + ecoef[4 * c + 3, i] * ub_a
                )
        for c in range(1, 3):
            edge[c, A_HIGH] = lroll(edge[c, A_LOW + 1], -WIDE)

    def ahead(f, i, axis):
        if axis == 0:
            return edge[f, i + 1]
        u = edge[f, i]
        return rroll(u, -1) if axis == 1 else lroll(u, -1)

    def curl(d, i):
        e, f = (d + 1) % 3, (d + 2) % 3
        return (ahead(f, i, e) - edge[f, i]) - (ahead(e, i, f) - edge[e, i])

    fields(lambda d, i: full[1 + d, within(i)], 1, XA)
    for i in (*range(1, XA - 1), *strip):
        for d in range(3):
            mid[d, i] = full[1 + d, within(i)] - dt * curl(d, i)
    for d in range(1, 3):
        mid[d, A_LOW] = lroll(mid[d, A_HIGH - 1], WIDE)
    fields(lambda d, i: mid[d, i], 2, XA - 1)

    def final(d, i):
        u = 0.5 * (full[1 + d, within(i)] + (mid[d, i] - dt * curl(d, i)))
        return u[W : 2 * W]

    for d in range(3):
        ends = [final(d, i) for i in strip]
        for x in range(W):
            g, k = divmod(W + x, XG)
            bout_ref[d, x] = seam(final(d, x + AX), ends[k], g)


def exchange(first, second, axis):
    count = lax.axis_size(axis)
    swaps = [(i, i + 1) for i in range(0, count, 2)] + [(i + 1, i) for i in range(0, count, 2)]
    others = [((a + 1) % count, (b + 1) % count) for a, b in swaps]
    return lax.ppermute(first, axis, swaps), lax.ppermute(second, axis, others)


def on_core(kernel, out, *args, scratch=(), last=False):
    space = pl.BlockSpec(memory_space=pltpu.VMEM)
    shape = [
        jax.ShapeDtypeStruct(o, jnp.float32) if last else pltpu.VMEM(o, jnp.float32) for o in out
    ]
    return pl.pallas_call(
        kernel,
        out_shape=shape,
        in_specs=[space] * len(args),
        out_specs=[space] * len(out),
        scratch_shapes=[pltpu.VMEM(shape, jnp.float32) for shape in scratch],
        compiler_params=pltpu.CompilerParams(vmem_limit_bytes=GRANT),
        name=kernel.__name__,
    )(*args)


def held(*arrays):
    return [pltpu.with_memory_space_constraint(a, pltpu.VMEM) for a in arrays]


def on_device(t, diffusivity, b, v, rho):
    zs = lax.axis_size("gz")
    outer = lax.axis_size("gx_2") * lax.axis_size("gy")
    inner = lax.axis_size("gx_0") * lax.axis_size("gx_1")
    out = [((FULL + AUX) * W, W, LANES), (zs, ZT, W, LANES)]
    cells, edges = on_core(pack_z, out, t, diffusivity, b, v, rho)
    edges = lax.all_to_all(edges, "gz", 0, 0, tiled=True)
    cells, edges = held(cells, edges)
    out = [(SIDE, W, LANES)] * 2 + [((W + 1) * AUX, W, LANES), (outer, 1, LANES)]
    first, second, aux, low = on_core(pack_x, out, cells, edges)
    x_first, x_second = exchange(first, second, GX)
    low = lax.all_to_all(low, ("gx_2", "gy"), 0, 0, tiled=True)
    args = held(first, aux, x_first, x_second, low)
    out = [(YT, W, LANES)] * 2 + [(A_TILES, W, LANES), (inner, 1, LANES)]
    first, second, aux, low = on_core(pack_y, out, *args)
    y_first, y_second = exchange(first, second, "gy")
    low = lax.all_to_all(low, ("gx_0", "gx_1"), 0, 0, tiled=True)
    out = [(W, W, LANES), (3, W, W, LANES)]
    args = held(first, aux, y_first, y_second, low)
    return tuple(on_core(advance, out, *args, scratch=SCRATCH, last=True))


def solution(mesh):
    gx, gy, gz = (mesh.shape[axis] for axis in ("gx", "gy", "gz"))
    outer = 3 if gx % 6 == 0 else 1
    finer = Mesh(mesh.devices.reshape(outer, gx // outer // 2, 2, gy, gz), (*GX, "gy", "gz"))
    cell = P(GX, "gy", "gz")
    face = P(None, GX, "gy", "gz")
    return jax.shard_map(
        on_device,
        mesh=finer,
        in_specs=(cell, cell, face, face, cell),
        out_specs=(cell, face),
        check_vma=False,
    )
```

```python
import jax
import jax.numpy as jnp
from jax import lax
from jax.experimental import pallas as pl
from jax.experimental.pallas import tpu as pltpu
from jax.sharding import Mesh
from jax.sharding import PartitionSpec as P

SECTIONS = 8
GAMMA = 5.0 / 3.0
FACE_FLOOR = 0.25

GX = ("gx_0", "gx_1", "gx_2")
W = 8
LANES = 128
XE = 3 * W
WIDE = 4 * W
GROUPS = LANES // WIDE
XG = XE // GROUPS
LOW, HIGH = XE, XE + XG + 1
PLANES = HIGH + 1
ROWS = 3 * W
FULL = 5
AUX = 4
AX = 2
XA = W + 2 * AX
OFF = W - AX
A_LOW, A_HIGH = XA, XA + XG + 1
A_PLANES = A_HIGH + 1
ZT = (FULL + AUX) * W // 16 + 1
SPARE = LANES // 2
SIDE = FULL * W + AUX * AX + FULL + 1
A_TILES = AUX * (XA + XG)
Y_FULL = FULL * (XE + XG)
YT = Y_FULL + A_TILES // 4
GRANT = 28 << 20
SCRATCH = [(PLANES, ROWS, LANES)] * 12 + [
    (FULL - 1, PLANES, ROWS, LANES),
    (AUX, A_PLANES, ROWS, LANES),
    (9, PLANES, ROWS, LANES),
    (3, PLANES, ROWS, LANES),
    (12, A_PLANES, ROWS, LANES),
    (3, A_PLANES, ROWS, LANES),
    (3, A_PLANES, ROWS, LANES),
]
LATE = 5
FIRST_RATE = 4.0 / (SECTIONS * SECTIONS + SECTIONS - 2)
LIMIT = (SECTIONS * SECTIONS + SECTIONS - 2) / 16.0


def lane_ids(rows):
    return lax.broadcasted_iota(jnp.int32, (rows, LANES), 1)


def lroll(u, amount):
    return pltpu.roll(u, amount % LANES, 1)


def rroll(u, amount):
    return pltpu.roll(u, amount % u.shape[0], 0)


def lowest(u):
    return jnp.min(jnp.min(u, axis=0, keepdims=True), axis=1, keepdims=True)


def neighbours(axis):
    count = lax.axis_size(axis)
    at = lax.axis_index(axis)
    return lax.rem(at + count - 1, count), lax.rem(at + 1, count)


def is_odd(axis):
    return lax.rem(lax.axis_index(axis), 2) == 1


def piece(field, plane):
    return divmod(field * W + plane, 16)


def pack_z(t_ref, d_ref, b_ref, v_ref, r_ref, all_ref, out_ref):
    t = t_ref[...]
    kappa = d_ref[...] * (t * t * jnp.sqrt(t))
    low = lowest(jnp.min(LIMIT / kappa, axis=0))
    lane = lane_ids(W)
    left, right = [], []
    for tile in range(ZT):
        below = above = jnp.broadcast_to(low, (W, LANES))
        for k in range(16):
            field, plane = divmod(tile * 16 + k, W)
            if field >= FULL + AUX:
                break
            if field == 0:
                u = t[plane]
            elif field == 1:
                u = kappa[plane]
            elif field < FULL:
                u = b_ref[field - 2, plane]
            else:
                u = v_ref[field - FULL, plane] if field < FULL + 3 else r_ref[plane]
            all_ref[field * W + plane] = u
            here = (lane >= 8 * k) & (lane < 8 * k + 8)
            below = jnp.where(here, lroll(u, 8 * k), below)
            above = jnp.where(here, lroll(u, 8 * k - (LANES - 8)), above)
        left.append(below)
        right.append(above)
    lo, _ = neighbours("gz")
    for slot in range(out_ref.shape[0]):
        for tile in range(ZT):
            out_ref[slot, tile] = jnp.where(lo == slot, left[tile], right[tile])


def pack_x(all_ref, z_ref, a_ref, o_ref, aux_ref, low_ref):
    odd = is_odd(GX)
    lo, hi = neighbours("gz")
    lane = lane_ids(W)
    left = [z_ref[lo, tile] for tile in range(ZT)]
    right = [z_ref[hi, tile] for tile in range(ZT)]
    up_ends = down_ends = jnp.zeros((W, LANES), jnp.float32)
    for field in range(FULL + AUX):
        ends = jnp.zeros((W, LANES), jnp.float32)
        for plane in range(W):
            u = all_ref[field * W + plane]
            tile, k = piece(field, plane)
            main = jnp.where(lane < 8, lroll(left[tile], -8 * k), lroll(u, 8))
            to = 16 * plane
            end = jnp.where(
                lane < to + 8, lroll(u, to + 8 - LANES), lroll(right[tile], to + 8 - 8 * k)
            )
            ends = jnp.where(lane < to, ends, end)
            if field < FULL:
                a_ref[field * W + plane] = main
                o_ref[field * W + plane] = main
                continue
            aux_ref[(field - FULL) * W + plane] = main
            at = FULL * W + (field - FULL) * AX
            if plane < AX:
                a_ref[at + plane] = main
                o_ref[at + plane] = main
            elif plane >= W - AX:
                i = at + plane - (W - AX)
                down = a_ref[i]
                a_ref[i] = jnp.where(odd, down, main)
                o_ref[i] = jnp.where(odd, main, down)
        if field < FULL:
            a_ref[FULL * W + AUX * AX + field] = ends
            o_ref[FULL * W + AUX * AX + field] = ends
        else:
            f = field - FULL
            aux_ref[AUX * W + f] = ends
            here = lane >= 32 * f
            down_ends = jnp.where(here, lroll(ends, 32 * f), down_ends)
            up_ends = jnp.where(here, lroll(ends, 32 * f - (LANES - 32)), up_ends)
    a_ref[SIDE - 1] = jnp.where(odd, down_ends, up_ends)
    o_ref[SIDE - 1] = jnp.where(odd, up_ends, down_ends)
    low = z_ref[0, ZT - 1]
    for slot in range(1, z_ref.shape[0]):
        low = jnp.minimum(low, z_ref[slot, ZT - 1])
    low = lowest(jnp.where(lane >= SPARE, low, jnp.max(low)))
    low_ref[...] = jnp.broadcast_to(low.reshape(1, 1, 1), low_ref.shape)


def pack_y(own_ref, ownaux_ref, xa_ref, xo_ref, min_ref, a_ref, o_ref, aux_ref, low_ref):
    odd_x, odd_y = is_odd(GX), is_odd("gy")
    lane = lane_ids(W)

    def below(i):
        return jnp.where(odd_x, xa_ref[i], xo_ref[i])

    def above(i):
        return jnp.where(odd_x, xo_ref[i], xa_ref[i])

    sides = (below, own_ref.__getitem__, above)

    def send(i, u):
        a_ref[i] = u
        o_ref[i] = u

    ends_at = FULL * W + AUX * AX
    for field in range(FULL):
        ends = [get(ends_at + field) for get in sides]
        mains = []
        for x in range(XE):
            part, at = divmod(x, W)
            mains.append(sides[part](field * W + at))
            send(field * XE + x, mains[x])
        for k in range(XG):
            strip = None
            for g in range(GROUPS):
                part, at = divmod(g * XG + k, W)
                to = g * WIDE
                new = jnp.where(
                    lane < to + 16,
                    lroll(mains[g * XG + k], to + 16 - LANES),
                    lroll(ends[part], to + 16 - 16 * at),
                )
                strip = jnp.where(lane < to, strip, new) if g else new
            send(FULL * XE + field * XG + k, strip)

    def put(i, u):
        aux_ref[i] = u
        tile, k = Y_FULL + i // 4, AX * (i % 4)
        up, down = u[W - AX : W], u[0:AX]
        a_ref[tile, k : k + AX] = jnp.where(odd_y, down, up)
        o_ref[tile, k : k + AX] = jnp.where(odd_y, up, down)

    outer = below(SIDE - 1), above(SIDE - 1)
    for field in range(AUX):
        mains, ends = [], []
        at = FULL * W + field * AX
        for i in range(XA):
            if i < AX:
                mains.append(below(at + i))
                ends.append((outer[0], field * AX + i))
            elif i < AX + W:
                mains.append(ownaux_ref[field * W + i - AX])
                ends.append((ownaux_ref[AUX * W + field], i - AX))
            else:
                mains.append(above(at + i - AX - W))
                ends.append((outer[1], field * AX + i - AX - W))
            put(field * XA + i, mains[i])
        for k in range(XG):
            strip = None
            for g in range(XA // XG):
                u, (end, at_end) = mains[g * XG + k], ends[g * XG + k]
                to = (g + OFF // XG) * WIDE
                new = lroll(u, to + 16 - LANES)
                strip = jnp.where(lane < to, strip, new) if g else new
                new = lroll(end, to + 16 - 16 * at_end)
                strip = jnp.where((lane >= to + 16) & (lane < to + 32), new, strip)
            put(AUX * XA + field * XG + k, strip)
    low = lowest(jnp.min(min_ref[...], axis=0))
    low_ref[...] = jnp.broadcast_to(low.reshape(1, 1, 1), low_ref.shape)


def sweep(first, last, body, carry, by):
    trips = (last - first) // by

    def several(i, carry):
        for k in range(by):
            carry = body(first + i * by + k, carry)
        return carry

    if trips:
        carry = lax.fori_loop(0, trips, several, carry)
    for x in range(first + trips * by, last):
        carry = body(x, carry)
    return carry


def advance(
    own_ref, aux_ref, ya_ref, yo_ref, low_ref, tout_ref, bout_ref,
    y00, y01, y02, y03, y10, y11, y12, y13, y20, y21, y22, y23, full, aux, coef, coef_up, ecoef, edge, mid,
):
    lane = lane_ids(W)
    dt = lowest(jnp.min(low_ref[...], axis=0))
    odd = is_odd("gy")

    sides = (
        lambda i: jnp.where(odd, ya_ref[i], yo_ref[i]),
        own_ref.__getitem__,
        lambda i: jnp.where(odd, yo_ref[i], ya_ref[i]),
    )
    for field in range(FULL):
        to = y00 if field == 0 else full.at[field - 1]
        for x in range(XE + XG):
            i, plane = field * XE + x, x
            if x >= XE:
                i, plane = FULL * XE + field * XG + x - XE, x + 1
            for part in range(3):
                to[plane, part * W : part * W + W] = sides[part](i)
    for field in range(AUX):
        for x in range(XA + XG):
            i, plane = field * XA + x, x
            if x >= XA:
                i, plane = AUX * XA + field * XG + x - XA, x + 1
            tile, k = Y_FULL + i // 4, AX * (i % 4)
            for part in range(3):
                u = aux_ref[i] if part == 1 else jnp.tile(sides[part](tile)[k : k + AX], (4, 1))
                aux[field, plane, part * W : part * W + W] = u

    def beside(ref, low, high):
        ref[low] = lroll(ref[high - 1], WIDE)
        ref[high] = lroll(ref[low + 1], -WIDE)

    beside(y00, LOW, HIGH)
    for k in range(FULL - 1):
        beside(full.at[k], LOW, HIGH)

    def sums(x, x_p):
        bx, by, bz = full[1, x], full[2, x], full[3, x]
        sx = bx + full[1, x_p]
        sy = by + rroll(by, -1)
        sz = bz + lroll(bz, -1)
        return bx, by, bz, sx, sy, sz

    def face(n, x, kk, bn, b1, b2):
        b1, b2 = 0.25 * b1, 0.25 * b2
        q = bn * bn + b1 * b1 + b2 * b2
        s = (0.5 * FIRST_RATE * dt) * kk / jnp.maximum(q, FACE_FLOOR) * bn
        coef[3 * n, x] = s * bn
        coef[3 * n + 1, x] = 0.25 * (s * b1)
        coef[3 * n + 2, x] = 0.25 * (s * b2)

    def faces(x, carry):
        k_m, sy_m, sz_m = carry
        kap = full[0, x]
        u = y00[x]
        y01[x] = lroll(u, -1)
        y02[x] = lroll(u, 1)
        y03[x] = lroll(rroll(u, -1) - rroll(u, 1), 1)
        x_p = min(x + 1, PLANES - 1)
        bx, by, bz, sx, sy, sz = sums(x, x_p)
        face(0, x, kap + k_m, bx, sy + sy_m, sz + sz_m)
        face(1, x, kap + rroll(kap, 1), by, sz + rroll(sz, 1), sx + rroll(sx, 1))
        face(2, x, kap + lroll(kap, 1), bz, sx + lroll(sx, 1), sy + lroll(sy, 1))
        return kap, sy, sz

    for first, last in ((0, XE), (LOW, PLANES)):
        _, _, _, _, sy, sz = sums(first, first + 1)
        carry = full[0, first], sy, sz
        for x in range(first, last):
            carry = faces(x, carry)

    arrays = ((y00, y01, y02, y03), (y10, y11, y12, y13), (y20, y21, y22, y23))
    source, older = arrays[0], None
    begun = []
    for j in range(1, SECTIONS + 1):
        target = arrays[2 - j % 2]
        grow = (2.0 * j - 1.0) / j
        back = (j - 1.0) / j

        def rolled(u, u_p, u_m):
            down = rroll(u, 1)
            return down, rroll(u, -1) - down, u_p - u_m

        def flux_x(x, du, sum_y, sum_z):
            return coef[0, x] * du + coef[1, x] * sum_y + coef[2, x] * sum_z

        def plane(x, carry, source=source):
            dy, dz, fx, down = carry
            u, p, m = source[0][x], source[1][x], source[2][x]
            u_p, p_p, m_p = source[0][x + 1], source[1][x + 1], source[2][x + 1]
            down_p, dy_p, dz_p = rolled(u_p, p_p, m_p)
            fx_p = flux_x(x + 1, u_p - u, dy_p + dy, dz_p + dz)
            dx = u_p - source[0][x - 1]
            dx_zm = m_p - source[2][x - 1]
            dy_zm = source[3][x]
            fy = (
                coef[3, x] * (u - down)
                + coef[4, x] * (dz + rroll(dz, 1))
                + coef[5, x] * (dx + rroll(dx, 1))
            )
            fz = coef[6, x] * (u - m) + coef[7, x] * (dx + dx_zm) + coef[8, x] * (dy + dy_zm)
            ahead_z = lroll(fz, -1)
            rate = (fx_p - fx) + (rroll(fy, -1) - fy) - fz
            return (dy_p, dz_p, fx_p, down_p), u + rate, ahead_z

        def finish(x, new, ahead_z, target=target, older=older, grow=grow, back=back, j=j):
            new = new + ahead_z
            if j > 1:
                new = grow * new - back * older[0][x]
            if j == SECTIONS:
                b = (SECTIONS * SECTIONS + SECTIONS - 2) / (2.0 * SECTIONS * (SECTIONS + 1))
                new = (1.0 - b) * y00[x] + b * new
            if j == SECTIONS:
                target[0][x, W : 2 * W] = new[W : 2 * W]
            else:
                target[0][x] = new
                target[1][x] = lroll(new, -1)
                target[2][x] = lroll(new, 1)
                target[3][x] = lroll(rroll(new, -1) - rroll(new, 1), 1)
            return new

        def start(x, source=source):
            u_m, u = source[0][x - 1], source[0][x]
            _, dy_m, dz_m = rolled(u_m, source[1][x - 1], source[2][x - 1])
            down, dy, dz = rolled(u, source[1][x], source[2][x])
            return dy, dz, flux_x(x, u - u_m, dy + dy_m, dz + dz_m), down

        strip = []

        def finish_strip(x, new, ahead_z, finish=finish, strip=strip, target=target, j=j):
            strip.append(finish(x, new, ahead_z))
            if x == HIGH - 1 and j < SECTIONS:
                for at, u, by in ((HIGH, strip[0], -WIDE), (LOW, strip[-1], WIDE)):
                    target[0][at] = lroll(u, by)
                    target[1][at] = lroll(u, by - 1)
                    target[2][at] = lroll(u, by + 1)

        for first, last, then in ((LOW + 1, HIGH, finish_strip), (j, XE - j, finish)):
            carry = start(first)
            for x in range(first, last):
                carry, *parts = plane(x, carry)
                begun.append((then, x, *parts))
                if len(begun) > LATE:
                    then_, *parts = begun.pop(0)
                    then_(*parts)
        source, older = target, source
    for then, *parts in begun:
        then(*parts)

    def seam(main, strip, g):
        return jnp.where(
            lane < LANES - 16, lroll(main, -8), lroll(strip, LANES - 16 - 8 - WIDE * g)
        )

    for x in range(W):
        g, k = divmod(W + x, XG)
        tout_ref[x] = seam(source[0][W + x, W : 2 * W], source[0][LOW + 1 + k, W : 2 * W], g)

    SPEED = 3
    strip = range(A_LOW + 1, A_HIGH)

    def within(i):
        return i + OFF if i < XA else i - A_LOW + LOW

    for i in (*range(XA), *strip):
        x = within(i)
        _, _, _, sx, sy, sz = sums(x, x + 1)
        field = 0.25 * (sx * sx + sy * sy + sz * sz)
        vx, vy, vz = aux[0, i], aux[1, i], aux[2, i]
        flow = jnp.sqrt(vx * vx + vy * vy + vz * vz)
        aux[SPEED, i] = flow + jnp.sqrt(GAMMA * y00[x] + field / aux[SPEED, i])
    for k in range(AUX):
        aux[k, A_LOW] = lroll(aux[k, A_HIGH - 1], WIDE)

    def by_axis(u, u_m, axis):
        if axis == 0:
            return u_m
        return rroll(u, 1) if axis == 1 else lroll(u, 1)

    for i in (*range(1, XA), *strip):
        for c in range(3):
            a, b = (c + 1) % 3, (c + 2) % 3

            def mean(f, i=i, a=a, b=b):
                if 0 in (a, b):
                    other = a + b
                    u = aux[f, i] + aux[f, i - 1]
                else:
                    other = 2
                    u = aux[f, i]
                    u = u + by_axis(u, None, 1)
                return 0.125 * (u + by_axis(u, None, other))

            va, vb, s = mean(a), mean(b), mean(SPEED)
            ecoef[4 * c, i] = vb - s
            ecoef[4 * c + 1, i] = vb + s
            ecoef[4 * c + 2, i] = s - va
            ecoef[4 * c + 3, i] = -s - va

    def fields(get, first, last):
        for i in (*range(first, last), *strip):
            for c in range(3):
                a, b = (c + 1) % 3, (c + 2) % 3
                ua, ub = get(a, i), get(b, i)
                ua_b = by_axis(ua, get(a, i - 1) if b == 0 else None, b)
                ub_a = by_axis(ub, get(b, i - 1) if a == 0 else None, a)
                edge[c, i] = (ecoef[4 * c, i] * ua + ecoef[4 * c + 1, i] * ua_b) + (
                    ecoef[4 * c + 2, i] * ub + ecoef[4 * c + 3, i] * ub_a
                )
        for c in range(1, 3):
            edge[c, A_HIGH] = lroll(edge[c, A_LOW + 1], -WIDE)

    def ahead(f, i, axis):
        if axis == 0:
            return edge[f, i + 1]
        u = edge[f, i]
        return rroll(u, -1) if axis == 1 else lroll(u, -1)

    def curl(d, i):
        e, f = (d + 1) % 3, (d + 2) % 3
        return (ahead(f, i, e) - edge[f, i]) - (ahead(e, i, f) - edge[e, i])

    fields(lambda d, i: full[1 + d, within(i)], 1, XA)
    for i in (*range(1, XA - 1), *strip):
        for d in range(3):
            mid[d, i] = full[1 + d, within(i)] - dt * curl(d, i)
    for d in range(1, 3):
        mid[d, A_LOW] = lroll(mid[d, A_HIGH - 1], WIDE)
    fields(lambda d, i: mid[d, i], 2, XA - 1)

    def final(d, i):
        u = 0.5 * (full[1 + d, within(i)] + (mid[d, i] - dt * curl(d, i)))
        return u[W : 2 * W]

    for d in range(3):
        ends = [final(d, i) for i in strip]
        for x in range(W):
            g, k = divmod(W + x, XG)
            bout_ref[d, x] = seam(final(d, x + AX), ends[k], g)


def exchange(first, second, axis):
    count = lax.axis_size(axis)
    swaps = [(i, i + 1) for i in range(0, count, 2)] + [(i + 1, i) for i in range(0, count, 2)]
    others = [((a + 1) % count, (b + 1) % count) for a, b in swaps]
    return lax.ppermute(first, axis, swaps), lax.ppermute(second, axis, others)


def on_core(kernel, out, *args, scratch=(), last=False, grant=GRANT):
    space = pl.BlockSpec(memory_space=pltpu.VMEM)
    shape = [
        jax.ShapeDtypeStruct(o, jnp.float32) if last else pltpu.VMEM(o, jnp.float32) for o in out
    ]
    return pl.pallas_call(
        kernel,
        out_shape=shape,
        in_specs=[space] * len(args),
        out_specs=[space] * len(out),
        scratch_shapes=[pltpu.VMEM(shape, jnp.float32) for shape in scratch],
        compiler_params=pltpu.CompilerParams(vmem_limit_bytes=grant),
        name=kernel.__name__,
    )(*args)


def held(*arrays):
    return [pltpu.with_memory_space_constraint(a, pltpu.VMEM) for a in arrays]


def on_device(t, diffusivity, b, v, rho):
    zs = lax.axis_size("gz")
    outer = lax.axis_size("gx_2") * lax.axis_size("gy")
    inner = lax.axis_size("gx_0") * lax.axis_size("gx_1")
    out = [((FULL + AUX) * W, W, LANES), (zs, ZT, W, LANES)]
    cells, edges = on_core(pack_z, out, t, diffusivity, b, v, rho, grant=None)
    edges = lax.all_to_all(edges, "gz", 0, 0, tiled=True)
    cells, edges = held(cells, edges)
    out = [(SIDE, W, LANES)] * 2 + [((W + 1) * AUX, W, LANES), (outer, 1, LANES)]
    first, second, aux, low = on_core(pack_x, out, cells, edges)
    x_first, x_second = exchange(first, second, GX)
    low = lax.all_to_all(low, ("gx_2", "gy"), 0, 0, tiled=True)
    args = held(first, aux, x_first, x_second, low)
    out = [(YT, W, LANES)] * 2 + [(A_TILES, W, LANES), (inner, 1, LANES)]
    first, second, aux, low = on_core(pack_y, out, *args)
    y_first, y_second = exchange(first, second, "gy")
    low = lax.all_to_all(low, ("gx_0", "gx_1"), 0, 0, tiled=True)
    out = [(W, W, LANES), (3, W, W, LANES)]
    args = held(first, aux, y_first, y_second, low)
    return tuple(on_core(advance, out, *args, scratch=SCRATCH, last=True))


def solution(mesh):
    gx, gy, gz = (mesh.shape[axis] for axis in ("gx", "gy", "gz"))
    outer = 3 if gx % 6 == 0 else 1
    finer = Mesh(mesh.devices.reshape(outer, gx // outer // 2, 2, gy, gz), (*GX, "gy", "gz"))
    cell = P(GX, "gy", "gz")
    face = P(None, GX, "gy", "gz")
    return jax.shard_map(
        on_device,
        mesh=finer,
        in_specs=(cell, cell, face, face, cell),
        out_specs=(cell, face),
        check_vma=False,
    )
```

```python
import jax
import jax.numpy as jnp
from jax import lax
from jax.experimental import pallas as pl
from jax.experimental.pallas import tpu as pltpu
from jax.sharding import Mesh
from jax.sharding import PartitionSpec as P

SECTIONS = 8
GAMMA = 5.0 / 3.0
FACE_FLOOR = 0.25

GX = ("gx_0", "gx_1", "gx_2")
W = 8
LANES = 128
XE = 3 * W
WIDE = 4 * W
GROUPS = LANES // WIDE
XG = XE // GROUPS
LOW, HIGH = XE, XE + XG + 1
PLANES = HIGH + 1
ROWS = 3 * W
FULL = 5
AUX = 4
AX = 2
XA = W + 2 * AX
OFF = W - AX
A_LOW, A_HIGH = XA, XA + XG + 1
A_PLANES = A_HIGH + 1
ZT = (FULL + AUX) * W // 16 + 1
SPARE = LANES // 2
SIDE = FULL * W + AUX * AX + FULL + 1
A_TILES = AUX * (XA + XG)
Y_FULL = FULL * (XE + XG)
YT = Y_FULL + A_TILES // 4
GRANT = 28 << 20
SCRATCH = [(PLANES, ROWS, LANES)] * 12 + [
    (FULL - 1, PLANES, ROWS, LANES),
    (AUX, A_PLANES, ROWS, LANES),
    (9, PLANES, ROWS, LANES),
    (3, PLANES, ROWS, LANES),
    (12, A_PLANES, ROWS, LANES),
    (3, A_PLANES, ROWS, LANES),
    (3, A_PLANES, ROWS, LANES),
]
LATE = 5
FIRST_RATE = 4.0 / (SECTIONS * SECTIONS + SECTIONS - 2)
LIMIT = (SECTIONS * SECTIONS + SECTIONS - 2) / 16.0


def lane_ids(rows):
    return lax.broadcasted_iota(jnp.int32, (rows, LANES), 1)


def lroll(u, amount):
    return pltpu.roll(u, amount % LANES, 1)


def rroll(u, amount):
    return pltpu.roll(u, amount % u.shape[0], 0)


def lowest(u):
    return jnp.min(jnp.min(u, axis=0, keepdims=True), axis=1, keepdims=True)


def neighbours(axis):
    count = lax.axis_size(axis)
    at = lax.axis_index(axis)
    return lax.rem(at + count - 1, count), lax.rem(at + 1, count)


def is_odd(axis):
    return lax.rem(lax.axis_index(axis), 2) == 1


def piece(field, plane):
    return divmod(field * W + plane, 16)


def pack_z(t_ref, d_ref, b_ref, v_ref, r_ref, all_ref, out_ref):
    t = t_ref[...]
    kappa = d_ref[...] * (t * t * jnp.sqrt(t))
    low = lowest(jnp.min(LIMIT / kappa, axis=0))
    lane = lane_ids(W)
    left, right = [], []
    for tile in range(ZT):
        below = above = jnp.broadcast_to(low, (W, LANES))
        for k in range(16):
            field, plane = divmod(tile * 16 + k, W)
            if field >= FULL + AUX:
                break
            if field == 0:
                u = t[plane]
            elif field == 1:
                u = kappa[plane]
            elif field < FULL:
                u = b_ref[field - 2, plane]
            else:
                u = v_ref[field - FULL, plane] if field < FULL + 3 else r_ref[plane]
            all_ref[field * W + plane] = u
            here = (lane >= 8 * k) & (lane < 8 * k + 8)
            below = jnp.where(here, lroll(u, 8 * k), below)
            above = jnp.where(here, lroll(u, 8 * k - (LANES - 8)), above)
        left.append(below)
        right.append(above)
    lo, _ = neighbours("gz")
    for slot in range(out_ref.shape[0]):
        for tile in range(ZT):
            out_ref[slot, tile] = jnp.where(lo == slot, left[tile], right[tile])


def pack_x(all_ref, z_ref, a_ref, o_ref, aux_ref, low_ref):
    odd = is_odd(GX)
    lo, hi = neighbours("gz")
    lane = lane_ids(W)
    left = [z_ref[lo, tile] for tile in range(ZT)]
    right = [z_ref[hi, tile] for tile in range(ZT)]
    up_ends = down_ends = jnp.zeros((W, LANES), jnp.float32)
    for field in range(FULL + AUX):
        ends = jnp.zeros((W, LANES), jnp.float32)
        for plane in range(W):
            u = all_ref[field * W + plane]
            tile, k = piece(field, plane)
            main = jnp.where(lane < 8, lroll(left[tile], -8 * k), lroll(u, 8))
            to = 16 * plane
            end = jnp.where(
                lane < to + 8, lroll(u, to + 8 - LANES), lroll(right[tile], to + 8 - 8 * k)
            )
            ends = jnp.where(lane < to, ends, end)
            if field < FULL:
                a_ref[field * W + plane] = main
                o_ref[field * W + plane] = main
                continue
            aux_ref[(field - FULL) * W + plane] = main
            at = FULL * W + (field - FULL) * AX
            if plane < AX:
                a_ref[at + plane] = main
                o_ref[at + plane] = main
            elif plane >= W - AX:
                i = at + plane - (W - AX)
                down = a_ref[i]
                a_ref[i] = jnp.where(odd, down, main)
                o_ref[i] = jnp.where(odd, main, down)
        if field < FULL:
            a_ref[FULL * W + AUX * AX + field] = ends
            o_ref[FULL * W + AUX * AX + field] = ends
        else:
            f = field - FULL
            aux_ref[AUX * W + f] = ends
            here = lane >= 32 * f
            down_ends = jnp.where(here, lroll(ends, 32 * f), down_ends)
            up_ends = jnp.where(here, lroll(ends, 32 * f - (LANES - 32)), up_ends)
    a_ref[SIDE - 1] = jnp.where(odd, down_ends, up_ends)
    o_ref[SIDE - 1] = jnp.where(odd, up_ends, down_ends)
    low = z_ref[0, ZT - 1]
    for slot in range(1, z_ref.shape[0]):
        low = jnp.minimum(low, z_ref[slot, ZT - 1])
    low = lowest(jnp.where(lane >= SPARE, low, jnp.max(low)))
    low_ref[...] = jnp.broadcast_to(low.reshape(1, 1, 1), low_ref.shape)


def pack_y(own_ref, ownaux_ref, xa_ref, xo_ref, min_ref, a_ref, o_ref, aux_ref, low_ref):
    odd_x, odd_y = is_odd(GX), is_odd("gy")
    lane = lane_ids(W)

    def below(i):
        return jnp.where(odd_x, xa_ref[i], xo_ref[i])

    def above(i):
        return jnp.where(odd_x, xo_ref[i], xa_ref[i])

    sides = (below, own_ref.__getitem__, above)

    def send(i, u):
        a_ref[i] = u
        o_ref[i] = u

    ends_at = FULL * W + AUX * AX
    for field in range(FULL):
        ends = [get(ends_at + field) for get in sides]
        mains = []
        for x in range(XE):
            part, at = divmod(x, W)
            mains.append(sides[part](field * W + at))
            send(field * XE + x, mains[x])
        for k in range(XG):
            strip = None
            for g in range(GROUPS):
                part, at = divmod(g * XG + k, W)
                to = g * WIDE
                new = jnp.where(
                    lane < to + 16,
                    lroll(mains[g * XG + k], to + 16 - LANES),
                    lroll(ends[part], to + 16 - 16 * at),
                )
                strip = jnp.where(lane < to, strip, new) if g else new
            send(FULL * XE + field * XG + k, strip)

    def put(i, u):
        aux_ref[i] = u
        tile, k = Y_FULL + i // 4, AX * (i % 4)
        up, down = u[W - AX : W], u[0:AX]
        a_ref[tile, k : k + AX] = jnp.where(odd_y, down, up)
        o_ref[tile, k : k + AX] = jnp.where(odd_y, up, down)

    outer = below(SIDE - 1), above(SIDE - 1)
    for field in range(AUX):
        mains, ends = [], []
        at = FULL * W + field * AX
        for i in range(XA):
            if i < AX:
                mains.append(below(at + i))
                ends.append((outer[0], field * AX + i))
            elif i < AX + W:
                mains.append(ownaux_ref[field * W + i - AX])
                ends.append((ownaux_ref[AUX * W + field], i - AX))
            else:
                mains.append(above(at + i - AX - W))
                ends.append((outer[1], field * AX + i - AX - W))
            put(field * XA + i, mains[i])
        for k in range(XG):
            strip = None
            for g in range(XA // XG):
                u, (end, at_end) = mains[g * XG + k], ends[g * XG + k]
                to = (g + OFF // XG) * WIDE
                new = lroll(u, to + 16 - LANES)
                strip = jnp.where(lane < to, strip, new) if g else new
                new = lroll(end, to + 16 - 16 * at_end)
                strip = jnp.where((lane >= to + 16) & (lane < to + 32), new, strip)
            put(AUX * XA + field * XG + k, strip)
    low = lowest(jnp.min(min_ref[...], axis=0))
    low_ref[...] = jnp.broadcast_to(low.reshape(1, 1, 1), low_ref.shape)


def sweep(first, last, body, carry, by):
    trips = (last - first) // by

    def several(i, carry):
        for k in range(by):
            carry = body(first + i * by + k, carry)
        return carry

    if trips:
        carry = lax.fori_loop(0, trips, several, carry)
    for x in range(first + trips * by, last):
        carry = body(x, carry)
    return carry


def advance(
    own_ref, aux_ref, ya_ref, yo_ref, low_ref, tout_ref, bout_ref,
    y00, y01, y02, y03, y10, y11, y12, y13, y20, y21, y22, y23, full, aux, coef, coef_up, ecoef, edge, mid,
):
    lane = lane_ids(W)
    dt = lowest(jnp.min(low_ref[...], axis=0))
    odd = is_odd("gy")

    sides = (
        lambda i: jnp.where(odd, ya_ref[i], yo_ref[i]),
        own_ref.__getitem__,
        lambda i: jnp.where(odd, yo_ref[i], ya_ref[i]),
    )
    for field in range(FULL):
        to = y00 if field == 0 else full.at[field - 1]
        for x in range(XE + XG):
            i, plane = field * XE + x, x
            if x >= XE:
                i, plane = FULL * XE + field * XG + x - XE, x + 1
            for part in range(3):
                to[plane, part * W : part * W + W] = sides[part](i)
    for field in range(AUX):
        for x in range(XA + XG):
            i, plane = field * XA + x, x
            if x >= XA:
                i, plane = AUX * XA + field * XG + x - XA, x + 1
            tile, k = Y_FULL + i // 4, AX * (i % 4)
            for part in range(3):
                u = aux_ref[i] if part == 1 else jnp.tile(sides[part](tile)[k : k + AX], (4, 1))
                aux[field, plane, part * W : part * W + W] = u

    def beside(ref, low, high):
        ref[low] = lroll(ref[high - 1], WIDE)
        ref[high] = lroll(ref[low + 1], -WIDE)

    beside(y00, LOW, HIGH)
    for k in range(FULL - 1):
        beside(full.at[k], LOW, HIGH)

    def sums(x, x_p):
        bx, by, bz = full[1, x], full[2, x], full[3, x]
        sx = bx + full[1, x_p]
        sy = by + rroll(by, -1)
        sz = bz + lroll(bz, -1)
        return bx, by, bz, sx, sy, sz

    def face(n, x, kk, bn, b1, b2):
        b1, b2 = 0.25 * b1, 0.25 * b2
        q = bn * bn + b1 * b1 + b2 * b2
        s = (0.5 * FIRST_RATE * dt) * kk / jnp.maximum(q, FACE_FLOOR) * bn
        coef[3 * n, x] = s * bn
        coef[3 * n + 1, x] = 0.25 * (s * b1)
        coef[3 * n + 2, x] = 0.25 * (s * b2)

    def faces(x, carry):
        k_m, sy_m, sz_m = carry
        kap = full[0, x]
        u = y00[x]
        y01[x] = lroll(u, -1)
        y02[x] = lroll(u, 1)
        y03[x] = lroll(rroll(u, -1) - rroll(u, 1), 1)
        x_p = min(x + 1, PLANES - 1)
        bx, by, bz, sx, sy, sz = sums(x, x_p)
        face(0, x, kap + k_m, bx, sy + sy_m, sz + sz_m)
        face(1, x, kap + rroll(kap, 1), by, sz + rroll(sz, 1), sx + rroll(sx, 1))
        face(2, x, kap + lroll(kap, 1), bz, sx + lroll(sx, 1), sy + lroll(sy, 1))
        return kap, sy, sz

    for first, last in ((0, XE), (LOW, PLANES)):
        _, _, _, _, sy, sz = sums(first, first + 1)
        carry = full[0, first], sy, sz
        for x in range(first, last):
            carry = faces(x, carry)

    arrays = ((y00, y01, y02, y03), (y10, y11, y12, y13), (y20, y21, y22, y23))
    source, older = arrays[0], None
    begun = []
    for j in range(1, SECTIONS + 1):
        target = arrays[2 - j % 2]
        grow = (2.0 * j - 1.0) / j
        back = (j - 1.0) / j

        def rolled(u, u_p, u_m):
            down = rroll(u, 1)
            return down, rroll(u, -1) - down, u_p - u_m

        def flux_x(x, du, sum_y, sum_z):
            return coef[0, x] * du + coef[1, x] * sum_y + coef[2, x] * sum_z

        def plane(x, carry, source=source):
            dy, dz, fx, down = carry
            u, p, m = source[0][x], source[1][x], source[2][x]
            u_p, p_p, m_p = source[0][x + 1], source[1][x + 1], source[2][x + 1]
            down_p, dy_p, dz_p = rolled(u_p, p_p, m_p)
            fx_p = flux_x(x + 1, u_p - u, dy_p + dy, dz_p + dz)
            dx = u_p - source[0][x - 1]
            dx_zm = m_p - source[2][x - 1]
            dy_zm = source[3][x]
            fy = (
                coef[3, x] * (u - down)
                + coef[4, x] * (dz + rroll(dz, 1))
                + coef[5, x] * (dx + rroll(dx, 1))
            )
            fz = coef[6, x] * (u - m) + coef[7, x] * (dx + dx_zm) + coef[8, x] * (dy + dy_zm)
            ahead_z = lroll(fz, -1)
            rate = (fx_p - fx) + (rroll(fy, -1) - fy) - fz
            return (dy_p, dz_p, fx_p, down_p), u + rate, ahead_z

        def finish(x, new, ahead_z, target=target, older=older, grow=grow, back=back, j=j):
            new = new + ahead_z
            if j > 1:
                new = grow * new - back * older[0][x]
            if j == SECTIONS:
                b = (SECTIONS * SECTIONS + SECTIONS - 2) / (2.0 * SECTIONS * (SECTIONS + 1))
                new = (1.0 - b) * y00[x] + b * new
            if j == SECTIONS:
                target[0][x, W : 2 * W] = new[W : 2 * W]
            else:
                target[0][x] = new
                target[1][x] = lroll(new, -1)
                target[2][x] = lroll(new, 1)
                target[3][x] = lroll(rroll(new, -1) - rroll(new, 1), 1)
            return new

        def start(x, source=source):
            u_m, u = source[0][x - 1], source[0][x]
            _, dy_m, dz_m = rolled(u_m, source[1][x - 1], source[2][x - 1])
            down, dy, dz = rolled(u, source[1][x], source[2][x])
            return dy, dz, flux_x(x, u - u_m, dy + dy_m, dz + dz_m), down

        strip = []

        def finish_strip(x, new, ahead_z, finish=finish, strip=strip, target=target, j=j):
            strip.append(finish(x, new, ahead_z))
            if x == HIGH - 1 and j < SECTIONS:
                for at, u, by in ((HIGH, strip[0], -WIDE), (LOW, strip[-1], WIDE)):
                    target[0][at] = lroll(u, by)
                    target[1][at] = lroll(u, by - 1)
                    target[2][at] = lroll(u, by + 1)

        for first, last, then in ((LOW + 1, HIGH, finish_strip), (j, XE - j, finish)):
            carry = start(first)
            for x in range(first, last):
                carry, *parts = plane(x, carry)
                begun.append((then, x, *parts))
                if len(begun) > LATE:
                    then_, *parts = begun.pop(0)
                    then_(*parts)
        source, older = target, source
    for then, *parts in begun:
        then(*parts)

    def seam(main, strip, g):
        return jnp.where(
            lane < LANES - 16, lroll(main, -8), lroll(strip, LANES - 16 - 8 - WIDE * g)
        )

    for x in range(W):
        g, k = divmod(W + x, XG)
        tout_ref[x] = seam(source[0][W + x, W : 2 * W], source[0][LOW + 1 + k, W : 2 * W], g)

    SPEED = 3
    strip = range(A_LOW + 1, A_HIGH)

    def within(i):
        return i + OFF if i < XA else i - A_LOW + LOW

    for i in (*range(XA), *strip):
        x = within(i)
        _, _, _, sx, sy, sz = sums(x, x + 1)
        field = 0.25 * (sx * sx + sy * sy + sz * sz)
        vx, vy, vz = aux[0, i], aux[1, i], aux[2, i]
        flow = jnp.sqrt(vx * vx + vy * vy + vz * vz)
        aux[SPEED, i] = flow + jnp.sqrt(GAMMA * y00[x] + field / aux[SPEED, i])
    for k in range(AUX):
        aux[k, A_LOW] = lroll(aux[k, A_HIGH - 1], WIDE)

    def by_axis(u, u_m, axis):
        if axis == 0:
            return u_m
        return rroll(u, 1) if axis == 1 else lroll(u, 1)

    for i in (*range(1, XA), *strip):
        for c in range(3):
            a, b = (c + 1) % 3, (c + 2) % 3

            def mean(f, i=i, a=a, b=b):
                if 0 in (a, b):
                    other = a + b
                    u = aux[f, i] + aux[f, i - 1]
                else:
                    other = 2
                    u = aux[f, i]
                    u = u + by_axis(u, None, 1)
                return 0.125 * (u + by_axis(u, None, other))

            va, vb, s = mean(a), mean(b), mean(SPEED)
            ecoef[4 * c, i] = vb - s
            ecoef[4 * c + 1, i] = vb + s
            ecoef[4 * c + 2, i] = s - va
            ecoef[4 * c + 3, i] = -s - va

    def fields(get, first, last):
        for i in (*range(first, last), *strip):
            for c in range(3):
                a, b = (c + 1) % 3, (c + 2) % 3
                ua, ub = get(a, i), get(b, i)
                ua_b = by_axis(ua, get(a, i - 1) if b == 0 else None, b)
                ub_a = by_axis(ub, get(b, i - 1) if a == 0 else None, a)
                edge[c, i] = (ecoef[4 * c, i] * ua + ecoef[4 * c + 1, i] * ua_b) + (
                    ecoef[4 * c + 2, i] * ub + ecoef[4 * c + 3, i] * ub_a
                )
        for c in range(1, 3):
            edge[c, A_HIGH] = lroll(edge[c, A_LOW + 1], -WIDE)

    def ahead(f, i, axis):
        if axis == 0:
            return edge[f, i + 1]
        u = edge[f, i]
        return rroll(u, -1) if axis == 1 else lroll(u, -1)

    def curl(d, i):
        e, f = (d + 1) % 3, (d + 2) % 3
        return (ahead(f, i, e) - edge[f, i]) - (ahead(e, i, f) - edge[e, i])

    fields(lambda d, i: full[1 + d, within(i)], 1, XA)
    for i in (*range(1, XA - 1), *strip):
        for d in range(3):
            mid[d, i] = full[1 + d, within(i)] - dt * curl(d, i)
    for d in range(1, 3):
        mid[d, A_LOW] = lroll(mid[d, A_HIGH - 1], WIDE)
    fields(lambda d, i: mid[d, i], 2, XA - 1)

    def final(d, i):
        u = 0.5 * (full[1 + d, within(i)] + (mid[d, i] - dt * curl(d, i)))
        return u[W : 2 * W]

    for d in range(3):
        ends = [final(d, i) for i in strip]
        for x in range(W):
            g, k = divmod(W + x, XG)
            bout_ref[d, x] = seam(final(d, x + AX), ends[k], g)


def exchange(first, second, axis):
    count = lax.axis_size(axis)
    swaps = [(i, i + 1) for i in range(0, count, 2)] + [(i + 1, i) for i in range(0, count, 2)]
    others = [((a + 1) % count, (b + 1) % count) for a, b in swaps]
    return lax.ppermute(first, axis, swaps), lax.ppermute(second, axis, others)


def on_core(kernel, out, *args, scratch=(), last=False, grant=GRANT):
    space = pl.BlockSpec(memory_space=pltpu.VMEM)
    shape = [
        jax.ShapeDtypeStruct(o, jnp.float32) if last else pltpu.VMEM(o, jnp.float32) for o in out
    ]
    return pl.pallas_call(
        kernel,
        out_shape=shape,
        in_specs=[space] * len(args),
        out_specs=[space] * len(out),
        scratch_shapes=[pltpu.VMEM(shape, jnp.float32) for shape in scratch],
        compiler_params=pltpu.CompilerParams(vmem_limit_bytes=grant),
        name=kernel.__name__,
    )(*args)


def held(*arrays):
    return [pltpu.with_memory_space_constraint(a, pltpu.VMEM) for a in arrays]


def on_device(t, diffusivity, b, v, rho):
    zs = lax.axis_size("gz")
    outer = lax.axis_size("gx_1") * lax.axis_size("gy")
    inner = lax.axis_size("gx_0") * lax.axis_size("gx_2")
    out = [((FULL + AUX) * W, W, LANES), (zs, ZT, W, LANES)]
    cells, edges = on_core(pack_z, out, t, diffusivity, b, v, rho, grant=None)
    edges = lax.all_to_all(edges, "gz", 0, 0, tiled=True)
    cells, edges = held(cells, edges)
    out = [(SIDE, W, LANES)] * 2 + [((W + 1) * AUX, W, LANES), (outer, 1, LANES)]
    first, second, aux, low = on_core(pack_x, out, cells, edges)
    x_first, x_second = exchange(first, second, GX)
    low = lax.all_to_all(low, ("gx_1", "gy"), 0, 0, tiled=True)
    args = held(first, aux, x_first, x_second, low)
    out = [(YT, W, LANES)] * 2 + [(A_TILES, W, LANES), (inner, 1, LANES)]
    first, second, aux, low = on_core(pack_y, out, *args)
    y_first, y_second = exchange(first, second, "gy")
    low = lax.all_to_all(low, ("gx_0", "gx_2"), 0, 0, tiled=True)
    out = [(W, W, LANES), (3, W, W, LANES)]
    args = held(first, aux, y_first, y_second, low)
    return tuple(on_core(advance, out, *args, scratch=SCRATCH, last=True))


def solution(mesh):
    gx, gy, gz = (mesh.shape[axis] for axis in ("gx", "gy", "gz"))
    outer = 3 if gx % 6 == 0 else 1
    finer = Mesh(mesh.devices.reshape(outer, gx // outer // 2, 2, gy, gz), (*GX, "gy", "gz"))
    cell = P(GX, "gy", "gz")
    face = P(None, GX, "gy", "gz")
    return jax.shard_map(
        on_device,
        mesh=finer,
        in_specs=(cell, cell, face, face, cell),
        out_specs=(cell, face),
        check_vma=False,
    )
```

```python
import jax
import jax.numpy as jnp
from jax import lax
from jax.experimental import pallas as pl
from jax.experimental.pallas import tpu as pltpu
from jax.sharding import Mesh
from jax.sharding import PartitionSpec as P

SECTIONS = 8
GAMMA = 5.0 / 3.0
FACE_FLOOR = 0.25

GX = ("gx_0", "gx_1", "gx_2")
W = 8
LANES = 128
XE = 3 * W
WIDE = 4 * W
GROUPS = LANES // WIDE
XG = XE // GROUPS
LOW, HIGH = XE, XE + XG + 1
PLANES = HIGH + 1
ROWS = 3 * W
FULL = 5
AUX = 4
AX = 2
XA = W + 2 * AX
OFF = W - AX
A_LOW, A_HIGH = XA, XA + XG + 1
A_PLANES = A_HIGH + 1
ZT = (FULL + AUX) * W // 16 + 1
SPARE = LANES // 2
SIDE = FULL * W + AUX * AX + FULL + 1
A_TILES = AUX * (XA + XG)
Y_FULL = FULL * (XE + XG)
YT = Y_FULL + A_TILES // 4
GRANT = 28 << 20
SCRATCH = [(PLANES, ROWS, LANES)] * 12 + [
    (FULL - 1, PLANES, ROWS, LANES),
    (AUX, A_PLANES, ROWS, LANES),
    (9, PLANES, ROWS, LANES),
    (3, PLANES, ROWS, LANES),
    (12, A_PLANES, ROWS, LANES),
    (3, A_PLANES, ROWS, LANES),
    (3, A_PLANES, ROWS, LANES),
]
LATE = 5
FIRST_RATE = 4.0 / (SECTIONS * SECTIONS + SECTIONS - 2)
LIMIT = (SECTIONS * SECTIONS + SECTIONS - 2) / 16.0


def lane_ids(rows):
    return lax.broadcasted_iota(jnp.int32, (rows, LANES), 1)


def lroll(u, amount):
    return pltpu.roll(u, amount % LANES, 1)


def rroll(u, amount):
    return pltpu.roll(u, amount % u.shape[0], 0)


def lowest(u):
    return jnp.min(jnp.min(u, axis=0, keepdims=True), axis=1, keepdims=True)


def neighbours(axis):
    count = lax.axis_size(axis)
    at = lax.axis_index(axis)
    return lax.rem(at + count - 1, count), lax.rem(at + 1, count)


def is_odd(axis):
    return lax.rem(lax.axis_index(axis), 2) == 1


def piece(field, plane):
    return divmod(field * W + plane, 16)


def pack_z(t_ref, d_ref, b_ref, v_ref, r_ref, all_ref, out_ref):
    t = t_ref[...]
    kappa = d_ref[...] * (t * t * jnp.sqrt(t))
    low = lowest(jnp.min(LIMIT / kappa, axis=0))
    lane = lane_ids(W)
    left, right = [], []
    for tile in range(ZT):
        below = above = jnp.broadcast_to(low, (W, LANES))
        for k in range(16):
            field, plane = divmod(tile * 16 + k, W)
            if field >= FULL + AUX:
                break
            if field == 0:
                u = t[plane]
            elif field == 1:
                u = kappa[plane]
            elif field < FULL:
                u = b_ref[field - 2, plane]
            else:
                u = v_ref[field - FULL, plane] if field < FULL + 3 else r_ref[plane]
            all_ref[field * W + plane] = u
            here = (lane >= 8 * k) & (lane < 8 * k + 8)
            below = jnp.where(here, lroll(u, 8 * k), below)
            above = jnp.where(here, lroll(u, 8 * k - (LANES - 8)), above)
        left.append(below)
        right.append(above)
    lo, _ = neighbours("gz")
    for slot in range(out_ref.shape[0]):
        for tile in range(ZT):
            out_ref[slot, tile] = jnp.where(lo == slot, left[tile], right[tile])


def pack_x(all_ref, z_ref, a_ref, o_ref, aux_ref, low_ref):
    odd = is_odd(GX)
    lo, hi = neighbours("gz")
    lane = lane_ids(W)
    left = [z_ref[lo, tile] for tile in range(ZT)]
    right = [z_ref[hi, tile] for tile in range(ZT)]
    up_ends = down_ends = jnp.zeros((W, LANES), jnp.float32)
    for field in range(FULL + AUX):
        ends = jnp.zeros((W, LANES), jnp.float32)
        for plane in range(W):
            u = all_ref[field * W + plane]
            tile, k = piece(field, plane)
            main = jnp.where(lane < 8, lroll(left[tile], -8 * k), lroll(u, 8))
            to = 16 * plane
            end = jnp.where(
                lane < to + 8, lroll(u, to + 8 - LANES), lroll(right[tile], to + 8 - 8 * k)
            )
            ends = jnp.where(lane < to, ends, end)
            if field < FULL:
                a_ref[field * W + plane] = main
                o_ref[field * W + plane] = main
                continue
            aux_ref[(field - FULL) * W + plane] = main
            at = FULL * W + (field - FULL) * AX
            if plane < AX:
                a_ref[at + plane] = main
                o_ref[at + plane] = main
            elif plane >= W - AX:
                i = at + plane - (W - AX)
                down = a_ref[i]
                a_ref[i] = jnp.where(odd, down, main)
                o_ref[i] = jnp.where(odd, main, down)
        if field < FULL:
            a_ref[FULL * W + AUX * AX + field] = ends
            o_ref[FULL * W + AUX * AX + field] = ends
        else:
            f = field - FULL
            aux_ref[AUX * W + f] = ends
            here = lane >= 32 * f
            down_ends = jnp.where(here, lroll(ends, 32 * f), down_ends)
            up_ends = jnp.where(here, lroll(ends, 32 * f - (LANES - 32)), up_ends)
    a_ref[SIDE - 1] = jnp.where(odd, down_ends, up_ends)
    o_ref[SIDE - 1] = jnp.where(odd, up_ends, down_ends)
    low = z_ref[0, ZT - 1]
    for slot in range(1, z_ref.shape[0]):
        low = jnp.minimum(low, z_ref[slot, ZT - 1])
    low = lowest(jnp.where(lane >= SPARE, low, jnp.max(low)))
    low_ref[...] = jnp.broadcast_to(low.reshape(1, 1, 1), low_ref.shape)


def pack_y(own_ref, ownaux_ref, xa_ref, xo_ref, min_ref, a_ref, o_ref, aux_ref, low_ref):
    odd_x, odd_y = is_odd(GX), is_odd("gy")
    lane = lane_ids(W)

    def below(i):
        return jnp.where(odd_x, xa_ref[i], xo_ref[i])

    def above(i):
        return jnp.where(odd_x, xo_ref[i], xa_ref[i])

    sides = (below, own_ref.__getitem__, above)

    def send(i, u):
        a_ref[i] = u
        o_ref[i] = u

    ends_at = FULL * W + AUX * AX
    for field in range(FULL):
        ends = [get(ends_at + field) for get in sides]
        mains = []
        for x in range(XE):
            part, at = divmod(x, W)
            mains.append(sides[part](field * W + at))
            send(field * XE + x, mains[x])
        for k in range(XG):
            strip = None
            for g in range(GROUPS):
                part, at = divmod(g * XG + k, W)
                to = g * WIDE
                new = jnp.where(
                    lane < to + 16,
                    lroll(mains[g * XG + k], to + 16 - LANES),
                    lroll(ends[part], to + 16 - 16 * at),
                )
                strip = jnp.where(lane < to, strip, new) if g else new
            send(FULL * XE + field * XG + k, strip)

    def put(i, u):
        aux_ref[i] = u
        tile, k = Y_FULL + i // 4, AX * (i % 4)
        up, down = u[W - AX : W], u[0:AX]
        a_ref[tile, k : k + AX] = jnp.where(odd_y, down, up)
        o_ref[tile, k : k + AX] = jnp.where(odd_y, up, down)

    outer = below(SIDE - 1), above(SIDE - 1)
    for field in range(AUX):
        mains, ends = [], []
        at = FULL * W + field * AX
        for i in range(XA):
            if i < AX:
                mains.append(below(at + i))
                ends.append((outer[0], field * AX + i))
            elif i < AX + W:
                mains.append(ownaux_ref[field * W + i - AX])
                ends.append((ownaux_ref[AUX * W + field], i - AX))
            else:
                mains.append(above(at + i - AX - W))
                ends.append((outer[1], field * AX + i - AX - W))
            put(field * XA + i, mains[i])
        for k in range(XG):
            strip = None
            for g in range(XA // XG):
                u, (end, at_end) = mains[g * XG + k], ends[g * XG + k]
                to = (g + OFF // XG) * WIDE
                new = lroll(u, to + 16 - LANES)
                strip = jnp.where(lane < to, strip, new) if g else new
                new = lroll(end, to + 16 - 16 * at_end)
                strip = jnp.where((lane >= to + 16) & (lane < to + 32), new, strip)
            put(AUX * XA + field * XG + k, strip)
    low = lowest(jnp.min(min_ref[...], axis=0))
    low_ref[...] = jnp.broadcast_to(low.reshape(1, 1, 1), low_ref.shape)


def sweep(first, last, body, carry, by):
    trips = (last - first) // by

    def several(i, carry):
        for k in range(by):
            carry = body(first + i * by + k, carry)
        return carry

    if trips:
        carry = lax.fori_loop(0, trips, several, carry)
    for x in range(first + trips * by, last):
        carry = body(x, carry)
    return carry


def advance(
    own_ref, aux_ref, ya_ref, yo_ref, low_ref, tout_ref, bout_ref,
    y00, y01, y02, y03, y10, y11, y12, y13, y20, y21, y22, y23, full, aux, coef, coef_up, ecoef, edge, mid,
):
    lane = lane_ids(W)
    dt = lowest(jnp.min(low_ref[...], axis=0))
    odd = is_odd("gy")

    sides = (
        lambda i: jnp.where(odd, ya_ref[i], yo_ref[i]),
        own_ref.__getitem__,
        lambda i: jnp.where(odd, yo_ref[i], ya_ref[i]),
    )
    for field in range(FULL):
        to = y00 if field == 0 else full.at[field - 1]
        for x in range(XE + XG):
            i, plane = field * XE + x, x
            if x >= XE:
                i, plane = FULL * XE + field * XG + x - XE, x + 1
            for part in range(3):
                to[plane, part * W : part * W + W] = sides[part](i)
    for field in range(AUX):
        for x in range(XA + XG):
            i, plane = field * XA + x, x
            if x >= XA:
                i, plane = AUX * XA + field * XG + x - XA, x + 1
            tile, k = Y_FULL + i // 4, AX * (i % 4)
            for part in range(3):
                u = aux_ref[i] if part == 1 else jnp.tile(sides[part](tile)[k : k + AX], (4, 1))
                aux[field, plane, part * W : part * W + W] = u

    def beside(ref, low, high):
        ref[low] = lroll(ref[high - 1], WIDE)
        ref[high] = lroll(ref[low + 1], -WIDE)

    beside(y00, LOW, HIGH)
    for k in range(FULL - 1):
        beside(full.at[k], LOW, HIGH)

    def sums(x, x_p):
        bx, by, bz = full[1, x], full[2, x], full[3, x]
        sx = bx + full[1, x_p]
        sy = by + rroll(by, -1)
        sz = bz + lroll(bz, -1)
        return bx, by, bz, sx, sy, sz

    def face(n, x, kk, bn, b1, b2):
        b1, b2 = 0.25 * b1, 0.25 * b2
        q = bn * bn + b1 * b1 + b2 * b2
        s = (0.5 * FIRST_RATE * dt) * kk / jnp.maximum(q, FACE_FLOOR) * bn
        coef[3 * n, x] = s * bn
        coef[3 * n + 1, x] = 0.25 * (s * b1)
        coef[3 * n + 2, x] = 0.25 * (s * b2)

    def faces(x, carry):
        k_m, sy_m, sz_m = carry
        kap = full[0, x]
        u = y00[x]
        y01[x] = lroll(u, -1)
        y02[x] = lroll(u, 1)
        y03[x] = lroll(rroll(u, -1) - rroll(u, 1), 1)
        x_p = min(x + 1, PLANES - 1)
        bx, by, bz, sx, sy, sz = sums(x, x_p)
        face(0, x, kap + k_m, bx, sy + sy_m, sz + sz_m)
        face(1, x, kap + rroll(kap, 1), by, sz + rroll(sz, 1), sx + rroll(sx, 1))
        face(2, x, kap + lroll(kap, 1), bz, sx + lroll(sx, 1), sy + lroll(sy, 1))
        return kap, sy, sz

    for first, last in ((0, XE), (LOW, PLANES)):
        _, _, _, _, sy, sz = sums(first, first + 1)
        carry = full[0, first], sy, sz
        for x in range(first, last):
            carry = faces(x, carry)

    arrays = ((y00, y01, y02, y03), (y10, y11, y12, y13), (y20, y21, y22, y23))
    source, older = arrays[0], None
    begun = []
    for j in range(1, SECTIONS + 1):
        target = arrays[2 - j % 2]
        grow = (2.0 * j - 1.0) / j
        back = (j - 1.0) / j

        def rolled(u, u_p, u_m):
            down = rroll(u, 1)
            return down, rroll(u, -1) - down, u_p - u_m

        def flux_x(x, du, sum_y, sum_z):
            return coef[0, x] * du + coef[1, x] * sum_y + coef[2, x] * sum_z

        def plane(x, carry, source=source):
            dy, dz, fx, down = carry
            u, p, m = source[0][x], source[1][x], source[2][x]
            u_p, p_p, m_p = source[0][x + 1], source[1][x + 1], source[2][x + 1]
            down_p, dy_p, dz_p = rolled(u_p, p_p, m_p)
            fx_p = flux_x(x + 1, u_p - u, dy_p + dy, dz_p + dz)
            dx = u_p - source[0][x - 1]
            dx_zm = m_p - source[2][x - 1]
            dy_zm = source[3][x]
            fy = (
                coef[3, x] * (u - down)
                + coef[4, x] * (dz + rroll(dz, 1))
                + coef[5, x] * (dx + rroll(dx, 1))
            )
            fz = coef[6, x] * (u - m) + coef[7, x] * (dx + dx_zm) + coef[8, x] * (dy + dy_zm)
            ahead_z = lroll(fz, -1)
            rate = (fx_p - fx) + (rroll(fy, -1) - fy) - fz
            return (dy_p, dz_p, fx_p, down_p), u + rate, ahead_z

        def finish(x, new, ahead_z, target=target, older=older, grow=grow, back=back, j=j):
            new = new + ahead_z
            if j > 1:
                new = grow * new - back * older[0][x]
            if j == SECTIONS:
                b = (SECTIONS * SECTIONS + SECTIONS - 2) / (2.0 * SECTIONS * (SECTIONS + 1))
                new = (1.0 - b) * y00[x] + b * new
            if j == SECTIONS:
                target[0][x, W : 2 * W] = new[W : 2 * W]
            else:
                target[0][x] = new
                target[1][x] = lroll(new, -1)
                target[2][x] = lroll(new, 1)
                target[3][x] = lroll(rroll(new, -1) - rroll(new, 1), 1)
            return new

        def start(x, source=source):
            u_m, u = source[0][x - 1], source[0][x]
            _, dy_m, dz_m = rolled(u_m, source[1][x - 1], source[2][x - 1])
            down, dy, dz = rolled(u, source[1][x], source[2][x])
            return dy, dz, flux_x(x, u - u_m, dy + dy_m, dz + dz_m), down

        strip = []

        def finish_strip(x, new, ahead_z, finish=finish, strip=strip, target=target, j=j):
            strip.append(finish(x, new, ahead_z))
            if x == HIGH - 1 and j < SECTIONS:
                for at, u, by in ((HIGH, strip[0], -WIDE), (LOW, strip[-1], WIDE)):
                    target[0][at] = lroll(u, by)
                    target[1][at] = lroll(u, by - 1)
                    target[2][at] = lroll(u, by + 1)

        for first, last, then in ((LOW + 1, HIGH, finish_strip), (j, XE - j, finish)):
            carry = start(first)
            for x in range(first, last):
                carry, *parts = plane(x, carry)
                begun.append((then, x, *parts))
                if len(begun) > LATE:
                    then_, *parts = begun.pop(0)
                    then_(*parts)
        source, older = target, source
    for then, *parts in begun:
        then(*parts)

    def seam(main, strip, g):
        return jnp.where(
            lane < LANES - 16, lroll(main, -8), lroll(strip, LANES - 16 - 8 - WIDE * g)
        )

    for x in range(W):
        g, k = divmod(W + x, XG)
        tout_ref[x] = seam(source[0][W + x, W : 2 * W], source[0][LOW + 1 + k, W : 2 * W], g)

    SPEED = 3
    strip = range(A_LOW + 1, A_HIGH)

    def within(i):
        return i + OFF if i < XA else i - A_LOW + LOW

    for i in (*range(XA), *strip):
        x = within(i)
        _, _, _, sx, sy, sz = sums(x, x + 1)
        field = 0.25 * (sx * sx + sy * sy + sz * sz)
        vx, vy, vz = aux[0, i], aux[1, i], aux[2, i]
        flow = jnp.sqrt(vx * vx + vy * vy + vz * vz)
        aux[SPEED, i] = flow + jnp.sqrt(GAMMA * y00[x] + field / aux[SPEED, i])
    for k in range(AUX):
        aux[k, A_LOW] = lroll(aux[k, A_HIGH - 1], WIDE)

    def by_axis(u, u_m, axis):
        if axis == 0:
            return u_m
        return rroll(u, 1) if axis == 1 else lroll(u, 1)

    for i in (*range(1, XA), *strip):
        for c in range(3):
            a, b = (c + 1) % 3, (c + 2) % 3

            def mean(f, i=i, a=a, b=b):
                if 0 in (a, b):
                    other = a + b
                    u = aux[f, i] + aux[f, i - 1]
                else:
                    other = 2
                    u = aux[f, i]
                    u = u + by_axis(u, None, 1)
                return 0.125 * (u + by_axis(u, None, other))

            va, vb, s = mean(a), mean(b), mean(SPEED)
            ecoef[4 * c, i] = vb - s
            ecoef[4 * c + 1, i] = vb + s
            ecoef[4 * c + 2, i] = s - va
            ecoef[4 * c + 3, i] = -s - va

    def fields(get, first, last):
        for i in (*range(first, last), *strip):
            for c in range(3):
                a, b = (c + 1) % 3, (c + 2) % 3
                ua, ub = get(a, i), get(b, i)
                ua_b = by_axis(ua, get(a, i - 1) if b == 0 else None, b)
                ub_a = by_axis(ub, get(b, i - 1) if a == 0 else None, a)
                edge[c, i] = (ecoef[4 * c, i] * ua + ecoef[4 * c + 1, i] * ua_b) + (
                    ecoef[4 * c + 2, i] * ub + ecoef[4 * c + 3, i] * ub_a
                )
        for c in range(1, 3):
            edge[c, A_HIGH] = lroll(edge[c, A_LOW + 1], -WIDE)

    def ahead(f, i, axis):
        if axis == 0:
            return edge[f, i + 1]
        u = edge[f, i]
        return rroll(u, -1) if axis == 1 else lroll(u, -1)

    def curl(d, i):
        e, f = (d + 1) % 3, (d + 2) % 3
        return (ahead(f, i, e) - edge[f, i]) - (ahead(e, i, f) - edge[e, i])

    fields(lambda d, i: full[1 + d, within(i)], 1, XA)
    for i in (*range(1, XA - 1), *strip):
        for d in range(3):
            mid[d, i] = full[1 + d, within(i)] - dt * curl(d, i)
    for d in range(1, 3):
        mid[d, A_LOW] = lroll(mid[d, A_HIGH - 1], WIDE)
    fields(lambda d, i: mid[d, i], 2, XA - 1)

    def final(d, i):
        u = 0.5 * (full[1 + d, within(i)] + (mid[d, i] - dt * curl(d, i)))
        return u[W : 2 * W]

    for d in range(3):
        ends = [final(d, i) for i in strip]
        for x in range(W):
            g, k = divmod(W + x, XG)
            bout_ref[d, x] = seam(final(d, x + AX), ends[k], g)


def exchange(first, second, axis):
    count = lax.axis_size(axis)
    swaps = [(i, i + 1) for i in range(0, count, 2)] + [(i + 1, i) for i in range(0, count, 2)]
    others = [((a + 1) % count, (b + 1) % count) for a, b in swaps]
    return lax.ppermute(first, axis, swaps), lax.ppermute(second, axis, others)


def on_core(kernel, out, *args, scratch=(), last=False, grant=GRANT):
    space = pl.BlockSpec(memory_space=pltpu.VMEM)
    shape = [
        jax.ShapeDtypeStruct(o, jnp.float32) if last else pltpu.VMEM(o, jnp.float32) for o in out
    ]
    return pl.pallas_call(
        kernel,
        out_shape=shape,
        in_specs=[space] * len(args),
        out_specs=[space] * len(out),
        scratch_shapes=[pltpu.VMEM(shape, jnp.float32) for shape in scratch],
        compiler_params=pltpu.CompilerParams(vmem_limit_bytes=grant),
        name=kernel.__name__,
    )(*args)


def held(*arrays):
    return [pltpu.with_memory_space_constraint(a, pltpu.VMEM) for a in arrays]


def on_device(t, diffusivity, b, v, rho):
    zs = lax.axis_size("gz")
    outer = lax.axis_size("gx_1") * lax.axis_size("gx_2") * lax.axis_size("gy")
    inner = lax.axis_size("gx_0")
    out = [((FULL + AUX) * W, W, LANES), (zs, ZT, W, LANES)]
    cells, edges = on_core(pack_z, out, t, diffusivity, b, v, rho, grant=None)
    edges = lax.all_to_all(edges, "gz", 0, 0, tiled=True)
    cells, edges = held(cells, edges)
    out = [(SIDE, W, LANES)] * 2 + [((W + 1) * AUX, W, LANES), (outer, 1, LANES)]
    first, second, aux, low = on_core(pack_x, out, cells, edges)
    x_first, x_second = exchange(first, second, GX)
    low = lax.all_to_all(low, ("gx_1", "gx_2", "gy"), 0, 0, tiled=True)
    args = held(first, aux, x_first, x_second, low)
    out = [(YT, W, LANES)] * 2 + [(A_TILES, W, LANES), (inner, 1, LANES)]
    first, second, aux, low = on_core(pack_y, out, *args)
    y_first, y_second = exchange(first, second, "gy")
    low = lax.all_to_all(low, "gx_0", 0, 0, tiled=True)
    out = [(W, W, LANES), (3, W, W, LANES)]
    args = held(first, aux, y_first, y_second, low)
    return tuple(on_core(advance, out, *args, scratch=SCRATCH, last=True))


def solution(mesh):
    gx, gy, gz = (mesh.shape[axis] for axis in ("gx", "gy", "gz"))
    outer = 3 if gx % 6 == 0 else 1
    finer = Mesh(mesh.devices.reshape(outer, gx // outer // 2, 2, gy, gz), (*GX, "gy", "gz"))
    cell = P(GX, "gy", "gz")
    face = P(None, GX, "gy", "gz")
    return jax.shard_map(
        on_device,
        mesh=finer,
        in_specs=(cell, cell, face, face, cell),
        out_specs=(cell, face),
        check_vma=False,
    )
```
